128 devices in a mesh: gz: 4 (over z), gy: 4 (over y), gx: 8 (over x, core).
Axes of the slice: x: 4, y: 4, z: 4, core: 2. Of those that a mesh axis runs over, the one named last changes fastest.
Arguments:
- k_cell: float32 [256, 256, 256], P('gx', 'gy', 'gz')
- k_ghost: float32 [6, 256, 256], replicated
- f_rhs: float32 [256, 256, 256], P('gx', 'gy', 'gz')
- u_init: float32 [256, 256, 256], P('gx', 'gy', 'gz')
Outputs:
- output 1: float32 [256, 256, 256], P('gx', 'gy', 'gz')
- output 2: float32 [256, 256, 256], P('gx', 'gy', 'gz')
- output 3: float32 [8], replicated
All inputs are finite; a program needn't handle non-finite values.
Results may differ from the reference program's by a relative error of at most 0.001.
Values sent between devices are 32-bit elements.
A program may use at most 1 GiB of HBM per device.

```python
import jax
import jax.numpy as jnp
from jax import lax

GRID_SIDE = 256
CG_ITERS = 8


def setup_inputs(seed: int = 0) -> dict:
    grid_side = GRID_SIDE
    key_list = jax.random.split(jax.random.key(seed), 9)
    block_len = grid_side // 8
    cube_shape = (grid_side, grid_side, grid_side)
    cell_part = jax.random.uniform(key_list[0], cube_shape, jnp.float32, -1.0, 1.0)
    block_part = jax.random.uniform(key_list[1], (8, 8, 8), jnp.float32, -1.0, 1.0)
    block_part = jnp.repeat(jnp.repeat(jnp.repeat(block_part, block_len, axis=0), block_len, axis=1), block_len, axis=2)
    k_cell = jnp.exp(2.302585 * (0.5 * cell_part + 0.5 * block_part))
    k_ghost = jnp.exp(2.302585 * jax.random.uniform(key_list[2], (6, grid_side, grid_side), jnp.float32, -1.0, 1.0))
    coord_1d = jnp.arange(grid_side, dtype=jnp.float32) + 1.0
    wave_num = jax.random.randint(key_list[3], (3, 3), 1, 5).astype(jnp.float32)
    mode_amp = 2.0 * jax.random.normal(key_list[4], (3,), jnp.float32)
    profile = jnp.sin(jnp.pi * wave_num[:, :, None] * coord_1d[None, None, :] / (grid_side + 1.0))
    smooth = jnp.einsum('m,mi,mj,mk->ijk', mode_amp, profile[:, 0], profile[:, 1], profile[:, 2])
    src_pos = jax.random.randint(key_list[5], (64, 3), 1, 8) * block_len + jax.random.randint(key_list[6], (64, 3), -1, 1)
    src_amp = 10.0 * jax.random.normal(key_list[7], (64,), jnp.float32)
    f_rhs = smooth.at[src_pos[:, 0], src_pos[:, 1], src_pos[:, 2]].add(src_amp)
    u_init = 0.3 * jax.random.normal(key_list[8], cube_shape, jnp.float32)
    return {'k_cell': k_cell, 'k_ghost': k_ghost, 'f_rhs': f_rhs, 'u_init': u_init}


def reference(k_cell, k_ghost, f_rhs, u_init):
    k_x = jnp.concatenate([k_ghost[0][None], k_cell, k_ghost[1][None]], axis=0)
    k_y = jnp.concatenate([k_ghost[2][:, None], k_cell, k_ghost[3][:, None]], axis=1)
    k_z = jnp.concatenate([k_ghost[4][:, :, None], k_cell, k_ghost[5][:, :, None]], axis=2)
    coef_x = 2.0 * k_x[:-1] * k_x[1:] / (k_x[:-1] + k_x[1:])
    coef_y = 2.0 * k_y[:, :-1] * k_y[:, 1:] / (k_y[:, :-1] + k_y[:, 1:])
    coef_z = 2.0 * k_z[:, :, :-1] * k_z[:, :, 1:] / (k_z[:, :, :-1] + k_z[:, :, 1:])
    diag_sum = coef_x[:-1] + coef_x[1:] + coef_y[:, :-1] + coef_y[:, 1:] + coef_z[:, :, :-1] + coef_z[:, :, 1:]
    inv_diag = 1.0 / diag_sum

    def apply_op(grid_field):
        pad_x = jnp.pad(grid_field, ((1, 1), (0, 0), (0, 0)))
        pad_y = jnp.pad(grid_field, ((0, 0), (1, 1), (0, 0)))
        pad_z = jnp.pad(grid_field, ((0, 0), (0, 0), (1, 1)))
        flux_x = coef_x * (pad_x[1:] - pad_x[:-1])
        flux_y = coef_y * (pad_y[:, 1:] - pad_y[:, :-1])
        flux_z = coef_z * (pad_z[:, :, 1:] - pad_z[:, :, :-1])
        return (flux_x[:-1] - flux_x[1:]) + (flux_y[:, :-1] - flux_y[:, 1:]) + (flux_z[:, :, :-1] - flux_z[:, :, 1:])

    residual = f_rhs - apply_op(u_init)
    precond = residual * inv_diag
    rz_start = jnp.sum(residual * precond)

    def cg_step(cg_state, unused):
        approx, residual, direction, rz_old = cg_state
        q_vec = apply_op(direction)
        step_alpha = rz_old / jnp.sum(direction * q_vec)
        approx = approx + step_alpha * direction
        residual = residual - step_alpha * q_vec
        precond = residual * inv_diag
        rz_new = jnp.sum(residual * precond)
        direction = precond + (rz_new / rz_old) * direction
        return (approx, residual, direction, rz_new), jnp.sum(residual * residual)

    final_state, history = lax.scan(cg_step, (u_init, residual, precond, rz_start), None, length=CG_ITERS)
    return final_state[0], final_state[1], history
```

```python
import functools

import jax
import jax.numpy as jnp
from jax import lax
from jax.experimental import pallas as pl
from jax.experimental.pallas import tpu as pltpu
from jax.sharding import PartitionSpec as P

CG_ITERS = 8
NB = CG_ITERS + 1
NX, NY, NZ = 32, 64, 64
NP = NX // 2
R0 = 8
MESH = pl.DeviceIdType.MESH
AXES = ('gx', 'gy', 'gz')
BOUND = 4096.0
F32 = jnp.float32
SUB, LANES, HALF, LOW = 8, 128, 64, 63
ROWS = NY // SUB
TILE = (SUB, LANES)
WIDE = (2 * SUB, LANES)
FACES = 6


def own(t):
    return slice(R0 + SUB * t, R0 + SUB * t + SUB)


def tile(t):
    return slice(SUB * t, SUB * t + SUB)


def one(i):
    return slice(i, i + 1)


def spin(values, by):
    return pltpu.roll(values, by, 1)


def turn_half(values):
    return spin(values, HALF)


def row_sum(values):
    return jnp.sum(values, axis=0, keepdims=True)


def lane_sum(values):
    return jnp.sum(values, axis=1, keepdims=True)


def total_of(parts):
    parts = list(parts)
    while len(parts) > 1:
        parts = [sum(parts[i + 1:i + 2], parts[i]) for i in range(0, len(parts), 2)]
    return parts[0]


def lane_iota(rows=8):
    return lax.broadcasted_iota(jnp.int32, (rows, LANES), 1)


def row_iota(rows):
    return lax.broadcasted_iota(jnp.int32, (rows, LANES), 0)


class Comm:
    def __init__(self, counts, bufs):
        self.counts = counts
        self.pos = [lax.axis_index(name) for name in AXES]
        self.has = []
        for axis in range(3):
            self.has.append(self.pos[axis] > 0)
            self.has.append(self.pos[axis] < counts[axis] - 1)
        (self.xs, self.ys, self.zs, self.xr, self.yr, self.zr, self.send_sem, self.recv_sem) = bufs

    def copies(self, rnd, face):
        axis, high = face // 2, face % 2
        src = (self.xs, self.ys, self.zs)[axis]
        dst = (self.xr, self.yr, self.zr)[axis]
        step = 1 if high else -1
        return pltpu.make_async_remote_copy(
            src_ref=src.at[rnd, high], dst_ref=dst.at[rnd, 1 - high],
            send_sem=self.send_sem.at[rnd, face], recv_sem=self.recv_sem.at[rnd, face ^ 1],
            device_id={AXES[axis]: self.pos[axis] + step}, device_id_type=MESH)

    def send(self, rnd, face):
        @pl.when(self.has[face])
        def _():
            self.copies(rnd, face).start()

    def wait_recv(self, rnd, face):
        axis, high = face // 2, face % 2
        src = (self.xs, self.ys, self.zs)[axis]
        dst = (self.xr, self.yr, self.zr)[axis]
        step = 1 if high else -1

        @pl.when(self.has[face])
        def _():
            pltpu.make_async_remote_copy(
                src_ref=src.at[rnd, high], dst_ref=dst.at[rnd, high],
                send_sem=self.send_sem.at[rnd, face], recv_sem=self.recv_sem.at[rnd, face],
                device_id={AXES[axis]: self.pos[axis] + step}, device_id_type=MESH).wait_recv()

    def wait_send(self, rnd, face):
        @pl.when(self.has[face])
        def _():
            self.copies(rnd, face).wait_send()


def barrier_all_lines(comm):
    sem = pltpu.get_barrier_semaphore()
    total = 0
    for axis in range(3):
        n = comm.counts[axis]
        for off in range(1, n):
            pl.semaphore_signal(sem, inc=1, device_id={AXES[axis]: lax.rem(comm.pos[axis] + off, n)}, device_id_type=MESH)
            total += 1
    return sem, total


class Reducer:
    def __init__(self, comm, send_row, recv_rows, send_sem, recv_sem):
        self.comm, self.send_row, self.recv_rows, self.ss, self.rs = comm, send_row, recv_rows, send_sem, recv_sem

    def copy(self, axis, off):
        n, me = self.comm.counts[axis], self.comm.pos[axis]
        return pltpu.make_async_remote_copy(
            src_ref=self.send_row.at[axis], dst_ref=self.recv_rows[axis].at[me],
            send_sem=self.ss.at[axis, off], recv_sem=self.rs.at[axis, off],
            device_id={AXES[axis]: lax.rem(me + off, n)}, device_id_type=MESH)

    def run(self, row):
        for axis in range(3):
            n, me = self.comm.counts[axis], self.comm.pos[axis]
            rows = self.recv_rows[axis]
            self.send_row[axis] = row
            rows[me] = row
            for off in range(1, n):
                self.copy(axis, off).start()
            for off in range(1, n):
                self.copy(axis, off).wait()
            parts = [rows[i] for i in range(n)]
            row = total_of(parts)
        return row


def store_plane_faces(comm, rnd, ref, p):
    comm.ys[rnd, 0, p] = ref[p + 1, R0:R0 + 1, :]
    comm.ys[rnd, 1, p] = ref[p + 1, R0 + NY - 1:R0 + NY, :]


def pack_x_faces(comm, rnd, ref):
    half = NY // 2
    lane = lane_iota(half)
    a, b = ref[1, R0:R0 + half, :], ref[1, R0 + half:R0 + NY, :]
    comm.xs[rnd, 0] = jnp.where(lane < HALF, a, turn_half(b))
    a, b = ref[NP, R0:R0 + half, :], ref[NP, R0 + half:R0 + NY, :]
    comm.xs[rnd, 1] = jnp.where(lane < HALF, turn_half(a), b)


def z_pack_tile(vals, t, p, acc):
    s = 4 * p + t % 4
    lane = lane_iota() & LOW
    w = pltpu.roll(vals, s, 1)
    e = t // 4
    acc[e] = jnp.where(lane == s, w, acc[e])
    acc[2 + e] = jnp.where(lane == ((s + LOW) & LOW), w, acc[2 + e])


def z_ghost_lo(zr, rnd, t, p):
    s = 4 * p + t % 4
    return pltpu.roll(zr[rnd, 0, t // 4], 65 - s, 1)


def z_ghost_hi(zr, rnd, t, p):
    s = 4 * p + t % 4
    return pltpu.roll(zr[rnd, 1, t // 4], LOW - s, 1)


def unpack_xy(comm, rnd, ref):
    half = NY // 2
    lane = lane_iota(half)
    lo, hi = comm.xr[rnd, 0], comm.xr[rnd, 1]
    top_a, top_b = ref[NP, R0:R0 + half, :], ref[NP, R0 + half:R0 + NY, :]
    ref[0, R0:R0 + half, :] = jnp.where(lane < HALF, lo, turn_half(top_a))
    ref[0, R0 + half:R0 + NY, :] = jnp.where(lane < HALF, turn_half(lo), turn_half(top_b))
    bot_a, bot_b = ref[1, R0:R0 + half, :], ref[1, R0 + half:R0 + NY, :]
    ref[NP + 1, R0:R0 + half, :] = jnp.where(lane < HALF, turn_half(bot_a), turn_half(hi))
    ref[NP + 1, R0 + half:R0 + NY, :] = jnp.where(lane < HALF, turn_half(bot_b), hi)
    for p in range(NP):
        ref[p + 1, R0 - 1:R0, :] = comm.yr[rnd, 0, p]
        ref[p + 1, R0 + NY:R0 + NY + 1, :] = comm.yr[rnd, 1, p]


def neighbours(ref, zr, rnd, p, t):
    row = R0 + 8 * t
    lane = lane_iota() & LOW
    centre = ref[p + 1, row:row + 8, :]
    xm = ref[p, row:row + 8, :]
    xp = ref[p + 2, row:row + 8, :]
    ym = ref[p + 1, row - 1:row + 7, :]
    yp = ref[p + 1, row + 1:row + 9, :]
    zm = jnp.where(lane == 0, z_ghost_lo(zr, rnd, t, p), pltpu.roll(centre, 1, 1))
    zp = jnp.where(lane == LOW, z_ghost_hi(zr, rnd, t, p), pltpu.roll(centre, 127, 1))
    return centre, (xm, xp, ym, yp, zm, zp)


def zero_tiles(n):
    return tuple(jnp.zeros(TILE, F32) for _ in range(n))


def send_faces(comm, rnd, ref, zacc):
    pack_x_faces(comm, rnd, ref)
    for i, part in enumerate(zacc):
        comm.zs[rnd, i // 2, i % 2] = part
    for face in reversed(range(FACES)):
        comm.send(rnd, face)


def load_field(comm, rnd, raw, ref):
    def body(p, zacc):
        zacc = list(zacc)
        ref[p + 1, R0:R0 + NY, :] = jnp.concatenate([raw[p], raw[p + NP]], axis=1)
        for t in range(ROWS):
            z_pack_tile(ref[p + 1, own(t), :], t, p, zacc)
        store_plane_faces(comm, rnd, ref, p)
        return tuple(zacc)
    return lax.fori_loop(0, NP, body, zero_tiles(4))


def fill_ghost_conductivity(comm, gx_slab, gy_slab, gz_slab):
    px, py, pz = comm.pos
    half = NY // 2
    turn = 64 * lax.rem(pz, 2)
    lane = lane_iota(half)
    a, b = pltpu.roll(gx_slab[0:half, :], turn, 1), pltpu.roll(gx_slab[half:NY, :], turn, 1)
    x_face = jnp.where(lane < HALF, a, turn_half(b))
    for end in range(2):
        @pl.when(jnp.logical_not(comm.has[end]))
        def _():
            comm.xr[0, end] = x_face
    rows = pltpu.roll(gy_slab[...], turn, 1)
    y_face = jnp.where(lane_iota(NP) < HALF, rows[0:NP], turn_half(rows[NP:NX]))
    for end in range(2):
        @pl.when(jnp.logical_not(comm.has[2 + end]))
        def _():
            for p in range(NP):
                comm.yr[0, end, p] = y_face[one(p)]
    for end in range(2):
        @pl.when(jnp.logical_not(comm.has[4 + end]))
        def _():
            cols = pltpu.roll(gz_slab[...], 64 * lax.rem(py, 2), 1)
            blank = jnp.zeros((48, LANES), F32)
            square = jnp.concatenate([cols[0:NP], blank, cols[NP:NX], blank], axis=0)
            turned = square.T
            acc = [jnp.zeros(TILE, F32)] * 2
            low = lane_iota() & LOW
            for p in range(NP):
                for t in range(ROWS):
                    s = 4 * p + t % 4
                    at = s if end else s + LOW
                    w = pltpu.roll(turned[tile(t)], (at - p) % 128, 1)
                    acc[t // 4] = jnp.where(low == at % 64, w, acc[t // 4])
            comm.zr[0, end, 0], comm.zr[0, end, 1] = acc[0], acc[1]


def zero_ends(comm, rounds):
    for face in range(FACES):
        @pl.when(jnp.logical_not(comm.has[face]))
        def _():
            buf = (comm.xr, comm.yr, comm.zr)[face // 2]
            for rnd in rounds:
                buf[rnd, face % 2] = jnp.zeros(buf.shape[2:], F32)


def lanes_of(pos):
    return pl.ds(pl.multiple_of(lax.div(pos, 2) * LANES, LANES), LANES)


def start_up(comm, ins, raws, slabs, load_sem):
    k_hbm, g_hbm, f_hbm, u_hbm = ins
    px, py, pz = comm.pos
    loads = [pltpu.make_async_copy(k_hbm, raws[0], load_sem.at[0]),
             pltpu.make_async_copy(u_hbm, raws[1], load_sem.at[1])]
    x_row = jnp.where(comm.has[1], 0, 1)
    y_row = jnp.where(comm.has[3], 2, 3)
    z_row = jnp.where(comm.has[5], 4, 5)
    z_lanes = lanes_of(pz)
    y_lanes = lanes_of(py)
    loads.append(pltpu.make_async_copy(
        g_hbm.at[x_row, pl.ds(pl.multiple_of(py * NY, NY), NY), z_lanes], slabs[0], load_sem.at[2]))
    loads.append(pltpu.make_async_copy(
        g_hbm.at[y_row, pl.ds(pl.multiple_of(px * NX, NX), NX), z_lanes], slabs[1], load_sem.at[3]))
    loads.append(pltpu.make_async_copy(
        g_hbm.at[z_row, pl.ds(pl.multiple_of(px * NX, NX), NX), y_lanes], slabs[2], load_sem.at[4]))
    loads.append(pltpu.make_async_copy(f_hbm, raws[2], load_sem.at[5]))
    for load in loads:
        load.start()
    return loads


def first_exchange(comm, loads, greet, raws, slabs, k_ref, u_ref):
    sem, total = greet
    loads[0].wait()
    zacc = load_field(comm, 0, raws[0], k_ref)
    pl.semaphore_wait(sem, total)
    send_faces(comm, 0, k_ref, zacc)
    loads[1].wait()
    zacc = load_field(comm, 1, raws[1], u_ref)
    send_faces(comm, 1, u_ref, zacc)
    for load in loads[2:]:
        load.wait()
    fill_ghost_conductivity(comm, *slabs)
    for rnd, ref in ((0, k_ref), (1, u_ref)):
        for face in range(FACES):
            comm.wait_recv(rnd, face)
        unpack_xy(comm, rnd, ref)


def first_residual(comm, raw_f, k_ref, u_ref, p, t, scale, coef_ref, d_ref):
    own, others = neighbours(k_ref, comm.zr, 0, p, t)
    u_own, u_others = neighbours(u_ref, comm.zr, 1, p, t)
    twice = own + own
    weights = [twice * other / (own + other) for other in others]
    diag = total_of(weights)
    flux = [w * (u_own - other) for w, other in zip(weights, u_others)]
    au = total_of(flux)
    rows = tile(t)
    inv = 1.0 / diag
    f_tile = jnp.concatenate([raw_f[p, rows, :], raw_f[p + NP, rows, :]], axis=1)
    resid = f_tile - au
    factor = inv + inv if scale else None
    for i in range(FACES):
        coef_ref[i, p, rows, :] = weights[i] * factor if scale else weights[i]
    d_ref[p, rows, :] = diag
    return resid, inv


def write_plane(raw_ref, p, values):
    raw_ref[p] = values[:, :HALF]
    raw_ref[p + NP] = turn_half(values)[:, :HALF]


def dot_rows(a, b):
    prod = a[:2 * SUB] * b[:2 * SUB]
    return row_sum(prod[:SUB] + prod[SUB:])


def solve_coefficients(row, mom_ref, pc_ref, hist_ref, full_ref):
    lane24, line24 = lane_iota(24), row_iota(24)
    wide = jnp.broadcast_to(row, (24, LANES))
    base = lane_sum(jnp.where((lane24 == line24) & (lane24 < 17), wide, 0.0))
    base = jnp.broadcast_to(base, (24, LANES))
    first, second = base[0:1], base[1:2]
    even = (line24 & 1) == 0
    mom = jnp.where(line24 >= 2, 2.0 * base - jnp.where(even, first, second), base)
    mom = jnp.where(line24 < 17, mom, 0.0)
    lane16, line16 = lane_iota(16), row_iota(16)
    wide = jnp.broadcast_to(row, WIDE)
    for k in range(NB):
        big = jnp.maximum(line16, k)
        small = jnp.minimum(line16, k)
        want = 17 + lax.shift_right_logical(big * (big + 1), 1) + small
        col = lane_sum(jnp.where((lane16 == want) & (line16 < NB), wide, 0.0))
        full_ref[k] = jnp.broadcast_to(col, WIDE)
    zeros8 = jnp.zeros(TILE, F32)
    mom_ref[:SUB] = zeros8
    mom_ref[32:40] = zeros8
    pc_ref[:SUB] = zeros8
    pc_ref[24:32] = zeros8
    unit = jnp.where(line16 == 0, 1.0, 0.0)
    cvec, pvec, avec = unit, unit, jnp.zeros(WIDE, F32)
    rvec, mvec = mom, mom
    mu0 = mom[0:1]
    rho = dot_rows(cvec, rvec)
    ok = jnp.where(rho > 0.0, 1.0, 0.0)
    two_one = jnp.where(line16 == 1, 2.0, 1.0)
    for t in range(CG_ITERS):
        mom_ref[8:32] = mvec
        mom_ref[7:8] = mvec[1:2]
        pc_ref[8:24] = pvec
        qvec = mvec - 0.5 * (mom_ref[9:33] + mom_ref[7:31])
        npvec = 0.5 * (two_one * pc_ref[7:23] + pc_ref[9:25])
        curv = dot_rows(pvec, qvec)
        size = row_sum(jnp.abs(pvec))
        ok = jnp.where(size * size * mu0 < BOUND * curv, ok, 0.0)
        alpha = rho / curv
        avec = avec + alpha * pvec
        cvec = cvec - alpha * (pvec - npvec)
        rvec = rvec - alpha * qvec
        hist_ref[t] = cvec
        rho_new = dot_rows(cvec, rvec)
        size = row_sum(jnp.abs(cvec))
        ok = jnp.where(size * size * mu0 < BOUND * rho_new, ok, 0.0)
        beta = rho_new / rho
        pvec = cvec + beta * pvec
        mvec = rvec + beta * mvec
        rho = rho_new
    return avec, cvec, ok


def squares_row(hist_ref, full_ref, ok):
    lane = lane_iota(1)
    out = jnp.where(lane == 8, ok, 0.0)
    for t in range(CG_ITERS):
        cvec = hist_ref[t]
        acc = full_ref[0] * hist_ref[t, one(0)]
        for j in range(1, NB):
            acc = acc + full_ref[j] * hist_ref[t, one(j)]
        out = jnp.where(lane == t, dot_rows(acc, cvec), out)
    return out


def basis_kernel(counts, k_hbm, g_hbm, f_hbm, u_hbm, uo_hbm, ro_hbm, h_ref,
                 raw_k, raw_u, raw_f, slab_x, slab_y, slab_z, k_ref, u_ref, z_ref, coef_ref, d_ref, sums_ref,
                 mom_ref, pc_ref, hist_ref, full_ref, comb_ref,
                 xs, ys, zs, xr, yr, zr, send_row, rows_x, rows_y, rows_z,
                 load_sem, store_sem, send_sem, recv_sem, red_ss, red_rs):
    comm = Comm(counts, (xs, ys, zs, xr, yr, zr, send_sem, recv_sem))
    raws, slabs = (raw_k, raw_u, raw_f), (slab_x, slab_y, slab_z)
    loads = start_up(comm, (k_hbm, g_hbm, f_hbm, u_hbm), raws, slabs, load_sem)
    greet = barrier_all_lines(comm)
    zero_ends(comm, range(1, CG_ITERS + 2))
    sums_ref[...] = jnp.zeros(sums_ref.shape, F32)
    first_exchange(comm, loads, greet, raws, slabs, k_ref, u_ref)

    def first(p, zacc):
        zacc = list(zacc)
        for t in range(ROWS):
            resid, inv = first_residual(comm, raw_f, k_ref, u_ref, p, t, True, coef_ref, d_ref)
            z_new = resid * inv
            z_ref[0, p + 1, own(t), :] = z_new
            z_pack_tile(z_new, t, p, zacc)
        store_plane_faces(comm, 2, z_ref.at[0], p)
        return tuple(zacc)

    zacc = lax.fori_loop(0, NP, first, zero_tiles(4))
    send_faces(comm, 2, z_ref.at[0], zacc)

    def products(k):
        def body(p, accs):
            accs = list(accs)
            for t in range(ROWS):
                row = own(t)
                d = d_ref[p, tile(t), :]
                z_k = z_ref[k, p + 1, row, :]
                dz = d * z_k
                ddz = d * dz
                for i in range(k + 1):
                    z_i = z_ref[i, p + 1, row, :]
                    accs[i] = accs[i] + ddz * z_i
                    if i >= k - 1:
                        accs[k + 1 + (k - i)] = accs[k + 1 + (k - i)] + dz * z_i
            return tuple(accs)
        accs = lax.fori_loop(0, NP, body, zero_tiles(k + 2 + (1 if k else 0)))
        for i in range(k + 1):
            at = 17 + k * (k + 1) // 2 + i
            sums_ref[one(at)] = row_sum(accs[i])
        sums_ref[one(2 * k)] = row_sum(accs[k + 1])
        if k:
            sums_ref[one(2 * k - 1)] = row_sum(accs[k + 2])

    for k in range(CG_ITERS):
        rnd = 2 + k
        products(k)
        for face in range(FACES):
            comm.wait_recv(rnd, face)
        unpack_xy(comm, rnd, z_ref.at[k])
        last = k == CG_ITERS - 1

        def step(p, zacc):
            zacc = list(zacc)
            for t in range(ROWS):
                _, others = neighbours(z_ref.at[k], zr, rnd, p, t)
                rows = tile(t)
                terms = [coef_ref[i, p, rows, :] * others[i] for i in range(FACES)]
                total = total_of(terms)
                row = own(t)
                z_new = 0.5 * total if k == 0 else total - z_ref[k - 1, p + 1, row, :]
                z_ref[k + 1, p + 1, row, :] = z_new
                if not last:
                    z_pack_tile(z_new, t, p, zacc)
            if not last:
                store_plane_faces(comm, rnd + 1, z_ref.at[k + 1], p)
            return tuple(zacc)

        zacc = lax.fori_loop(0, NP, step, zero_tiles(4))
        if not last:
            send_faces(comm, rnd + 1, z_ref.at[k + 1], zacc)
    products(CG_ITERS)

    total = jnp.broadcast_to(lane_sum(sums_ref[...]), (NY, LANES))
    row = row_sum(jnp.where(lane_iota(64) == row_iota(64), total, 0.0))
    red = Reducer(comm, send_row, (rows_x, rows_y, rows_z), red_ss, red_rs)
    row = red.run(row)
    avec, cvec, ok = solve_coefficients(row, mom_ref, pc_ref, hist_ref, full_ref)
    comb_ref[0] = avec
    comb_ref[1] = cvec

    a_co = [jnp.broadcast_to(comb_ref[0, one(i)], TILE) for i in range(CG_ITERS)]
    c_co = [jnp.broadcast_to(comb_ref[1, one(i)], TILE) for i in range(NB)]

    def combine(p, carry):
        for t in range(ROWS):
            row = own(t)
            rows = tile(t)
            basis = [z_ref[i, p + 1, row, :] for i in range(NB)]
            ut, rt = a_co[0] * basis[0], c_co[0] * basis[0]
            for i in range(1, NB):
                if i < CG_ITERS:
                    ut = ut + a_co[i] * basis[i]
                rt = rt + c_co[i] * basis[i]
            ut = u_ref[p + 1, row, :] + ut
            rt = d_ref[p, rows, :] * rt
            raw_u[p, rows, :] = ut[:, :HALF]
            raw_u[p + NP, rows, :] = turn_half(ut)[:, :HALF]
            raw_f[p, rows, :] = rt[:, :HALF]
            raw_f[p + NP, rows, :] = turn_half(rt)[:, :HALF]
        return carry

    lax.fori_loop(0, NP, combine, 0)
    outs = [pltpu.make_async_copy(raw_u, uo_hbm, store_sem.at[0]), pltpu.make_async_copy(raw_f, ro_hbm, store_sem.at[1])]
    for out in outs:
        out.start()
    h_ref[...] = squares_row(hist_ref, full_ref, ok)
    for rnd in range(CG_ITERS + 2):
        for face in range(FACES):
            comm.wait_send(rnd, face)
    for out in outs:
        out.wait()


def plain_kernel(counts, k_hbm, g_hbm, f_hbm, u_hbm, uo_hbm, ro_hbm, h_ref,
                 raw_k, raw_u, raw_f, slab_x, slab_y, slab_z, k_ref, u_ref, p_ref, q_ref, r_ref, coef_ref, d_ref,
                 xs, ys, zs, xr, yr, zr, send_row, rows_x, rows_y, rows_z,
                 load_sem, store_sem, send_sem, recv_sem, red_ss, red_rs):
    comm = Comm(counts, (xs, ys, zs, xr, yr, zr, send_sem, recv_sem))
    raws, slabs = (raw_k, raw_u, raw_f), (slab_x, slab_y, slab_z)
    loads = start_up(comm, (k_hbm, g_hbm, f_hbm, u_hbm), raws, slabs, load_sem)
    greet = barrier_all_lines(comm)
    zero_ends(comm, range(1, 3))
    first_exchange(comm, loads, greet, raws, slabs, k_ref, u_ref)
    red = [Reducer(comm, send_row.at[i], (rows_x.at[i], rows_y.at[i], rows_z.at[i]), red_ss.at[i], red_rs.at[i]) for i in range(2)]

    def reduce(which, accs):
        lane = lane_iota(1)
        row = jnp.zeros((1, LANES), F32)
        for i, acc in enumerate(accs):
            total = row_sum(lane_sum(acc))
            row = jnp.where(lane == i, jnp.broadcast_to(total, (1, LANES)), row)
        row = red[which].run(row)
        return [lane_sum(jnp.where(lane == i, row, 0.0)) for i in range(len(accs))]

    def first(p, accs):
        acc = accs[0]
        for t in range(ROWS):
            resid, inv = first_residual(comm, raw_f, k_ref, u_ref, p, t, False, coef_ref, d_ref)
            rows = tile(t)
            r_ref[p, rows, :] = resid
            z_new = resid * inv
            p_ref[p + 1, own(t), :] = z_new
            acc = acc + resid * z_new
        return (acc,)

    rho, = reduce(0, lax.fori_loop(0, NP, first, zero_tiles(1)))

    def iteration(it, carry):
        rho, hist = carry

        def pack(p, zacc):
            zacc = list(zacc)
            for t in range(ROWS):
                z_pack_tile(p_ref[p + 1, own(t), :], t, p, zacc)
            store_plane_faces(comm, 2, p_ref, p)
            return tuple(zacc)

        send_faces(comm, 2, p_ref, lax.fori_loop(0, NP, pack, zero_tiles(4)))
        for face in range(FACES):
            comm.wait_recv(2, face)
            comm.wait_send(2, face)
        unpack_xy(comm, 2, p_ref)

        def apply(p, accs):
            acc = accs[0]
            for t in range(ROWS):
                own, others = neighbours(p_ref, zr, 2, p, t)
                rows = tile(t)
                flux = [coef_ref[i, p, rows, :] * (own - others[i]) for i in range(FACES)]
                q = total_of(flux)
                q_ref[p, rows, :] = q
                acc = acc + own * q
            return (acc,)

        curv, = reduce(1, lax.fori_loop(0, NP, apply, zero_tiles(1)))
        alpha = jnp.broadcast_to(rho / curv, TILE)

        def update(p, accs):
            acc_z, acc_r = accs
            for t in range(ROWS):
                row = own(t)
                rows = tile(t)
                u_ref[p + 1, row, :] = u_ref[p + 1, row, :] + alpha * p_ref[p + 1, row, :]
                resid = r_ref[p, rows, :] - alpha * q_ref[p, rows, :]
                r_ref[p, rows, :] = resid
                acc_z = acc_z + resid * (resid / d_ref[p, rows, :])
                acc_r = acc_r + resid * resid
            return acc_z, acc_r

        rho_new, rr = reduce(0, lax.fori_loop(0, NP, update, zero_tiles(2)))
        beta = jnp.broadcast_to(rho_new / rho, TILE)

        def turn(p, carry):
            for t in range(ROWS):
                row = own(t)
                rows = tile(t)
                p_ref[p + 1, row, :] = r_ref[p, rows, :] / d_ref[p, rows, :] + beta * p_ref[p + 1, row, :]
            return carry

        lax.fori_loop(0, NP, turn, 0)
        hist = jnp.where(lane_iota(1) == it, jnp.broadcast_to(rr, (1, LANES)), hist)
        return rho_new, hist

    _, hist = lax.fori_loop(0, CG_ITERS, iteration, (rho, jnp.zeros((1, LANES), F32)))
    h_ref[...] = hist

    def finish(p, carry):
        write_plane(raw_u, p, u_ref[p + 1, R0:R0 + NY, :])
        write_plane(raw_f, p, r_ref[p])
        return carry

    lax.fori_loop(0, NP, finish, 0)
    outs = [pltpu.make_async_copy(raw_u, uo_hbm, store_sem.at[0]), pltpu.make_async_copy(raw_f, ro_hbm, store_sem.at[1])]
    for out in outs:
        out.start()
    for rnd in range(2):
        for face in range(FACES):
            comm.wait_send(rnd, face)
    for out in outs:
        out.wait()


def scratch_for(kind, counts):
    field = (NP + 2, NY + 16, LANES)
    block = (NP, NY, LANES)
    vm = lambda *shape: pltpu.VMEM(shape, F32)
    raws = [vm(NX, NY, NZ)] * 3 + [vm(NY, LANES), vm(NX, LANES), vm(NX, LANES)]
    if kind == 'basis':
        rounds, reds = CG_ITERS + 2, ()
        work = [vm(*field), vm(*field), vm(NB, *field), vm(6, *block), vm(*block), vm(NY, LANES),
                vm(40, LANES), vm(32, LANES), vm(CG_ITERS, 16, LANES), vm(NB, 16, LANES), vm(2, 16, LANES)]
    else:
        rounds, reds = 3, (2,)
        work = [vm(*field), vm(*field), vm(*field), vm(*block), vm(*block), vm(6, *block), vm(*block)]
    faces = [vm(rounds, 2, NY // 2, LANES), vm(rounds, 2, NP, 1, LANES), vm(rounds, 2, 2, 8, LANES)] * 2
    rows = [vm(*reds, 3, 1, LANES)] + [vm(*reds, n, 1, LANES) for n in counts]
    dma = pltpu.SemaphoreType.DMA
    sems = [dma((6,)), dma((2,)), dma((rounds, 6)), dma((rounds, 6)), dma((*reds, 3, 8)), dma((*reds, 3, 8))]
    return raws + work + faces + rows + sems


def solution(mesh):
    counts = tuple(mesh.shape[name] for name in AXES)
    grid_spec = P(*AXES)
    block = jax.ShapeDtypeStruct((NX, NY, NZ), F32)

    def call(kernel, kind, ident):
        hbm = pl.BlockSpec(memory_space=pl.ANY)
        return pl.pallas_call(
            functools.partial(kernel, counts),
            out_shape=(block, block, jax.ShapeDtypeStruct((1, LANES), F32)),
            in_specs=[hbm] * 4,
            out_specs=(hbm, hbm, pl.BlockSpec(memory_space=pltpu.VMEM)),
            scratch_shapes=scratch_for(kind, counts),
            compiler_params=pltpu.CompilerParams(collective_id=ident, has_side_effects=True),
            name=kind,
        )

    def local_solve(k_cell, k_ghost, f_rhs, u_init):
        args = (k_cell, k_ghost, f_rhs, u_init)
        u_out, r_out, row = call(basis_kernel, 'basis', 0)(*args)
        u_out, r_out, row = lax.cond(
            row[0, 8] > 0.5,
            lambda: (u_out, r_out, row),
            lambda: tuple(call(plain_kernel, 'plain', 1)(*args)))
        return u_out, r_out, row[0, 0:CG_ITERS]

    return jax.shard_map(local_solve, mesh=mesh, in_specs=(grid_spec, P(), grid_spec, grid_spec),
                         out_specs=(grid_spec, grid_spec, P()), check_vma=False)
```

```python
import functools

import jax
import jax.numpy as jnp
from jax import lax
from jax.experimental import pallas as pl
from jax.experimental.pallas import tpu as pltpu
from jax.sharding import PartitionSpec as P

CG_ITERS = 8
NB = CG_ITERS + 1
NX, NY, NZ = 32, 64, 64
NP = NX // 2
R0 = 8
MESH = pl.DeviceIdType.MESH
AXES = ('gx', 'gy', 'gz')
BOUND = 4096.0
F32 = jnp.float32
SUB, LANES, HALF, LOW = 8, 128, 64, 63
ROWS = NY // SUB
TILE = (SUB, LANES)
WIDE = (2 * SUB, LANES)
FACES = 6
FOLD = NY // 2
TURNS = (4, 8, 16, 32)


def own(t):
    return slice(R0 + SUB * t, R0 + SUB * t + SUB)


def tile(t):
    return slice(SUB * t, SUB * t + SUB)


def one(i):
    return slice(i, i + 1)


def spin(values, by):
    return pltpu.roll(values, by, 1)


def turn_half(values):
    return spin(values, HALF)


def row_sum(values):
    return jnp.sum(values, axis=0, keepdims=True)


def lane_sum(values):
    return jnp.sum(values, axis=1, keepdims=True)


def total_of(parts):
    parts = list(parts)
    while len(parts) > 1:
        parts = [sum(parts[i + 1:i + 2], parts[i]) for i in range(0, len(parts), 2)]
    return parts[0]


def lane_iota(rows=8):
    return lax.broadcasted_iota(jnp.int32, (rows, LANES), 1)


def row_iota(rows):
    return lax.broadcasted_iota(jnp.int32, (rows, LANES), 0)


class Comm:
    def __init__(self, counts, bufs):
        self.counts = counts
        self.pos = [lax.axis_index(name) for name in AXES]
        self.has = []
        for axis in range(3):
            self.has.append(self.pos[axis] > 0)
            self.has.append(self.pos[axis] < counts[axis] - 1)
        (self.xs, self.ys, self.zs, self.xr, self.yr, self.zr, self.send_sem, self.recv_sem) = bufs

    def source(self, rnd, face):
        axis, high = face // 2, face % 2
        return self.zs.at[rnd] if axis == 2 else (self.xs, self.ys)[axis].at[rnd, high]

    def copies(self, rnd, face):
        axis, high = face // 2, face % 2
        src = self.source(rnd, face)
        dst = (self.xr, self.yr, self.zr)[axis]
        step = 1 if high else -1
        return pltpu.make_async_remote_copy(
            src_ref=src, dst_ref=dst.at[rnd, 1 - high],
            send_sem=self.send_sem.at[rnd, face], recv_sem=self.recv_sem.at[rnd, face ^ 1],
            device_id={AXES[axis]: self.pos[axis] + step}, device_id_type=MESH)

    def send(self, rnd, face):
        @pl.when(self.has[face])
        def _():
            self.copies(rnd, face).start()

    def wait_recv(self, rnd, face):
        axis, high = face // 2, face % 2
        src = self.source(rnd, face)
        dst = (self.xr, self.yr, self.zr)[axis]
        step = 1 if high else -1

        @pl.when(self.has[face])
        def _():
            pltpu.make_async_remote_copy(
                src_ref=src, dst_ref=dst.at[rnd, high],
                send_sem=self.send_sem.at[rnd, face], recv_sem=self.recv_sem.at[rnd, face],
                device_id={AXES[axis]: self.pos[axis] + step}, device_id_type=MESH).wait_recv()

    def wait_send(self, rnd, face):
        @pl.when(self.has[face])
        def _():
            self.copies(rnd, face).wait_send()


def barrier_all_lines(comm):
    sem = pltpu.get_barrier_semaphore()
    total = 0
    for axis in range(3):
        n = comm.counts[axis]
        for off in range(1, n):
            pl.semaphore_signal(sem, inc=1, device_id={AXES[axis]: lax.rem(comm.pos[axis] + off, n)}, device_id_type=MESH)
            total += 1
    return sem, total


class Reducer:
    def __init__(self, comm, send_row, recv_rows, send_sem, recv_sem):
        self.comm, self.send_row, self.recv_rows, self.ss, self.rs = comm, send_row, recv_rows, send_sem, recv_sem

    def copy(self, axis, off):
        n, me = self.comm.counts[axis], self.comm.pos[axis]
        return pltpu.make_async_remote_copy(
            src_ref=self.send_row.at[axis], dst_ref=self.recv_rows[axis].at[me],
            send_sem=self.ss.at[axis, off], recv_sem=self.rs.at[axis, off],
            device_id={AXES[axis]: lax.rem(me + off, n)}, device_id_type=MESH)

    def run(self, row):
        for axis in range(3):
            n, me = self.comm.counts[axis], self.comm.pos[axis]
            rows = self.recv_rows[axis]
            self.send_row[axis] = row
            rows[me] = row
            for off in range(1, n):
                self.copy(axis, off).start()
            for off in range(1, n):
                self.copy(axis, off).wait()
            parts = [rows[i] for i in range(n)]
            row = total_of(parts)
        return row


def store_plane_faces(comm, rnd, ref, p):
    comm.ys[rnd, 0, p] = ref[p + 1, R0:R0 + 1, :]
    comm.ys[rnd, 1, p] = ref[p + 1, R0 + NY - 1:R0 + NY, :]


def pack_x_faces(comm, rnd, ref):
    half = FOLD
    lane = lane_iota(half)
    a, b = ref[1, R0:R0 + half, :], ref[1, R0 + half:R0 + NY, :]
    comm.xs[rnd, 0] = jnp.where(lane < HALF, a, turn_half(b))
    a, b = ref[NP, R0:R0 + half, :], ref[NP, R0 + half:R0 + NY, :]
    comm.xs[rnd, 1] = jnp.where(lane < HALF, turn_half(a), b)


def face_mask(turn):
    return ((lane_iota(FOLD) + 1) & LOW) < turn


def pack_z(comm, rnd, ref, tree):
    def fold(p, carry):
        low, high = ref[p + 1, R0:R0 + FOLD, :], ref[p + 1, R0 + FOLD:R0 + NY, :]
        tree[p] = jnp.where(face_mask(2), low, spin(high, 2))
        return carry
    lax.fori_loop(0, NP, fold, 0, unroll=8)
    parts = [tree[p] for p in range(NP)]
    for turn in TURNS:
        parts = [jnp.where(face_mask(turn), parts[i], spin(parts[i + 1], turn)) for i in range(0, len(parts), 2)]
    comm.zs[rnd] = parts[0]


def unpack_z(comm, rnd, tree):
    odd = (lane_iota(FOLD) & 1) == 1
    parts = [jnp.where(odd, spin(comm.zr[rnd, 1], LOW), spin(comm.zr[rnd, 0], HALF + 1))]
    for turn in reversed(TURNS):
        parts = [q for part in parts for q in (part, spin(part, LANES - turn))]
    for p in range(NP):
        tree[p] = parts[p]


def spread_z(comm, rnd, tree, ghost):
    unpack_z(comm, rnd, tree)

    def fold(p, carry):
        ghost[p, 0:FOLD, :] = tree[p]
        ghost[p, FOLD:NY, :] = spin(tree[p], LANES - 2)
        return carry
    lax.fori_loop(0, NP, fold, 0, unroll=8)


def inner_planes(ref):
    low = lane_iota(NY) < HALF
    ref[0, R0:R0 + NY, :] = jnp.where(low, 0.0, turn_half(ref[NP, R0:R0 + NY, :]))
    ref[NP + 1, R0:R0 + NY, :] = jnp.where(low, turn_half(ref[1, R0:R0 + NY, :]), 0.0)


def x_ghosts(comm, rnd):
    low = lane_iota(FOLD) < HALF
    lo, hi = comm.xr[rnd, 0], comm.xr[rnd, 1]
    below = [jnp.where(low, lo, 0.0), jnp.where(low, turn_half(lo), 0.0)]
    above = [jnp.where(low, 0.0, turn_half(hi)), jnp.where(low, 0.0, hi)]
    return below, above


def outer_layers(comm, rnd, ref):
    inner_planes(ref)
    below, above = x_ghosts(comm, rnd)
    for i in range(2):
        rows = slice(R0 + FOLD * i, R0 + FOLD * i + FOLD)
        ref[0, rows, :] = ref[0, rows, :] + below[i]
        ref[NP + 1, rows, :] = ref[NP + 1, rows, :] + above[i]
    for p in range(NP):
        ref[p + 1, R0 - 1:R0, :] = comm.yr[rnd, 0, p]
        ref[p + 1, R0 + NY:R0 + NY + 1, :] = comm.yr[rnd, 1, p]


def blank_rows(ref):
    for p in range(NP):
        ref[p + 1, R0 - 1:R0, :] = jnp.zeros((1, LANES), F32)
        ref[p + 1, R0 + NY:R0 + NY + 1, :] = jnp.zeros((1, LANES), F32)


def neighbours(ref, p, t, ghost=None):
    row = R0 + SUB * t
    lane = lane_iota() & LOW
    centre = ref[p + 1, own(t), :]
    xm = ref[p, own(t), :]
    xp = ref[p + 2, own(t), :]
    ym = ref[p + 1, row - 1:row + SUB - 1, :]
    yp = ref[p + 1, row + 1:row + SUB + 1, :]
    zm, zp = spin(centre, 1), spin(centre, LANES - 1)
    if ghost is not None:
        edge = ghost[p, tile(t), :]
        zm, zp = jnp.where(lane == 0, edge, zm), jnp.where(lane == LOW, edge, zp)
    return centre, (xm, xp, ym, yp, zm, zp)


def sweep(body, state=(), unroll=2):
    def plane(p, carry):
        carry = list(carry)
        body(p, carry)
        return tuple(carry)
    return lax.fori_loop(0, NP, plane, tuple(state), unroll=unroll)


def zero_tiles(n):
    return tuple(jnp.zeros(TILE, F32) for _ in range(n))


def send_faces(comm, rnd, ref, tree):
    pack_z(comm, rnd, ref, tree)
    for face in (4, 5):
        comm.send(rnd, face)
    pack_x_faces(comm, rnd, ref)
    for p in range(NP):
        store_plane_faces(comm, rnd, ref, p)
    for face in range(4):
        comm.send(rnd, face)


def load_field(raw, ref):
    def body(p, state):
        ref[p + 1, R0:R0 + NY, :] = jnp.concatenate([raw[p], raw[p + NP]], axis=1)
    sweep(body, unroll=4)


def fill_ghost_conductivity(comm, square, gx_slab, gy_slab, gz_slab):
    px, py, pz = comm.pos
    half = FOLD
    turn = 64 * lax.rem(pz, 2)
    lane = lane_iota(half)
    a, b = pltpu.roll(gx_slab[0:half, :], turn, 1), pltpu.roll(gx_slab[half:NY, :], turn, 1)
    x_face = jnp.where(lane < HALF, a, turn_half(b))
    for end in range(2):
        @pl.when(jnp.logical_not(comm.has[end]))
        def _():
            comm.xr[0, end] = x_face
    rows = pltpu.roll(gy_slab[...], turn, 1)
    y_face = jnp.where(lane_iota(NP) < HALF, rows[0:NP], turn_half(rows[NP:NX]))
    for end in range(2):
        @pl.when(jnp.logical_not(comm.has[2 + end]))
        def _():
            for p in range(NP):
                comm.yr[0, end, p] = y_face[one(p)]
    for end in range(2):
        @pl.when(jnp.logical_not(comm.has[4 + end]))
        def _():
            cols = spin(gz_slab[...], HALF * lax.rem(py, 2))
            shift = 0 if end else LOW
            square[...] = jnp.zeros(square.shape, F32)
            for x in range(NX):
                for c in range(2):
                    square[one((4 * (x % NP) + 2 * c + HALF * (x // NP) + shift) % LANES)] = cols[one(x)]
            turned = square[...].T
            second = ((lane_iota(FOLD) - shift) & 3) == 2
            comm.zr[0, end] = jnp.where(second, turned[FOLD:NY], turned[:FOLD])


def zero_ends(comm, rounds):
    for face in range(FACES):
        @pl.when(jnp.logical_not(comm.has[face]))
        def _():
            buf = (comm.xr, comm.yr, comm.zr)[face // 2]
            for rnd in rounds:
                buf[rnd, face % 2] = jnp.zeros(buf.shape[2:], F32)


def lanes_of(pos):
    return pl.ds(pl.multiple_of(lax.div(pos, 2) * LANES, LANES), LANES)


def start_up(comm, ins, raws, slabs, load_sem):
    k_hbm, g_hbm, f_hbm, u_hbm = ins
    px, py, pz = comm.pos
    loads = [pltpu.make_async_copy(k_hbm, raws[0], load_sem.at[0]),
             pltpu.make_async_copy(u_hbm, raws[1], load_sem.at[1])]
    x_row = jnp.where(comm.has[1], 0, 1)
    y_row = jnp.where(comm.has[3], 2, 3)
    z_row = jnp.where(comm.has[5], 4, 5)
    z_lanes = lanes_of(pz)
    y_lanes = lanes_of(py)
    loads.append(pltpu.make_async_copy(
        g_hbm.at[x_row, pl.ds(pl.multiple_of(py * NY, NY), NY), z_lanes], slabs[0], load_sem.at[2]))
    loads.append(pltpu.make_async_copy(
        g_hbm.at[y_row, pl.ds(pl.multiple_of(px * NX, NX), NX), z_lanes], slabs[1], load_sem.at[3]))
    loads.append(pltpu.make_async_copy(
        g_hbm.at[z_row, pl.ds(pl.multiple_of(px * NX, NX), NX), y_lanes], slabs[2], load_sem.at[4]))
    loads.append(pltpu.make_async_copy(f_hbm, raws[2], load_sem.at[5]))
    for load in loads:
        load.start()
    return loads


def first_exchange(comm, loads, greet, raws, slabs, k_ref, u_ref, tree, square, k_ghost, u_ghost):
    sem, total = greet
    loads[0].wait()
    load_field(raws[0], k_ref)
    pl.semaphore_wait(sem, total)
    send_faces(comm, 0, k_ref, tree)
    loads[1].wait()
    load_field(raws[1], u_ref)
    send_faces(comm, 1, u_ref, tree)
    for load in loads[2:]:
        load.wait()
    fill_ghost_conductivity(comm, square, *slabs)
    for rnd, ref, ghost in ((0, k_ref, k_ghost), (1, u_ref, u_ghost)):
        for face in range(FACES):
            comm.wait_recv(rnd, face)
        outer_layers(comm, rnd, ref)
        spread_z(comm, rnd, tree, ghost)


def first_residual(raw_f, k_ref, u_ref, k_ghost, u_ghost, p, t, d_ref):
    centre, others = neighbours(k_ref, p, t, k_ghost)
    u_own, u_others = neighbours(u_ref, p, t, u_ghost)
    twice = centre + centre
    weights = [twice * other / (centre + other) for other in others]
    diag = total_of(weights)
    au = total_of([w * (u_own - other) for w, other in zip(weights, u_others)])
    f_tile = jnp.concatenate([raw_f[p, tile(t), :], raw_f[p + NP, tile(t), :]], axis=1)
    d_ref[p, tile(t), :] = diag
    return weights, f_tile - au, 1.0 / diag


def write_plane(raw_ref, p, values):
    raw_ref[p] = values[:, :HALF]
    raw_ref[p + NP] = turn_half(values)[:, :HALF]


def dot_rows(a, b):
    prod = a[:2 * SUB] * b[:2 * SUB]
    return row_sum(prod[:SUB] + prod[SUB:])


def solve_coefficients(row, mom_ref, pc_ref, hist_ref, full_ref):
    lane24, line24 = lane_iota(24), row_iota(24)
    wide = jnp.broadcast_to(row, (24, LANES))
    base = lane_sum(jnp.where((lane24 == line24) & (lane24 < 17), wide, 0.0))
    base = jnp.broadcast_to(base, (24, LANES))
    first, second = base[0:1], base[1:2]
    even = (line24 & 1) == 0
    mom = jnp.where(line24 >= 2, 2.0 * base - jnp.where(even, first, second), base)
    mom = jnp.where(line24 < 17, mom, 0.0)
    lane16, line16 = lane_iota(16), row_iota(16)
    wide = jnp.broadcast_to(row, WIDE)
    for k in range(NB):
        big = jnp.maximum(line16, k)
        small = jnp.minimum(line16, k)
        want = 17 + lax.shift_right_logical(big * (big + 1), 1) + small
        col = lane_sum(jnp.where((lane16 == want) & (line16 < NB), wide, 0.0))
        full_ref[k] = jnp.broadcast_to(col, WIDE)
    zeros8 = jnp.zeros(TILE, F32)
    mom_ref[:SUB] = zeros8
    mom_ref[32:40] = zeros8
    pc_ref[:SUB] = zeros8
    pc_ref[24:32] = zeros8
    unit = jnp.where(line16 == 0, 1.0, 0.0)
    cvec, pvec, avec = unit, unit, jnp.zeros(WIDE, F32)
    rvec, mvec = mom, mom
    mu0 = mom[0:1]
    rho = dot_rows(cvec, rvec)
    ok = jnp.where(rho > 0.0, 1.0, 0.0)
    two_one = jnp.where(line16 == 1, 2.0, 1.0)
    for t in range(CG_ITERS):
        mom_ref[8:32] = mvec
        mom_ref[7:8] = mvec[1:2]
        pc_ref[8:24] = pvec
        qvec = mvec - 0.5 * (mom_ref[9:33] + mom_ref[7:31])
        npvec = 0.5 * (two_one * pc_ref[7:23] + pc_ref[9:25])
        curv = dot_rows(pvec, qvec)
        size = row_sum(jnp.abs(pvec))
        ok = jnp.where(size * size * mu0 < BOUND * curv, ok, 0.0)
        alpha = rho / curv
        avec = avec + alpha * pvec
        cvec = cvec - alpha * (pvec - npvec)
        rvec = rvec - alpha * qvec
        hist_ref[t] = cvec
        rho_new = dot_rows(cvec, rvec)
        size = row_sum(jnp.abs(cvec))
        ok = jnp.where(size * size * mu0 < BOUND * rho_new, ok, 0.0)
        beta = rho_new / rho
        pvec = cvec + beta * pvec
        mvec = rvec + beta * mvec
        rho = rho_new
    return avec, cvec, ok


def squares_row(hist_ref, full_ref, ok):
    lane = lane_iota(1)
    out = jnp.where(lane == 8, ok, 0.0)
    for t in range(CG_ITERS):
        cvec = hist_ref[t]
        acc = full_ref[0] * hist_ref[t, one(0)]
        for j in range(1, NB):
            acc = acc + full_ref[j] * hist_ref[t, one(j)]
        out = jnp.where(lane == t, dot_rows(acc, cvec), out)
    return out


def basis_kernel(counts, k_hbm, g_hbm, f_hbm, u_hbm, uo_hbm, ro_hbm, h_ref,
                 raw_k, raw_u, raw_f, slab_x, slab_y, slab_z, k_ref, u_ref, z_ref, coef_ref, d_ref, sums_ref,
                 mom_ref, pc_ref, hist_ref, full_ref, comb_ref, edge_ref, tree, square, k_ghost, u_ghost,
                 xs, ys, zs, xr, yr, zr, send_row, rows_x, rows_y, rows_z,
                 load_sem, store_sem, send_sem, recv_sem, red_ss, red_rs):
    comm = Comm(counts, (xs, ys, zs, xr, yr, zr, send_sem, recv_sem))
    raws, slabs = (raw_k, raw_u, raw_f), (slab_x, slab_y, slab_z)
    loads = start_up(comm, (k_hbm, g_hbm, f_hbm, u_hbm), raws, slabs, load_sem)
    greet = barrier_all_lines(comm)
    zero_ends(comm, range(1, CG_ITERS + 2))
    sums_ref[...] = jnp.zeros(sums_ref.shape, F32)
    for k in range(CG_ITERS):
        blank_rows(z_ref.at[k])
    first_exchange(comm, loads, greet, raws, slabs, k_ref, u_ref, tree, square, k_ghost, u_ghost)

    def first(p, state):
        lane = lane_iota() & LOW
        for t in range(ROWS):
            weights, resid, inv = first_residual(raw_f, k_ref, u_ref, k_ghost, u_ghost, p, t, d_ref)
            factor = inv + inv
            scaled = [w * factor for w in weights]
            low, high = scaled[4:]
            edge_ref[p, tile(t), :] = jnp.where(lane == 0, low, jnp.where(lane == LOW, high, 0.0))
            scaled[4:] = jnp.where(lane == 0, 0.0, low), jnp.where(lane == LOW, 0.0, high)
            for i in range(FACES):
                coef_ref[p, t, i] = scaled[i]
            z_ref[0, p + 1, own(t), :] = resid * inv

    sweep(first)
    send_faces(comm, 2, z_ref.at[0], tree)

    def products(k):
        def body(p, accs):
            accs = list(accs)
            for t in range(ROWS):
                row = own(t)
                d = d_ref[p, tile(t), :]
                z_k = z_ref[k, p + 1, row, :]
                dz = d * z_k
                ddz = d * dz
                for i in range(k + 1):
                    z_i = z_ref[i, p + 1, row, :]
                    accs[i] = accs[i] + ddz * z_i
                    if i >= k - 1:
                        accs[k + 1 + (k - i)] = accs[k + 1 + (k - i)] + dz * z_i
            return tuple(accs)
        accs = lax.fori_loop(0, NP, body, zero_tiles(k + 2 + (1 if k else 0)))
        for i in range(k + 1):
            at = 17 + k * (k + 1) // 2 + i
            sums_ref[one(at)] = row_sum(accs[i])
        sums_ref[one(2 * k)] = row_sum(accs[k + 1])
        if k:
            sums_ref[one(2 * k - 1)] = row_sum(accs[k + 2])

    def late_terms(k, rnd):
        ref = z_ref.at[k + 1]
        weigh = (lambda term: 0.5 * term) if k == 0 else (lambda term: term)
        unpack_z(comm, rnd, tree)
        below, above = x_ghosts(comm, rnd)
        for t in range(ROWS):
            part = slice(SUB * (t % 4), SUB * (t % 4) + SUB)
            for plane, face, layer in ((1, 0, below), (NP, 1, above)):
                term = coef_ref[plane - 1, t, face] * layer[t // 4][part]
                ref[plane, own(t), :] = ref[plane, own(t), :] + weigh(term)

        def body(p, state):
            for end, t, sub in ((0, 0, 0), (1, ROWS - 1, SUB - 1)):
                row = R0 + SUB * t + sub
                term = coef_ref[p, t, 2 + end, one(sub), :] * comm.yr[rnd, end, p]
                ref[p + 1, one(row), :] = ref[p + 1, one(row), :] + weigh(term)
            for i in range(2):
                rows = slice(R0 + FOLD * i, R0 + FOLD * i + FOLD)
                ghost = spin(tree[p], LANES - 2) if i else tree[p]
                term = edge_ref[p, FOLD * i:FOLD * i + FOLD, :] * ghost
                ref[p + 1, rows, :] = ref[p + 1, rows, :] + weigh(term)
        sweep(body, unroll=4)

    for k in range(CG_ITERS):
        rnd = 2 + k
        inner_planes(z_ref.at[k])

        def step(p, state):
            for t in range(ROWS):
                _, others = neighbours(z_ref.at[k], p, t)
                total = total_of(coef_ref[p, t, i] * others[i] for i in range(FACES))
                z_new = 0.5 * total if k == 0 else total - z_ref[k - 1, p + 1, own(t), :]
                z_ref[k + 1, p + 1, own(t), :] = z_new

        sweep(step)
        products(k)
        for face in range(FACES):
            comm.wait_recv(rnd, face)
        late_terms(k, rnd)
        if k < CG_ITERS - 1:
            send_faces(comm, rnd + 1, z_ref.at[k + 1], tree)
    products(CG_ITERS)

    total = jnp.broadcast_to(lane_sum(sums_ref[...]), (NY, LANES))
    row = row_sum(jnp.where(lane_iota(64) == row_iota(64), total, 0.0))
    red = Reducer(comm, send_row, (rows_x, rows_y, rows_z), red_ss, red_rs)
    row = red.run(row)
    avec, cvec, ok = solve_coefficients(row, mom_ref, pc_ref, hist_ref, full_ref)
    comb_ref[0] = avec
    comb_ref[1] = cvec

    a_co = [jnp.broadcast_to(comb_ref[0, one(i)], TILE) for i in range(CG_ITERS)]
    c_co = [jnp.broadcast_to(comb_ref[1, one(i)], TILE) for i in range(NB)]

    def combine(p, carry):
        for t in range(ROWS):
            row = own(t)
            rows = tile(t)
            basis = [z_ref[i, p + 1, row, :] for i in range(NB)]
            ut, rt = a_co[0] * basis[0], c_co[0] * basis[0]
            for i in range(1, NB):
                if i < CG_ITERS:
                    ut = ut + a_co[i] * basis[i]
                rt = rt + c_co[i] * basis[i]
            ut = u_ref[p + 1, row, :] + ut
            rt = d_ref[p, rows, :] * rt
            raw_u[p, rows, :] = ut[:, :HALF]
            raw_u[p + NP, rows, :] = turn_half(ut)[:, :HALF]
            raw_f[p, rows, :] = rt[:, :HALF]
            raw_f[p + NP, rows, :] = turn_half(rt)[:, :HALF]
        return carry

    lax.fori_loop(0, NP, combine, 0)
    outs = [pltpu.make_async_copy(raw_u, uo_hbm, store_sem.at[0]), pltpu.make_async_copy(raw_f, ro_hbm, store_sem.at[1])]
    for out in outs:
        out.start()
    h_ref[...] = squares_row(hist_ref, full_ref, ok)
    for rnd in range(CG_ITERS + 2):
        for face in range(FACES):
            comm.wait_send(rnd, face)
    for out in outs:
        out.wait()


def plain_kernel(counts, k_hbm, g_hbm, f_hbm, u_hbm, uo_hbm, ro_hbm, h_ref,
                 raw_k, raw_u, raw_f, slab_x, slab_y, slab_z, k_ref, u_ref, p_ref, q_ref, r_ref, coef_ref, d_ref, tree, square, k_ghost, u_ghost,
                 xs, ys, zs, xr, yr, zr, send_row, rows_x, rows_y, rows_z,
                 load_sem, store_sem, send_sem, recv_sem, red_ss, red_rs):
    comm = Comm(counts, (xs, ys, zs, xr, yr, zr, send_sem, recv_sem))
    raws, slabs = (raw_k, raw_u, raw_f), (slab_x, slab_y, slab_z)
    loads = start_up(comm, (k_hbm, g_hbm, f_hbm, u_hbm), raws, slabs, load_sem)
    greet = barrier_all_lines(comm)
    zero_ends(comm, range(1, 3))
    first_exchange(comm, loads, greet, raws, slabs, k_ref, u_ref, tree, square, k_ghost, u_ghost)
    red = [Reducer(comm, send_row.at[i], (rows_x.at[i], rows_y.at[i], rows_z.at[i]), red_ss.at[i], red_rs.at[i]) for i in range(2)]

    def reduce(which, accs):
        lane = lane_iota(1)
        row = jnp.zeros((1, LANES), F32)
        for i, acc in enumerate(accs):
            total = row_sum(lane_sum(acc))
            row = jnp.where(lane == i, jnp.broadcast_to(total, (1, LANES)), row)
        row = red[which].run(row)
        return [lane_sum(jnp.where(lane == i, row, 0.0)) for i in range(len(accs))]

    def first(p, state):
        for t in range(ROWS):
            weights, resid, inv = first_residual(raw_f, k_ref, u_ref, k_ghost, u_ghost, p, t, d_ref)
            for i in range(FACES):
                coef_ref[p, t, i] = weights[i]
            r_ref[p, tile(t), :] = resid
            z_new = resid * inv
            p_ref[p + 1, own(t), :] = z_new
            state[0] = state[0] + resid * z_new

    rho, = reduce(0, sweep(first, zero_tiles(1)))

    def iteration(it, carry):
        rho, hist = carry

        send_faces(comm, 2, p_ref, tree)
        for face in range(FACES):
            comm.wait_recv(2, face)
            comm.wait_send(2, face)
        outer_layers(comm, 2, p_ref)
        spread_z(comm, 2, tree, k_ghost)

        def apply(p, state):
            for t in range(ROWS):
                centre, others = neighbours(p_ref, p, t, k_ghost)
                q = total_of(coef_ref[p, t, i] * (centre - others[i]) for i in range(FACES))
                q_ref[p, tile(t), :] = q
                state[0] = state[0] + centre * q

        curv, = reduce(1, sweep(apply, zero_tiles(1)))
        alpha = jnp.broadcast_to(rho / curv, TILE)

        def update(p, accs):
            acc_z, acc_r = accs
            for t in range(ROWS):
                row = own(t)
                rows = tile(t)
                u_ref[p + 1, row, :] = u_ref[p + 1, row, :] + alpha * p_ref[p + 1, row, :]
                resid = r_ref[p, rows, :] - alpha * q_ref[p, rows, :]
                r_ref[p, rows, :] = resid
                acc_z = acc_z + resid * (resid / d_ref[p, rows, :])
                acc_r = acc_r + resid * resid
            return acc_z, acc_r

        rho_new, rr = reduce(0, lax.fori_loop(0, NP, update, zero_tiles(2)))
        beta = jnp.broadcast_to(rho_new / rho, TILE)

        def turn(p, carry):
            for t in range(ROWS):
                row = own(t)
                rows = tile(t)
                p_ref[p + 1, row, :] = r_ref[p, rows, :] / d_ref[p, rows, :] + beta * p_ref[p + 1, row, :]
            return carry

        lax.fori_loop(0, NP, turn, 0)
        hist = jnp.where(lane_iota(1) == it, jnp.broadcast_to(rr, (1, LANES)), hist)
        return rho_new, hist

    _, hist = lax.fori_loop(0, CG_ITERS, iteration, (rho, jnp.zeros((1, LANES), F32)))
    h_ref[...] = hist

    def finish(p, carry):
        write_plane(raw_u, p, u_ref[p + 1, R0:R0 + NY, :])
        write_plane(raw_f, p, r_ref[p])
        return carry

    lax.fori_loop(0, NP, finish, 0)
    outs = [pltpu.make_async_copy(raw_u, uo_hbm, store_sem.at[0]), pltpu.make_async_copy(raw_f, ro_hbm, store_sem.at[1])]
    for out in outs:
        out.start()
    for rnd in range(2):
        for face in range(FACES):
            comm.wait_send(rnd, face)
    for out in outs:
        out.wait()


def scratch_for(kind, counts):
    field = (NP + 2, NY + 16, LANES)
    block = (NP, NY, LANES)
    vm = lambda *shape: pltpu.VMEM(shape, F32)
    raws = [vm(NX, NY, NZ)] * 3 + [vm(NY, LANES), vm(NX, LANES), vm(NX, LANES)]
    if kind == 'basis':
        rounds, reds = CG_ITERS + 2, ()
        work = [vm(*field), vm(*field), vm(NB, *field), vm(NP, ROWS, FACES, *TILE), vm(*block), vm(NY, LANES),
                vm(40, LANES), vm(32, LANES), vm(CG_ITERS, 16, LANES), vm(NB, 16, LANES), vm(2, 16, LANES), vm(*block)]
    else:
        rounds, reds = 3, (2,)
        work = [vm(*field), vm(*field), vm(*field), vm(*block), vm(*block), vm(NP, ROWS, FACES, *TILE), vm(*block)]
    work += [vm(NP, FOLD, LANES), vm(LANES, LANES), vm(*block), vm(*block)]
    sides = [vm(rounds, 2, FOLD, LANES), vm(rounds, 2, NP, 1, LANES)]
    faces = sides + [vm(rounds, FOLD, LANES)] + sides + [vm(rounds, 2, FOLD, LANES)]
    rows = [vm(*reds, 3, 1, LANES)] + [vm(*reds, n, 1, LANES) for n in counts]
    dma = pltpu.SemaphoreType.DMA
    sems = [dma((6,)), dma((2,)), dma((rounds, 6)), dma((rounds, 6)), dma((*reds, 3, 8)), dma((*reds, 3, 8))]
    return raws + work + faces + rows + sems


def solution(mesh):
    counts = tuple(mesh.shape[name] for name in AXES)
    grid_spec = P(*AXES)
    block = jax.ShapeDtypeStruct((NX, NY, NZ), F32)

    def call(kernel, kind, ident):
        hbm = pl.BlockSpec(memory_space=pl.ANY)
        return pl.pallas_call(
            functools.partial(kernel, counts),
            out_shape=(block, block, jax.ShapeDtypeStruct((1, LANES), F32)),
            in_specs=[hbm] * 4,
            out_specs=(hbm, hbm, pl.BlockSpec(memory_space=pltpu.VMEM)),
            scratch_shapes=scratch_for(kind, counts),
            compiler_params=pltpu.CompilerParams(collective_id=ident, has_side_effects=True),
            name=kind,
        )

    def local_solve(k_cell, k_ghost, f_rhs, u_init):
        args = (k_cell, k_ghost, f_rhs, u_init)
        u_out, r_out, row = call(basis_kernel, 'basis', 0)(*args)
        u_out, r_out, row = lax.cond(
            row[0, 8] > 0.5,
            lambda: (u_out, r_out, row),
            lambda: tuple(call(plain_kernel, 'plain', 1)(*args)))
        return u_out, r_out, row[0, 0:CG_ITERS]

    return jax.shard_map(local_solve, mesh=mesh, in_specs=(grid_spec, P(), grid_spec, grid_spec),
                         out_specs=(grid_spec, grid_spec, P()), check_vma=False)
```

```python
import functools

import jax
import jax.numpy as jnp
from jax import lax
from jax.experimental import pallas as pl
from jax.experimental.pallas import tpu as pltpu
from jax.sharding import PartitionSpec as P

CG_ITERS = 8
NB = CG_ITERS + 1
NX, NY, NZ = 32, 64, 64
NP = NX // 2
R0 = 8
MESH = pl.DeviceIdType.MESH
AXES = ('gx', 'gy', 'gz')
BOUND = 4096.0
VMEM_BYTES = 60_000_000
F32 = jnp.float32
SUB, LANES, HALF, LOW = 8, 128, 64, 63
ROWS = NY // SUB
TILE = (SUB, LANES)
WIDE = (2 * SUB, LANES)
FACES = 6
FOLD = NY // 2
TURNS = (4, 8, 16, 32)


def own(t):
    return slice(R0 + SUB * t, R0 + SUB * t + SUB)


def tile(t):
    return slice(SUB * t, SUB * t + SUB)


def one(i):
    return slice(i, i + 1)


def spin(values, by):
    return pltpu.roll(values, by, 1)


def turn_half(values):
    return spin(values, HALF)


def row_sum(values):
    return jnp.sum(values, axis=0, keepdims=True)


def lane_sum(values):
    return jnp.sum(values, axis=1, keepdims=True)


def total_of(parts):
    parts = list(parts)
    while len(parts) > 1:
        parts = [sum(parts[i + 1:i + 2], parts[i]) for i in range(0, len(parts), 2)]
    return parts[0]


def lane_iota(rows=8):
    return lax.broadcasted_iota(jnp.int32, (rows, LANES), 1)


def row_iota(rows):
    return lax.broadcasted_iota(jnp.int32, (rows, LANES), 0)


class Comm:
    def __init__(self, counts, bufs):
        self.counts = counts
        self.pos = [lax.axis_index(name) for name in AXES]
        self.has = []
        for axis in range(3):
            self.has.append(self.pos[axis] > 0)
            self.has.append(self.pos[axis] < counts[axis] - 1)
        (self.xs, self.ys, self.zs, self.xr, self.yr, self.zr, self.send_sem, self.recv_sem) = bufs

    def neighbour(self, face):
        return {AXES[face // 2]: self.pos[face // 2] + (1 if face % 2 else -1)}

    def source(self, rnd, face):
        axis, high = face // 2, face % 2
        return self.zs.at[rnd] if axis == 2 else (self.xs, self.ys)[axis].at[rnd, high]

    def copies(self, rnd, face):
        axis, high = face // 2, face % 2
        src = self.source(rnd, face)
        dst = (self.xr, self.yr, self.zr)[axis]
        return pltpu.make_async_remote_copy(
            src_ref=src, dst_ref=dst.at[rnd, 1 - high],
            send_sem=self.send_sem.at[rnd, face], recv_sem=self.recv_sem.at[rnd, face ^ 1],
            device_id=self.neighbour(face), device_id_type=MESH)

    def send(self, rnd, face):
        @pl.when(self.has[face])
        def _():
            self.copies(rnd, face).start()

    def wait_recv(self, rnd, face):
        axis, high = face // 2, face % 2
        src = self.source(rnd, face)
        dst = (self.xr, self.yr, self.zr)[axis]

        @pl.when(self.has[face])
        def _():
            pltpu.make_async_remote_copy(
                src_ref=src, dst_ref=dst.at[rnd, high],
                send_sem=self.send_sem.at[rnd, face], recv_sem=self.recv_sem.at[rnd, face],
                device_id=self.neighbour(face), device_id_type=MESH).wait_recv()

    def wait_send(self, rnd, face):
        @pl.when(self.has[face])
        def _():
            self.copies(rnd, face).wait_send()


GROUPS = (('gx',), ('gy', 'gz'))


def group_of(comm, group):
    sizes = [comm.counts[AXES.index(name)] for name in group]
    size, rank = 1, 0
    for name, n in zip(group, sizes):
        size, rank = size * n, rank * n + comm.pos[AXES.index(name)]

    def peer(off):
        left, where = lax.rem(rank + off, size), {}
        for name, n in reversed(tuple(zip(group, sizes))):
            where[name], left = lax.rem(left, n), lax.div(left, n)
        return where
    return size, rank, peer


def greet_faces(comm):
    sem = pltpu.get_barrier_semaphore()
    for face in range(FACES):
        @pl.when(comm.has[face])
        def _():
            pl.semaphore_signal(sem, inc=1, device_id=comm.neighbour(face), device_id_type=MESH)
    return sem, sum(flag.astype(jnp.int32) for flag in comm.has)


def greet_groups(comm):
    sem, total = pltpu.get_barrier_semaphore(), 0
    for group in GROUPS:
        size, _, peer = group_of(comm, group)
        for off in range(1, size):
            pl.semaphore_signal(sem, inc=1, device_id=peer(off), device_id_type=MESH)
        total += size - 1
    return sem, total


class Reducer:
    def __init__(self, comm, send_row, recv_rows, send_sem, recv_sem):
        self.comm, self.send_row, self.recv_rows, self.ss, self.rs = comm, send_row, recv_rows, send_sem, recv_sem

    def run(self, row):
        for stage, group in enumerate(GROUPS):
            size, rank, peer = group_of(self.comm, group)
            rows = self.recv_rows[stage]
            self.send_row[stage] = row
            copies = [pltpu.make_async_remote_copy(
                src_ref=self.send_row.at[stage], dst_ref=rows.at[rank], send_sem=self.ss.at[stage, off],
                recv_sem=self.rs.at[stage, off], device_id=peer(off), device_id_type=MESH) for off in range(1, size)]
            for copy in copies:
                copy.start()
            rows[rank] = row
            for copy in copies:
                copy.wait()
            row = total_of(rows[i] for i in range(size))
        return row


def store_plane_faces(comm, rnd, ref, p):
    comm.ys[rnd, 0, p] = ref[p + 1, R0:R0 + 1, :]
    comm.ys[rnd, 1, p] = ref[p + 1, R0 + NY - 1:R0 + NY, :]


def pack_x_faces(comm, rnd, ref):
    half = FOLD
    lane = lane_iota(half)
    a, b = ref[1, R0:R0 + half, :], ref[1, R0 + half:R0 + NY, :]
    comm.xs[rnd, 0] = jnp.where(lane < HALF, a, turn_half(b))
    a, b = ref[NP, R0:R0 + half, :], ref[NP, R0 + half:R0 + NY, :]
    comm.xs[rnd, 1] = jnp.where(lane < HALF, turn_half(a), b)


def face_mask(turn, rows=FOLD):
    return ((lane_iota(rows) + 1) & LOW) < turn


def pack_z(comm, rnd, ref, tree):
    def fold(p, carry):
        low, high = ref[p + 1, R0:R0 + FOLD, :], ref[p + 1, R0 + FOLD:R0 + NY, :]
        tree[p] = jnp.where(face_mask(2), low, spin(high, 2))
        return carry
    lax.fori_loop(0, NP, fold, 0, unroll=8)
    join_z(comm, rnd, tree)


def join_z(comm, rnd, tree):
    parts = [tree[p] for p in range(NP)]
    for turn in TURNS:
        parts = [jnp.where(face_mask(turn), parts[i], spin(parts[i + 1], turn)) for i in range(0, len(parts), 2)]
    comm.zs[rnd] = parts[0]


def unpack_z(comm, rnd, tree):
    odd = (lane_iota(FOLD) & 1) == 1
    parts = [jnp.where(odd, spin(comm.zr[rnd, 1], LOW - 2), spin(comm.zr[rnd, 0], HALF - 1))]
    for turn in reversed(TURNS):
        parts = [q for part in parts for q in (part, spin(part, LANES - turn))]
    for p in range(NP):
        tree[p] = parts[p]


def spread_z(comm, rnd, tree, ghost):
    unpack_z(comm, rnd, tree)

    def fold(p, carry):
        ghost[p, 0:FOLD, :] = spin(tree[p], 2)
        ghost[p, FOLD:NY, :] = tree[p]
        return carry
    lax.fori_loop(0, NP, fold, 0, unroll=8)


def inner_planes(ref):
    low = lane_iota(NY) < HALF
    ref[0, R0:R0 + NY, :] = jnp.where(low, 0.0, turn_half(ref[NP, R0:R0 + NY, :]))
    ref[NP + 1, R0:R0 + NY, :] = jnp.where(low, turn_half(ref[1, R0:R0 + NY, :]), 0.0)


def x_ghosts(comm, rnd):
    low = lane_iota(FOLD) < HALF
    lo, hi = comm.xr[rnd, 0], comm.xr[rnd, 1]
    below = [jnp.where(low, lo, 0.0), jnp.where(low, turn_half(lo), 0.0)]
    above = [jnp.where(low, 0.0, turn_half(hi)), jnp.where(low, 0.0, hi)]
    return below, above


def outer_layers(comm, rnd, ref):
    inner_planes(ref)
    below, above = x_ghosts(comm, rnd)
    for i in range(2):
        rows = slice(R0 + FOLD * i, R0 + FOLD * i + FOLD)
        ref[0, rows, :] = ref[0, rows, :] + below[i]
        ref[NP + 1, rows, :] = ref[NP + 1, rows, :] + above[i]
    for p in range(NP):
        ref[p + 1, R0 - 1:R0, :] = comm.yr[rnd, 0, p]
        ref[p + 1, R0 + NY:R0 + NY + 1, :] = comm.yr[rnd, 1, p]


def blank_rows(ref):
    for p in range(NP):
        ref[p + 1, R0 - 1:R0, :] = jnp.zeros((1, LANES), F32)
        ref[p + 1, R0 + NY:R0 + NY + 1, :] = jnp.zeros((1, LANES), F32)


def neighbours(ref, p, t, ghost=None):
    row = R0 + SUB * t
    lane = lane_iota() & LOW
    centre = ref[p + 1, own(t), :]
    xm = ref[p, own(t), :]
    xp = ref[p + 2, own(t), :]
    ym = ref[p + 1, row - 1:row + SUB - 1, :]
    yp = ref[p + 1, row + 1:row + SUB + 1, :]
    zm, zp = spin(centre, 1), spin(centre, LANES - 1)
    if ghost is not None:
        edge = ghost[p, tile(t), :]
        zm, zp = jnp.where(lane == 0, edge, zm), jnp.where(lane == LOW, edge, zp)
    return centre, (xm, xp, ym, yp, zm, zp)


def sweep(body, state=(), unroll=2):
    def plane(p, carry):
        carry = list(carry)
        body(p, carry)
        return tuple(carry)
    return lax.fori_loop(0, NP, plane, tuple(state), unroll=unroll)


def zero_tiles(n):
    return tuple(jnp.zeros(TILE, F32) for _ in range(n))


def send_faces(comm, rnd, ref, tree, folded=False):
    (join_z if folded else functools.partial(pack_z, ref=ref))(comm, rnd, tree=tree)
    for face in (4, 5):
        comm.send(rnd, face)
    pack_x_faces(comm, rnd, ref)
    for p in range(NP):
        store_plane_faces(comm, rnd, ref, p)
    for face in range(4):
        comm.send(rnd, face)


def load_field(raw, ref):
    def body(p, state):
        ref[p + 1, R0:R0 + NY, :] = jnp.concatenate([raw[p], raw[p + NP]], axis=1)
    sweep(body, unroll=4)


def fill_ghost_conductivity(comm, square, gx_slab, gy_slab, gz_slab):
    px, py, pz = comm.pos
    half = FOLD
    turn = 64 * lax.rem(pz, 2)
    lane = lane_iota(half)
    a, b = pltpu.roll(gx_slab[0:half, :], turn, 1), pltpu.roll(gx_slab[half:NY, :], turn, 1)
    x_face = jnp.where(lane < HALF, a, turn_half(b))
    for end in range(2):
        @pl.when(jnp.logical_not(comm.has[end]))
        def _():
            comm.xr[0, end] = x_face
    rows = pltpu.roll(gy_slab[...], turn, 1)
    y_face = jnp.where(lane_iota(NP) < HALF, rows[0:NP], turn_half(rows[NP:NX]))
    for end in range(2):
        @pl.when(jnp.logical_not(comm.has[2 + end]))
        def _():
            for p in range(NP):
                comm.yr[0, end, p] = y_face[one(p)]
    for end in range(2):
        @pl.when(jnp.logical_not(comm.has[4 + end]))
        def _():
            cols = spin(gz_slab[...], HALF * lax.rem(py, 2))
            shift = 0 if end else LOW
            square[...] = jnp.zeros(square.shape, F32)
            for x in range(NX):
                for c in range(2):
                    square[one((4 * (x % NP) + 2 * c + HALF * (x // NP) + shift) % LANES)] = cols[one(x)]
            turned = square[...].T
            second = ((lane_iota(FOLD) - shift) & 3) == 2
            comm.zr[0, end] = jnp.where(second, turned[FOLD:NY], turned[:FOLD])


def zero_ends(comm, rounds):
    for face in range(FACES):
        @pl.when(jnp.logical_not(comm.has[face]))
        def _():
            buf = (comm.xr, comm.yr, comm.zr)[face // 2]
            for rnd in rounds:
                buf[rnd, face % 2] = jnp.zeros(buf.shape[2:], F32)


def lanes_of(pos):
    return pl.ds(pl.multiple_of(lax.div(pos, 2) * LANES, LANES), LANES)


def start_up(comm, ins, raws, slabs, load_sem):
    k_hbm, g_hbm, f_hbm, u_hbm = ins
    px, py, pz = comm.pos
    loads = [pltpu.make_async_copy(k_hbm, raws[0], load_sem.at[0]),
             pltpu.make_async_copy(u_hbm, raws[1], load_sem.at[1])]
    x_row = jnp.where(comm.has[1], 0, 1)
    y_row = jnp.where(comm.has[3], 2, 3)
    z_row = jnp.where(comm.has[5], 4, 5)
    z_lanes = lanes_of(pz)
    y_lanes = lanes_of(py)
    loads.append(pltpu.make_async_copy(
        g_hbm.at[x_row, pl.ds(pl.multiple_of(py * NY, NY), NY), z_lanes], slabs[0], load_sem.at[2]))
    loads.append(pltpu.make_async_copy(
        g_hbm.at[y_row, pl.ds(pl.multiple_of(px * NX, NX), NX), z_lanes], slabs[1], load_sem.at[3]))
    loads.append(pltpu.make_async_copy(
        g_hbm.at[z_row, pl.ds(pl.multiple_of(px * NX, NX), NX), y_lanes], slabs[2], load_sem.at[4]))
    loads.append(pltpu.make_async_copy(f_hbm, raws[2], load_sem.at[5]))
    for load in loads:
        load.start()
    return loads


def first_exchange(comm, loads, greet, raws, slabs, k_ref, u_ref, tree, square, k_ghost, u_ghost):
    sem, total = greet
    loads[0].wait()
    load_field(raws[0], k_ref)
    pl.semaphore_wait(sem, total)
    send_faces(comm, 0, k_ref, tree)
    loads[1].wait()
    load_field(raws[1], u_ref)
    send_faces(comm, 1, u_ref, tree)
    for load in loads[2:]:
        load.wait()
    fill_ghost_conductivity(comm, square, *slabs)
    for rnd, ref, ghost in ((0, k_ref, k_ghost), (1, u_ref, u_ghost)):
        for face in range(FACES):
            comm.wait_recv(rnd, face)
        outer_layers(comm, rnd, ref)
        spread_z(comm, rnd, tree, ghost)


def first_residual(raw_f, k_ref, u_ref, k_ghost, u_ghost, p, t, d_ref):
    centre, others = neighbours(k_ref, p, t, k_ghost)
    u_own, u_others = neighbours(u_ref, p, t, u_ghost)
    twice = centre + centre
    weights = [twice * other / (centre + other) for other in others]
    diag = total_of(weights)
    au = total_of([w * (u_own - other) for w, other in zip(weights, u_others)])
    f_tile = jnp.concatenate([raw_f[p, tile(t), :], raw_f[p + NP, tile(t), :]], axis=1)
    d_ref[p, tile(t), :] = diag
    return weights, f_tile - au, 1.0 / diag


def write_plane(raw_ref, p, values):
    raw_ref[p] = values[:, :HALF]
    raw_ref[p + NP] = turn_half(values)[:, :HALF]


def dot_rows(a, b):
    prod = a[:2 * SUB] * b[:2 * SUB]
    return row_sum(prod[:SUB] + prod[SUB:])


def solve_coefficients(row, mom_ref, pc_ref, hist_ref, full_ref):
    lane24, line24 = lane_iota(24), row_iota(24)
    wide = jnp.broadcast_to(row, (24, LANES))
    base = lane_sum(jnp.where((lane24 == line24) & (lane24 < 17), wide, 0.0))
    base = jnp.broadcast_to(base, (24, LANES))
    first, second = base[0:1], base[1:2]
    even = (line24 & 1) == 0
    mom = jnp.where(line24 >= 2, 2.0 * base - jnp.where(even, first, second), base)
    mom = jnp.where(line24 < 17, mom, 0.0)
    lane16, line16 = lane_iota(16), row_iota(16)
    wide = jnp.broadcast_to(row, WIDE)
    for k in range(NB):
        big = jnp.maximum(line16, k)
        small = jnp.minimum(line16, k)
        want = 17 + lax.shift_right_logical(big * (big + 1), 1) + small
        col = lane_sum(jnp.where((lane16 == want) & (line16 < NB), wide, 0.0))
        full_ref[k] = jnp.broadcast_to(col, WIDE)
    zeros8 = jnp.zeros(TILE, F32)
    mom_ref[:SUB] = zeros8
    mom_ref[32:40] = zeros8
    pc_ref[:SUB] = zeros8
    pc_ref[24:32] = zeros8
    unit = jnp.where(line16 == 0, 1.0, 0.0)
    cvec, pvec, avec = unit, unit, jnp.zeros(WIDE, F32)
    rvec, mvec = mom, mom
    mu0 = mom[0:1]
    rho = dot_rows(cvec, rvec)
    ok = jnp.where(rho > 0.0, 1.0, 0.0)
    two_one = jnp.where(line16 == 1, 2.0, 1.0)
    for t in range(CG_ITERS):
        mom_ref[8:32] = mvec
        mom_ref[7:8] = mvec[1:2]
        pc_ref[8:24] = pvec
        qvec = mvec - 0.5 * (mom_ref[9:33] + mom_ref[7:31])
        npvec = 0.5 * (two_one * pc_ref[7:23] + pc_ref[9:25])
        curv = dot_rows(pvec, qvec)
        size = row_sum(jnp.abs(pvec))
        ok = jnp.where(size * size * mu0 < BOUND * curv, ok, 0.0)
        alpha = rho / curv
        avec = avec + alpha * pvec
        cvec = cvec - alpha * (pvec - npvec)
        rvec = rvec - alpha * qvec
        hist_ref[t] = cvec
        rho_new = dot_rows(cvec, rvec)
        size = row_sum(jnp.abs(cvec))
        ok = jnp.where(size * size * mu0 < BOUND * rho_new, ok, 0.0)
        beta = rho_new / rho
        pvec = cvec + beta * pvec
        mvec = rvec + beta * mvec
        rho = rho_new
    return avec, cvec, ok


def squares_row(hist_ref, full_ref):
    lane = lane_iota(1)
    out = jnp.zeros((1, LANES), F32)
    for t in range(CG_ITERS):
        cvec = hist_ref[t]
        acc = full_ref[0] * hist_ref[t, one(0)]
        for j in range(1, NB):
            acc = acc + full_ref[j] * hist_ref[t, one(j)]
        out = jnp.where(lane == t, dot_rows(acc, cvec), out)
    return out


def basis_kernel(counts, k_hbm, g_hbm, f_hbm, u_hbm, u_out, r_out, h_ref, ok_ref,
                 raw_k, raw_u, raw_f, slab_x, slab_y, slab_z, k_ref, u_ref, z_ref, coef_ref, d_ref, sums_ref,
                 mom_ref, pc_ref, hist_ref, full_ref, comb_ref, edge_ref, tree, square, k_ghost, u_ghost,
                 xs, ys, zs, xr, yr, zr, send_row, rows_a, rows_b,
                 load_sem, send_sem, recv_sem, red_ss, red_rs):
    comm = Comm(counts, (xs, ys, zs, xr, yr, zr, send_sem, recv_sem))
    raws, slabs = (raw_k, raw_u, raw_f), (slab_x, slab_y, slab_z)
    loads = start_up(comm, (k_hbm, g_hbm, f_hbm, u_hbm), raws, slabs, load_sem)
    greet = greet_faces(comm)
    zero_ends(comm, range(1, CG_ITERS + 2))
    sums_ref[...] = jnp.zeros(sums_ref.shape, F32)
    for k in range(CG_ITERS):
        blank_rows(z_ref.at[k])
    first_exchange(comm, loads, greet, raws, slabs, k_ref, u_ref, tree, square, k_ghost, u_ghost)

    def first(p, state):
        lane = lane_iota() & LOW
        for t in range(ROWS):
            weights, resid, inv = first_residual(raw_f, k_ref, u_ref, k_ghost, u_ghost, p, t, d_ref)
            factor = inv + inv
            scaled = [w * factor for w in weights]
            low, high = scaled[4:]
            edge_ref[p, tile(t), :] = jnp.where(lane == 0, low, jnp.where(lane == LOW, high, 0.0))
            scaled[4:] = jnp.where(lane == 0, 0.0, low), jnp.where(lane == LOW, 0.0, high)
            for i in range(FACES):
                coef_ref[p, t, i] = scaled[i]
            z_ref[0, p + 1, own(t), :] = resid * inv

    sweep(first)
    send_faces(comm, 2, z_ref.at[0], tree)

    def products(k):
        def body(p, accs):
            accs = list(accs)
            for t in range(ROWS):
                row = own(t)
                d = d_ref[p, tile(t), :]
                z_k = z_ref[k, p + 1, row, :]
                dz = d * z_k
                ddz = d * dz
                for i in range(k + 1):
                    z_i = z_ref[i, p + 1, row, :]
                    accs[i] = accs[i] + ddz * z_i
                    if i >= k - 1:
                        accs[k + 1 + (k - i)] = accs[k + 1 + (k - i)] + dz * z_i
            return tuple(accs)
        accs = lax.fori_loop(0, NP, body, zero_tiles(k + 2 + (1 if k else 0)))
        for i in range(k + 1):
            at = 17 + k * (k + 1) // 2 + i
            sums_ref[one(at)] = row_sum(accs[i])
        sums_ref[one(2 * k)] = row_sum(accs[k + 1])
        if k:
            sums_ref[one(2 * k - 1)] = row_sum(accs[k + 2])

    def late_terms(k, rnd):
        ref = z_ref.at[k + 1]
        weigh = (lambda term: 0.5 * term) if k == 0 else (lambda term: term)
        unpack_z(comm, rnd, tree)
        below, above = x_ghosts(comm, rnd)
        for t in range(ROWS):
            part = slice(SUB * (t % 4), SUB * (t % 4) + SUB)
            for plane, face, layer in ((1, 0, below), (NP, 1, above)):
                term = coef_ref[plane - 1, t, face] * layer[t // 4][part]
                ref[plane, own(t), :] = ref[plane, own(t), :] + weigh(term)

        first, last = row_iota(SUB) == 0, row_iota(SUB) == SUB - 1

        def body(p, state):
            turned = [spin(tree[p], 2), tree[p]]
            news = []
            for t in range(ROWS):
                part = slice(SUB * (t % 4), SUB * (t % 4) + SUB)
                term = edge_ref[p, tile(t), :] * turned[t // 4][part]
                for end, at, sub, mask in ((0, 0, 0, first), (1, ROWS - 1, SUB - 1, last)):
                    if t == at:
                        line = coef_ref[p, t, 2 + end, one(sub), :] * comm.yr[rnd, end, p]
                        term = term + jnp.where(mask, line, 0.0)
                news.append(ref[p + 1, own(t), :] + weigh(term))
                ref[p + 1, own(t), :] = news[t]
            if k < CG_ITERS - 1:
                for t in range(4):
                    tree[p, tile(t), :] = jnp.where(face_mask(2, SUB), news[t], spin(news[t + 4], 2))
        sweep(body, unroll=4)

    for k in range(CG_ITERS):
        rnd = 2 + k
        inner_planes(z_ref.at[k])

        def step(p, state):
            for t in range(ROWS):
                _, others = neighbours(z_ref.at[k], p, t)
                total = total_of(coef_ref[p, t, i] * others[i] for i in range(FACES))
                z_new = 0.5 * total if k == 0 else total - z_ref[k - 1, p + 1, own(t), :]
                z_ref[k + 1, p + 1, own(t), :] = z_new

        sweep(step)
        products(k)
        for face in range(FACES):
            comm.wait_recv(rnd, face)
        late_terms(k, rnd)
        if k < CG_ITERS - 1:
            send_faces(comm, rnd + 1, z_ref.at[k + 1], tree, folded=True)
    products(CG_ITERS)

    total = jnp.broadcast_to(lane_sum(sums_ref[...]), (NY, LANES))
    row = row_sum(jnp.where(lane_iota(64) == row_iota(64), total, 0.0))
    red = Reducer(comm, send_row, (rows_a, rows_b), red_ss, red_rs)
    row = red.run(row)
    avec, cvec, ok = solve_coefficients(row, mom_ref, pc_ref, hist_ref, full_ref)
    comb_ref[0] = avec
    comb_ref[1] = cvec

    a_co = [jnp.broadcast_to(comb_ref[0, one(i)], TILE) for i in range(CG_ITERS)]
    c_co = [jnp.broadcast_to(comb_ref[1, one(i)], TILE) for i in range(NB)]

    def combine(p, carry):
        for t in range(ROWS):
            row = own(t)
            rows = tile(t)
            basis = [z_ref[i, p + 1, row, :] for i in range(NB)]
            ut, rt = a_co[0] * basis[0], c_co[0] * basis[0]
            for i in range(1, NB):
                if i < CG_ITERS:
                    ut = ut + a_co[i] * basis[i]
                rt = rt + c_co[i] * basis[i]
            ut = u_ref[p + 1, row, :] + ut
            rt = d_ref[p, rows, :] * rt
            u_out[p, rows, :] = ut[:, :HALF]
            u_out[p + NP, rows, :] = turn_half(ut)[:, :HALF]
            r_out[p, rows, :] = rt[:, :HALF]
            r_out[p + NP, rows, :] = turn_half(rt)[:, :HALF]
        return carry

    lax.fori_loop(0, NP, combine, 0)
    h_ref[...] = squares_row(hist_ref, full_ref)
    ok_ref[0, 0] = ok[0, 0].astype(jnp.int32)
    for rnd in range(CG_ITERS + 2):
        for face in range(FACES):
            comm.wait_send(rnd, face)


def plain_kernel(counts, k_hbm, g_hbm, f_hbm, u_hbm, u_out, r_out, h_ref,
                 raw_k, raw_u, raw_f, slab_x, slab_y, slab_z, k_ref, u_ref, p_ref, q_ref, r_ref, coef_ref, d_ref, tree, square, k_ghost, u_ghost,
                 xs, ys, zs, xr, yr, zr, send_row, rows_a, rows_b,
                 load_sem, send_sem, recv_sem, red_ss, red_rs):
    comm = Comm(counts, (xs, ys, zs, xr, yr, zr, send_sem, recv_sem))
    raws, slabs = (raw_k, raw_u, raw_f), (slab_x, slab_y, slab_z)
    loads = start_up(comm, (k_hbm, g_hbm, f_hbm, u_hbm), raws, slabs, load_sem)
    greet = greet_groups(comm)
    zero_ends(comm, range(1, 3))
    first_exchange(comm, loads, greet, raws, slabs, k_ref, u_ref, tree, square, k_ghost, u_ghost)
    red = [Reducer(comm, send_row.at[i], (rows_a.at[i], rows_b.at[i]), red_ss.at[i], red_rs.at[i]) for i in range(2)]

    def reduce(which, accs):
        lane = lane_iota(1)
        row = jnp.zeros((1, LANES), F32)
        for i, acc in enumerate(accs):
            total = row_sum(lane_sum(acc))
            row = jnp.where(lane == i, jnp.broadcast_to(total, (1, LANES)), row)
        row = red[which].run(row)
        return [lane_sum(jnp.where(lane == i, row, 0.0)) for i in range(len(accs))]

    def first(p, state):
        for t in range(ROWS):
            weights, resid, inv = first_residual(raw_f, k_ref, u_ref, k_ghost, u_ghost, p, t, d_ref)
            for i in range(FACES):
                coef_ref[p, t, i] = weights[i]
            r_ref[p, tile(t), :] = resid
            z_new = resid * inv
            p_ref[p + 1, own(t), :] = z_new
            state[0] = state[0] + resid * z_new

    rho, = reduce(0, sweep(first, zero_tiles(1)))

    def iteration(it, carry):
        rho, hist = carry

        send_faces(comm, 2, p_ref, tree)
        for face in range(FACES):
            comm.wait_recv(2, face)
            comm.wait_send(2, face)
        outer_layers(comm, 2, p_ref)
        spread_z(comm, 2, tree, k_ghost)

        def apply(p, state):
            for t in range(ROWS):
                centre, others = neighbours(p_ref, p, t, k_ghost)
                q = total_of(coef_ref[p, t, i] * (centre - others[i]) for i in range(FACES))
                q_ref[p, tile(t), :] = q
                state[0] = state[0] + centre * q

        curv, = reduce(1, sweep(apply, zero_tiles(1)))
        alpha = jnp.broadcast_to(rho / curv, TILE)

        def update(p, accs):
            acc_z, acc_r = accs
            for t in range(ROWS):
                row = own(t)
                rows = tile(t)
                u_ref[p + 1, row, :] = u_ref[p + 1, row, :] + alpha * p_ref[p + 1, row, :]
                resid = r_ref[p, rows, :] - alpha * q_ref[p, rows, :]
                r_ref[p, rows, :] = resid
                acc_z = acc_z + resid * (resid / d_ref[p, rows, :])
                acc_r = acc_r + resid * resid
            return acc_z, acc_r

        rho_new, rr = reduce(0, lax.fori_loop(0, NP, update, zero_tiles(2)))
        beta = jnp.broadcast_to(rho_new / rho, TILE)

        def turn(p, carry):
            for t in range(ROWS):
                row = own(t)
                rows = tile(t)
                p_ref[p + 1, row, :] = r_ref[p, rows, :] / d_ref[p, rows, :] + beta * p_ref[p + 1, row, :]
            return carry

        lax.fori_loop(0, NP, turn, 0)
        hist = jnp.where(lane_iota(1) == it, jnp.broadcast_to(rr, (1, LANES)), hist)
        return rho_new, hist

    _, hist = lax.fori_loop(0, CG_ITERS, iteration, (rho, jnp.zeros((1, LANES), F32)))
    h_ref[...] = hist

    def finish(p, carry):
        write_plane(u_out, p, u_ref[p + 1, R0:R0 + NY, :])
        write_plane(r_out, p, r_ref[p])
        return carry

    lax.fori_loop(0, NP, finish, 0)
    for rnd in range(2):
        for face in range(FACES):
            comm.wait_send(rnd, face)


def scratch_for(kind, counts):
    field = (NP + 2, NY + 16, LANES)
    block = (NP, NY, LANES)
    vm = lambda *shape: pltpu.VMEM(shape, F32)
    raws = [vm(NX, NY, NZ)] * 3 + [vm(NY, LANES), vm(NX, LANES), vm(NX, LANES)]
    if kind == 'basis':
        rounds, reds = CG_ITERS + 2, ()
        work = [vm(*field), vm(*field), vm(NB, *field), vm(NP, ROWS, FACES, *TILE), vm(*block), vm(NY, LANES),
                vm(40, LANES), vm(32, LANES), vm(CG_ITERS, 16, LANES), vm(NB, 16, LANES), vm(2, 16, LANES), vm(*block)]
    else:
        rounds, reds = 3, (2,)
        work = [vm(*field), vm(*field), vm(*field), vm(*block), vm(*block), vm(NP, ROWS, FACES, *TILE), vm(*block)]
    work += [vm(NP, FOLD, LANES), vm(LANES, LANES), vm(*block), vm(*block)]
    sides = [vm(rounds, 2, FOLD, LANES), vm(rounds, 2, NP, 1, LANES)]
    faces = sides + [vm(rounds, FOLD, LANES)] + sides + [vm(rounds, 2, FOLD, LANES)]
    sizes = [counts[0], counts[1] * counts[2]]
    rows = [vm(*reds, 2, 1, LANES)] + [vm(*reds, n, 1, LANES) for n in sizes]
    dma = pltpu.SemaphoreType.DMA
    sems = [dma((6,)), dma((rounds, 6)), dma((rounds, 6)), dma((*reds, 2, max(sizes))), dma((*reds, 2, max(sizes)))]
    return raws + work + faces + rows + sems


def solution(mesh):
    counts = tuple(mesh.shape[name] for name in AXES)
    grid_spec = P(*AXES)
    block = jax.ShapeDtypeStruct((NX, NY, NZ), F32)

    def call(kernel, kind, ident, *more):
        hbm, vmem = pl.BlockSpec(memory_space=pltpu.HBM), pl.BlockSpec(memory_space=pltpu.VMEM)
        smem = [pl.BlockSpec(memory_space=pltpu.SMEM)] * len(more)
        return pl.pallas_call(
            functools.partial(kernel, counts),
            out_shape=(block, block, jax.ShapeDtypeStruct((1, LANES), F32), *more),
            in_specs=[hbm] * 4,
            out_specs=(vmem, vmem, vmem, *smem),
            scratch_shapes=scratch_for(kind, counts),
            compiler_params=pltpu.CompilerParams(collective_id=ident, has_side_effects=True, vmem_limit_bytes=VMEM_BYTES),
            name=kind,
        )

    def local_solve(k_cell, k_ghost, f_rhs, u_init):
        args = (k_cell, k_ghost, f_rhs, u_init)
        *fast, ok = call(basis_kernel, 'basis', 0, jax.ShapeDtypeStruct((1, 1), jnp.int32))(*args)
        u_out, r_out, row = lax.cond(ok[0, 0] > 0, lambda: tuple(fast),
                                     lambda: tuple(call(plain_kernel, 'plain', 1)(*args)))
        return u_out, r_out, row[0, 0:CG_ITERS]

    return jax.shard_map(local_solve, mesh=mesh, in_specs=(grid_spec, P(), grid_spec, grid_spec),
                         out_specs=(grid_spec, grid_spec, P()), check_vma=False)
```

```python
import functools

import jax
import jax.numpy as jnp
from jax import lax
from jax.experimental import pallas as pl
from jax.experimental.pallas import tpu as pltpu
from jax.sharding import PartitionSpec as P

CG_ITERS = 8
NB = CG_ITERS + 1
NX, NY, NZ = 32, 64, 64
NP = NX // 2
R0 = 8
MESH = pl.DeviceIdType.MESH
AXES = ('gx', 'gy', 'gz')
BOUND = 4096.0
GRAM = 2 * NB
VMEM_BYTES = 60_000_000
F32 = jnp.float32
SUB, LANES, HALF, LOW = 8, 128, 64, 63
ROWS = NY // SUB
TILE = (SUB, LANES)
WIDE = (2 * SUB, LANES)
FACES = 6
FOLD = NY // 2
TURNS = (4, 8, 16, 32)


def own(t):
    return slice(R0 + SUB * t, R0 + SUB * t + SUB)


def tile(t):
    return slice(SUB * t, SUB * t + SUB)


def one(i):
    return slice(i, i + 1)


def spin(values, by):
    return pltpu.roll(values, by, 1)


def turn_half(values):
    return spin(values, HALF)


def row_sum(values):
    return jnp.sum(values, axis=0, keepdims=True)


def lane_sum(values):
    return jnp.sum(values, axis=1, keepdims=True)


def total_of(parts):
    parts = list(parts)
    while len(parts) > 1:
        parts = [sum(parts[i + 1:i + 2], parts[i]) for i in range(0, len(parts), 2)]
    return parts[0]


def lane_iota(rows=8):
    return lax.broadcasted_iota(jnp.int32, (rows, LANES), 1)


def row_iota(rows):
    return lax.broadcasted_iota(jnp.int32, (rows, LANES), 0)


class Comm:
    def __init__(self, counts, bufs):
        self.counts = counts
        self.pos = [lax.axis_index(name) for name in AXES]
        self.has = []
        for axis in range(3):
            self.has.append(self.pos[axis] > 0)
            self.has.append(self.pos[axis] < counts[axis] - 1)
        (self.xs, self.ys, self.zs, self.xr, self.yr, self.zr, self.send_sem, self.recv_sem) = bufs

    def neighbour(self, face):
        return {AXES[face // 2]: self.pos[face // 2] + (1 if face % 2 else -1)}

    def source(self, rnd, face):
        axis, high = face // 2, face % 2
        return self.zs.at[rnd] if axis == 2 else (self.xs, self.ys)[axis].at[rnd, high]

    def copies(self, rnd, face):
        axis, high = face // 2, face % 2
        src = self.source(rnd, face)
        dst = (self.xr, self.yr, self.zr)[axis]
        return pltpu.make_async_remote_copy(
            src_ref=src, dst_ref=dst.at[rnd, 1 - high],
            send_sem=self.send_sem.at[rnd, face], recv_sem=self.recv_sem.at[rnd, face ^ 1],
            device_id=self.neighbour(face), device_id_type=MESH)

    def send(self, rnd, face):
        @pl.when(self.has[face])
        def _():
            self.copies(rnd, face).start()

    def wait_recv(self, rnd, face):
        axis, high = face // 2, face % 2
        src = self.source(rnd, face)
        dst = (self.xr, self.yr, self.zr)[axis]

        @pl.when(self.has[face])
        def _():
            pltpu.make_async_remote_copy(
                src_ref=src, dst_ref=dst.at[rnd, high],
                send_sem=self.send_sem.at[rnd, face], recv_sem=self.recv_sem.at[rnd, face],
                device_id=self.neighbour(face), device_id_type=MESH).wait_recv()

    def wait_send(self, rnd, face):
        @pl.when(self.has[face])
        def _():
            self.copies(rnd, face).wait_send()


GROUPS = (('gx',), ('gy', 'gz'))


def group_of(comm, group):
    sizes = [comm.counts[AXES.index(name)] for name in group]
    size, rank = 1, 0
    for name, n in zip(group, sizes):
        size, rank = size * n, rank * n + comm.pos[AXES.index(name)]

    def peer(off):
        left, where = lax.rem(rank + off, size), {}
        for name, n in reversed(tuple(zip(group, sizes))):
            where[name], left = lax.rem(left, n), lax.div(left, n)
        return where
    return size, rank, peer


def greet_faces(comm):
    sem = pltpu.get_barrier_semaphore()
    for face in range(FACES):
        @pl.when(comm.has[face])
        def _():
            pl.semaphore_signal(sem, inc=1, device_id=comm.neighbour(face), device_id_type=MESH)
    return sem, sum(flag.astype(jnp.int32) for flag in comm.has)


def greet_groups(comm):
    sem, total = pltpu.get_barrier_semaphore(), 0
    for group in GROUPS:
        size, _, peer = group_of(comm, group)
        for off in range(1, size):
            pl.semaphore_signal(sem, inc=1, device_id=peer(off), device_id_type=MESH)
        total += size - 1
    return sem, total


class Reducer:
    def __init__(self, comm, send_row, recv_rows, send_sem, recv_sem):
        self.comm, self.send_row, self.recv_rows, self.ss, self.rs = comm, send_row, recv_rows, send_sem, recv_sem

    def run(self, row):
        for stage, group in enumerate(GROUPS):
            size, rank, peer = group_of(self.comm, group)
            rows = self.recv_rows[stage]
            self.send_row[stage] = row
            copies = [pltpu.make_async_remote_copy(
                src_ref=self.send_row.at[stage], dst_ref=rows.at[rank], send_sem=self.ss.at[stage, off],
                recv_sem=self.rs.at[stage, off], device_id=peer(off), device_id_type=MESH) for off in range(1, size)]
            for copy in copies:
                copy.start()
            rows[rank] = row
            for copy in copies:
                copy.wait()
            row = total_of(rows[i] for i in range(size))
        return row


def store_plane_faces(comm, rnd, ref, p):
    comm.ys[rnd, 0, p] = ref[p + 1, R0:R0 + 1, :]
    comm.ys[rnd, 1, p] = ref[p + 1, R0 + NY - 1:R0 + NY, :]


def pack_x_faces(comm, rnd, ref):
    half = FOLD
    lane = lane_iota(half)
    a, b = ref[1, R0:R0 + half, :], ref[1, R0 + half:R0 + NY, :]
    comm.xs[rnd, 0] = jnp.where(lane < HALF, a, turn_half(b))
    a, b = ref[NP, R0:R0 + half, :], ref[NP, R0 + half:R0 + NY, :]
    comm.xs[rnd, 1] = jnp.where(lane < HALF, turn_half(a), b)


def face_mask(turn, rows=FOLD):
    return ((lane_iota(rows) + 1) & LOW) < turn


def pack_z(comm, rnd, ref, tree):
    def fold(p, carry):
        low, high = ref[p + 1, R0:R0 + FOLD, :], ref[p + 1, R0 + FOLD:R0 + NY, :]
        tree[p] = jnp.where(face_mask(2), low, spin(high, 2))
        return carry
    lax.fori_loop(0, NP, fold, 0, unroll=NP)
    join_z(comm, rnd, tree)


def join_z(comm, rnd, tree):
    parts = [tree[p] for p in range(NP)]
    for turn in TURNS:
        parts = [jnp.where(face_mask(turn), parts[i], spin(parts[i + 1], turn)) for i in range(0, len(parts), 2)]
    comm.zs[rnd] = parts[0]


def unpack_z(comm, rnd, tree):
    odd = (lane_iota(FOLD) & 1) == 1
    parts = [jnp.where(odd, spin(comm.zr[rnd, 1], LOW - 2), spin(comm.zr[rnd, 0], HALF - 1))]
    for turn in reversed(TURNS):
        parts = [q for part in parts for q in (part, spin(part, LANES - turn))]
    for p in range(NP):
        tree[p] = parts[p]


def spread_z(comm, rnd, tree, ghost):
    unpack_z(comm, rnd, tree)

    def fold(p, carry):
        ghost[p, 0:FOLD, :] = spin(tree[p], 2)
        ghost[p, FOLD:NY, :] = tree[p]
        return carry
    lax.fori_loop(0, NP, fold, 0, unroll=NP)


def inner_planes(ref):
    low = lane_iota(NY) < HALF
    ref[0, R0:R0 + NY, :] = jnp.where(low, 0.0, turn_half(ref[NP, R0:R0 + NY, :]))
    ref[NP + 1, R0:R0 + NY, :] = jnp.where(low, turn_half(ref[1, R0:R0 + NY, :]), 0.0)


def x_ghosts(comm, rnd):
    low = lane_iota(FOLD) < HALF
    lo, hi = comm.xr[rnd, 0], comm.xr[rnd, 1]
    below = [jnp.where(low, lo, 0.0), jnp.where(low, turn_half(lo), 0.0)]
    above = [jnp.where(low, 0.0, turn_half(hi)), jnp.where(low, 0.0, hi)]
    return below, above


def outer_layers(comm, rnd, ref):
    inner_planes(ref)
    below, above = x_ghosts(comm, rnd)
    for i in range(2):
        rows = slice(R0 + FOLD * i, R0 + FOLD * i + FOLD)
        ref[0, rows, :] = ref[0, rows, :] + below[i]
        ref[NP + 1, rows, :] = ref[NP + 1, rows, :] + above[i]
    for p in range(NP):
        ref[p + 1, R0 - 1:R0, :] = comm.yr[rnd, 0, p]
        ref[p + 1, R0 + NY:R0 + NY + 1, :] = comm.yr[rnd, 1, p]


def blank_rows(ref):
    for p in range(NP):
        ref[p + 1, R0 - 1:R0, :] = jnp.zeros((1, LANES), F32)
        ref[p + 1, R0 + NY:R0 + NY + 1, :] = jnp.zeros((1, LANES), F32)


def neighbours(ref, p, t, ghost=None):
    row = R0 + SUB * t
    lane = lane_iota() & LOW
    centre = ref[p + 1, own(t), :]
    xm = ref[p, own(t), :]
    xp = ref[p + 2, own(t), :]
    ym = ref[p + 1, row - 1:row + SUB - 1, :]
    yp = ref[p + 1, row + 1:row + SUB + 1, :]
    zm, zp = spin(centre, 1), spin(centre, LANES - 1)
    if ghost is not None:
        edge = ghost[p, tile(t), :]
        zm, zp = jnp.where(lane == 0, edge, zm), jnp.where(lane == LOW, edge, zp)
    return centre, (xm, xp, ym, yp, zm, zp)


def sweep(body, state=(), unroll=2):
    def plane(p, carry):
        carry = list(carry)
        body(p, carry)
        return tuple(carry)
    return lax.fori_loop(0, NP, plane, tuple(state), unroll=unroll)


def zero_tiles(n):
    return tuple(jnp.zeros(TILE, F32) for _ in range(n))


def send_faces(comm, rnd, ref, tree, folded=False):
    (join_z if folded else functools.partial(pack_z, ref=ref))(comm, rnd, tree=tree)
    for face in (4, 5):
        comm.send(rnd, face)
    pack_x_faces(comm, rnd, ref)
    for p in range(NP):
        store_plane_faces(comm, rnd, ref, p)
    for face in range(4):
        comm.send(rnd, face)


def load_field(raw, ref):
    def body(p, state):
        ref[p + 1, R0:R0 + NY, :] = jnp.concatenate([raw[p], raw[p + NP]], axis=1)
    sweep(body, unroll=NP)


def fill_ghost_conductivity(comm, square, gx_slab, gy_slab, gz_slab):
    px, py, pz = comm.pos
    half = FOLD
    turn = 64 * lax.rem(pz, 2)
    lane = lane_iota(half)
    a, b = pltpu.roll(gx_slab[0:half, :], turn, 1), pltpu.roll(gx_slab[half:NY, :], turn, 1)
    x_face = jnp.where(lane < HALF, a, turn_half(b))
    for end in range(2):
        @pl.when(jnp.logical_not(comm.has[end]))
        def _():
            comm.xr[0, end] = x_face
    rows = pltpu.roll(gy_slab[...], turn, 1)
    y_face = jnp.where(lane_iota(NP) < HALF, rows[0:NP], turn_half(rows[NP:NX]))
    for end in range(2):
        @pl.when(jnp.logical_not(comm.has[2 + end]))
        def _():
            for p in range(NP):
                comm.yr[0, end, p] = y_face[one(p)]
    for end in range(2):
        @pl.when(jnp.logical_not(comm.has[4 + end]))
        def _():
            cols = spin(gz_slab[...], HALF * lax.rem(py, 2))
            shift = 0 if end else LOW
            square[...] = jnp.zeros(square.shape, F32)
            for x in range(NX):
                for c in range(2):
                    square[one((4 * (x % NP) + 2 * c + HALF * (x // NP) + shift) % LANES)] = cols[one(x)]
            turned = square[...].T
            second = ((lane_iota(FOLD) - shift) & 3) == 2
            comm.zr[0, end] = jnp.where(second, turned[FOLD:NY], turned[:FOLD])


def zero_ends(comm, rounds):
    for face in range(FACES):
        @pl.when(jnp.logical_not(comm.has[face]))
        def _():
            buf = (comm.xr, comm.yr, comm.zr)[face // 2]

            def clear(rnd, carry):
                buf[rnd, face % 2] = jnp.zeros(buf.shape[2:], F32)
                return carry
            lax.fori_loop(1, rounds, clear, 0)


def lanes_of(pos):
    return pl.ds(pl.multiple_of(lax.div(pos, 2) * LANES, LANES), LANES)


def start_up(comm, ins, raws, slabs, load_sem):
    k_hbm, g_hbm, f_hbm, u_hbm = ins
    px, py, pz = comm.pos
    loads = [pltpu.make_async_copy(k_hbm, raws[0], load_sem.at[0]),
             pltpu.make_async_copy(u_hbm, raws[1], load_sem.at[1])]
    x_row = jnp.where(comm.has[1], 0, 1)
    y_row = jnp.where(comm.has[3], 2, 3)
    z_row = jnp.where(comm.has[5], 4, 5)
    z_lanes = lanes_of(pz)
    y_lanes = lanes_of(py)
    loads.append(pltpu.make_async_copy(
        g_hbm.at[x_row, pl.ds(pl.multiple_of(py * NY, NY), NY), z_lanes], slabs[0], load_sem.at[2]))
    loads.append(pltpu.make_async_copy(
        g_hbm.at[y_row, pl.ds(pl.multiple_of(px * NX, NX), NX), z_lanes], slabs[1], load_sem.at[3]))
    loads.append(pltpu.make_async_copy(
        g_hbm.at[z_row, pl.ds(pl.multiple_of(px * NX, NX), NX), y_lanes], slabs[2], load_sem.at[4]))
    loads.append(pltpu.make_async_copy(f_hbm, raws[2], load_sem.at[5]))
    for load in loads:
        load.start()
    return loads


def first_exchange(comm, loads, greet, raws, slabs, k_ref, u_ref, tree, square, k_ghost, u_ghost):
    sem, total = greet
    loads[0].wait()
    load_field(raws[0], k_ref)
    pl.semaphore_wait(sem, total)
    send_faces(comm, 0, k_ref, tree)
    loads[1].wait()
    load_field(raws[1], u_ref)
    send_faces(comm, 1, u_ref, tree)
    for load in loads[2:]:
        load.wait()
    fill_ghost_conductivity(comm, square, *slabs)
    for rnd, ref, ghost in ((0, k_ref, k_ghost), (1, u_ref, u_ghost)):
        for face in range(FACES):
            comm.wait_recv(rnd, face)
        outer_layers(comm, rnd, ref)
        spread_z(comm, rnd, tree, ghost)


def first_residual(raw_f, k_ref, u_ref, k_ghost, u_ghost, p, t, d_ref):
    centre, others = neighbours(k_ref, p, t, k_ghost)
    u_own, u_others = neighbours(u_ref, p, t, u_ghost)
    twice = centre + centre
    weights = [twice * other / (centre + other) for other in others]
    diag = total_of(weights)
    au = total_of([w * (u_own - other) for w, other in zip(weights, u_others)])
    f_tile = jnp.concatenate([raw_f[p, tile(t), :], raw_f[p + NP, tile(t), :]], axis=1)
    d_ref[p, tile(t), :] = diag
    return weights, f_tile - au, 1.0 / diag


def write_plane(raw_ref, p, values):
    raw_ref[p] = values[:, :HALF]
    raw_ref[p + NP] = turn_half(values)[:, :HALF]


def dot_rows(a, b):
    prod = a[:2 * SUB] * b[:2 * SUB]
    return row_sum(prod[:SUB] + prod[SUB:])


def solve_coefficients(row, mom_ref, pc_ref, hist_ref, full_ref):
    lane24, line24 = lane_iota(24), row_iota(24)
    wide = jnp.broadcast_to(row, (24, LANES))
    base = lane_sum(jnp.where((lane24 == line24 + 1) & (line24 < 17), wide, 0.0))
    base = jnp.broadcast_to(base, (24, LANES))
    first, second = base[0:1], base[1:2]
    even = (line24 & 1) == 0
    mom = jnp.where(line24 >= 2, 2.0 * base - jnp.where(even, first, second), base)
    mom = jnp.where(line24 < 17, mom, 0.0)
    lane16, line16 = lane_iota(16), row_iota(16)
    wide = jnp.broadcast_to(row, WIDE)
    for k in range(NB):
        big = jnp.maximum(line16, k)
        small = jnp.minimum(line16, k)
        want = GRAM + NB * big + small
        col = lane_sum(jnp.where((lane16 == want) & (line16 < NB), wide, 0.0))
        full_ref[k] = jnp.broadcast_to(col, WIDE)
    zeros8 = jnp.zeros(TILE, F32)
    mom_ref[:SUB] = zeros8
    mom_ref[32:40] = zeros8
    pc_ref[:SUB] = zeros8
    pc_ref[24:32] = zeros8
    unit = jnp.where(line16 == 0, 1.0, 0.0)
    cvec, pvec, avec = unit, unit, jnp.zeros(WIDE, F32)
    rvec, mvec = mom, mom
    mu0 = mom[0:1]
    rho = dot_rows(cvec, rvec)
    ok = jnp.where(rho > 0.0, 1.0, 0.0)
    two_one = jnp.where(line16 == 1, 2.0, 1.0)
    for t in range(CG_ITERS):
        mom_ref[8:32] = mvec
        mom_ref[7:8] = mvec[1:2]
        pc_ref[8:24] = pvec
        qvec = mvec - 0.5 * (mom_ref[9:33] + mom_ref[7:31])
        npvec = 0.5 * (two_one * pc_ref[7:23] + pc_ref[9:25])
        curv = dot_rows(pvec, qvec)
        size = row_sum(jnp.abs(pvec))
        ok = jnp.where(size * size * mu0 < BOUND * curv, ok, 0.0)
        alpha = rho / curv
        avec = avec + alpha * pvec
        cvec = cvec - alpha * (pvec - npvec)
        rvec = rvec - alpha * qvec
        hist_ref[t] = cvec
        rho_new = dot_rows(cvec, rvec)
        size = row_sum(jnp.abs(cvec))
        ok = jnp.where(size * size * mu0 < BOUND * rho_new, ok, 0.0)
        beta = rho_new / rho
        pvec = cvec + beta * pvec
        mvec = rvec + beta * mvec
        rho = rho_new
    return avec, cvec, ok


def squares_row(hist_ref, full_ref):
    lane = lane_iota(1)
    out = jnp.zeros((1, LANES), F32)
    for t in range(CG_ITERS):
        cvec = hist_ref[t]
        acc = full_ref[0] * hist_ref[t, one(0)]
        for j in range(1, NB):
            acc = acc + full_ref[j] * hist_ref[t, one(j)]
        out = jnp.where(lane == t, dot_rows(acc, cvec), out)
    return out


def basis_kernel(counts, k_hbm, g_hbm, f_hbm, u_hbm, u_out, r_out, h_ref, ok_ref,
                 raw_k, raw_u, raw_f, slab_x, slab_y, slab_z, k_ref, u_ref, z_ref, coef_ref, d_ref, sums_ref,
                 mom_ref, pc_ref, hist_ref, full_ref, comb_ref, edge_ref, part_ref, tree, square, k_ghost, u_ghost,
                 xs, ys, zs, xr, yr, zr, send_row, rows_a, rows_b,
                 load_sem, send_sem, recv_sem, red_ss, red_rs):
    comm = Comm(counts, (xs, ys, zs, xr, yr, zr, send_sem, recv_sem))
    raws, slabs = (raw_k, raw_u, raw_f), (slab_x, slab_y, slab_z)
    loads = start_up(comm, (k_hbm, g_hbm, f_hbm, u_hbm), raws, slabs, load_sem)
    greet = greet_faces(comm)
    zero_ends(comm, CG_ITERS + 2)
    sums_ref[...] = jnp.zeros(sums_ref.shape, F32)

    def blank(k, carry):
        blank_rows(z_ref.at[k + 1])
        return carry
    lax.fori_loop(0, CG_ITERS, blank, 0)

    def nothing(p, state):
        z_ref[0, p + 1, R0:R0 + NY, :] = jnp.zeros((NY, LANES), F32)
    sweep(nothing, unroll=4)
    first_exchange(comm, loads, greet, raws, slabs, k_ref, u_ref, tree, square, k_ghost, u_ghost)

    def first(p, state):
        lane = lane_iota() & LOW
        for t in range(ROWS):
            weights, resid, inv = first_residual(raw_f, k_ref, u_ref, k_ghost, u_ghost, p, t, d_ref)
            factor = inv + inv
            scaled = [w * factor for w in weights]
            low, high = scaled[4:]
            edge_ref[p, tile(t), :] = jnp.where(lane == 0, low, jnp.where(lane == LOW, high, 0.0))
            scaled[4:] = jnp.where(lane == 0, 0.0, low), jnp.where(lane == LOW, 0.0, high)
            for i in range(FACES):
                coef_ref[p, t, i] = scaled[i]
            z_ref[1, p + 1, own(t), :] = resid * inv

    sweep(first, unroll=4)
    send_faces(comm, 2, z_ref.at[1], tree)

    def products(k):
        def body(p, accs):
            for t in range(ROWS):
                d = d_ref[p, tile(t), :]
                z_k = z_ref[k + 1, p + 1, own(t), :]
                dz = d * z_k
                ddz = d * dz
                for i in range(NB):
                    accs[i] = accs[i] + ddz * z_ref[i + 1, p + 1, own(t), :]
                accs[NB] = accs[NB] + dz * z_k
                accs[NB + 1] = accs[NB + 1] + dz * z_ref[k, p + 1, own(t), :]
        accs = sweep(body, zero_tiles(NB + 2))
        rows = [GRAM + NB * k + i for i in range(NB)] + [2 * k + 1, 2 * k]
        for row, acc in zip(rows, accs):
            sums_ref[pl.ds(row, 1), :] = row_sum(acc)

    def weight(k):
        return jnp.where(k == 0, 0.5, 1.0)

    def late_terms(k, rnd):
        ref, factor = z_ref.at[k + 2], weight(k)
        unpack_z(comm, rnd, tree)
        below, above = x_ghosts(comm, rnd)
        for t in range(ROWS):
            part = slice(SUB * (t % 4), SUB * (t % 4) + SUB)
            for plane, face, layer in ((1, 0, below), (NP, 1, above)):
                term = coef_ref[plane - 1, t, face] * layer[t // 4][part]
                part_ref[plane - 1, tile(t), :] = part_ref[plane - 1, tile(t), :] + factor * term

        first, last = row_iota(SUB) == 0, row_iota(SUB) == SUB - 1

        def body(p, state):
            turned = [spin(tree[p], 2), tree[p]]
            news = []
            for t in range(ROWS):
                part = slice(SUB * (t % 4), SUB * (t % 4) + SUB)
                term = edge_ref[p, tile(t), :] * turned[t // 4][part]
                for end, at, sub, mask in ((0, 0, 0, first), (1, ROWS - 1, SUB - 1, last)):
                    if t == at:
                        line = coef_ref[p, t, 2 + end, one(sub), :] * comm.yr[rnd, end, p]
                        term = term + jnp.where(mask, line, 0.0)
                news.append(part_ref[p, tile(t), :] + factor * term)
                ref[p + 1, own(t), :] = news[t]
            for t in range(4):
                tree[p, tile(t), :] = jnp.where(face_mask(2, SUB), news[t], spin(news[t + 4], 2))
        sweep(body, unroll=NP)

    def apply(k, carry):
        rnd, factor = k + 2, weight(k)
        ref = z_ref.at[k + 1]
        inner_planes(ref)

        def step(p, state):
            for t in range(ROWS):
                _, others = neighbours(ref, p, t)
                total = total_of(coef_ref[p, t, i] * others[i] for i in range(FACES))
                part_ref[p, tile(t), :] = factor * total - z_ref[k, p + 1, own(t), :]

        sweep(step)
        products(k)
        for face in range(FACES):
            comm.wait_recv(rnd, face)
        late_terms(k, rnd)

        @pl.when(k < CG_ITERS - 1)
        def _():
            send_faces(comm, rnd + 1, z_ref.at[k + 2], tree, folded=True)
        return carry

    lax.fori_loop(0, CG_ITERS, apply, 0)
    products(CG_ITERS)

    total = jnp.broadcast_to(lane_sum(sums_ref[...]), (LANES, LANES))
    row = row_sum(jnp.where(lane_iota(LANES) == row_iota(LANES), total, 0.0))
    red = Reducer(comm, send_row, (rows_a, rows_b), red_ss, red_rs)
    row = red.run(row)
    avec, cvec, ok = solve_coefficients(row, mom_ref, pc_ref, hist_ref, full_ref)
    comb_ref[0] = avec
    comb_ref[1] = cvec

    a_co = [jnp.broadcast_to(comb_ref[0, one(i)], TILE) for i in range(CG_ITERS)]
    c_co = [jnp.broadcast_to(comb_ref[1, one(i)], TILE) for i in range(NB)]

    def combine(p, carry):
        for t in range(ROWS):
            row = own(t)
            rows = tile(t)
            basis = [z_ref[i + 1, p + 1, row, :] for i in range(NB)]
            ut, rt = a_co[0] * basis[0], c_co[0] * basis[0]
            for i in range(1, NB):
                if i < CG_ITERS:
                    ut = ut + a_co[i] * basis[i]
                rt = rt + c_co[i] * basis[i]
            ut = u_ref[p + 1, row, :] + ut
            rt = d_ref[p, rows, :] * rt
            u_out[p, rows, :] = ut[:, :HALF]
            u_out[p + NP, rows, :] = turn_half(ut)[:, :HALF]
            r_out[p, rows, :] = rt[:, :HALF]
            r_out[p + NP, rows, :] = turn_half(rt)[:, :HALF]
        return carry

    lax.fori_loop(0, NP, combine, 0, unroll=4)
    h_ref[...] = squares_row(hist_ref, full_ref)
    ok_ref[0, 0] = ok[0, 0].astype(jnp.int32)

    def drain(rnd, carry):
        for face in range(FACES):
            comm.wait_send(rnd, face)
        return carry
    lax.fori_loop(0, CG_ITERS + 2, drain, 0)


def plain_kernel(counts, k_hbm, g_hbm, f_hbm, u_hbm, u_out, r_out, h_ref,
                 raw_k, raw_u, raw_f, slab_x, slab_y, slab_z, k_ref, u_ref, p_ref, q_ref, r_ref, coef_ref, d_ref, tree, square, k_ghost, u_ghost,
                 xs, ys, zs, xr, yr, zr, send_row, rows_a, rows_b,
                 load_sem, send_sem, recv_sem, red_ss, red_rs):
    comm = Comm(counts, (xs, ys, zs, xr, yr, zr, send_sem, recv_sem))
    raws, slabs = (raw_k, raw_u, raw_f), (slab_x, slab_y, slab_z)
    loads = start_up(comm, (k_hbm, g_hbm, f_hbm, u_hbm), raws, slabs, load_sem)
    greet = greet_groups(comm)
    zero_ends(comm, 3)
    first_exchange(comm, loads, greet, raws, slabs, k_ref, u_ref, tree, square, k_ghost, u_ghost)
    red = [Reducer(comm, send_row.at[i], (rows_a.at[i], rows_b.at[i]), red_ss.at[i], red_rs.at[i]) for i in range(2)]

    def reduce(which, accs):
        lane = lane_iota(1)
        row = jnp.zeros((1, LANES), F32)
        for i, acc in enumerate(accs):
            total = row_sum(lane_sum(acc))
            row = jnp.where(lane == i, jnp.broadcast_to(total, (1, LANES)), row)
        row = red[which].run(row)
        return [lane_sum(jnp.where(lane == i, row, 0.0)) for i in range(len(accs))]

    def first(p, state):
        for t in range(ROWS):
            weights, resid, inv = first_residual(raw_f, k_ref, u_ref, k_ghost, u_ghost, p, t, d_ref)
            for i in range(FACES):
                coef_ref[p, t, i] = weights[i]
            r_ref[p, tile(t), :] = resid
            z_new = resid * inv
            p_ref[p + 1, own(t), :] = z_new
            state[0] = state[0] + resid * z_new

    rho, = reduce(0, sweep(first, zero_tiles(1)))

    def iteration(it, carry):
        rho, hist = carry

        send_faces(comm, 2, p_ref, tree)
        for face in range(FACES):
            comm.wait_recv(2, face)
            comm.wait_send(2, face)
        outer_layers(comm, 2, p_ref)
        spread_z(comm, 2, tree, k_ghost)

        def apply(p, state):
            for t in range(ROWS):
                centre, others = neighbours(p_ref, p, t, k_ghost)
                q = total_of(coef_ref[p, t, i] * (centre - others[i]) for i in range(FACES))
                q_ref[p, tile(t), :] = q
                state[0] = state[0] + centre * q

        curv, = reduce(1, sweep(apply, zero_tiles(1)))
        alpha = jnp.broadcast_to(rho / curv, TILE)

        def update(p, accs):
            acc_z, acc_r = accs
            for t in range(ROWS):
                row = own(t)
                rows = tile(t)
                u_ref[p + 1, row, :] = u_ref[p + 1, row, :] + alpha * p_ref[p + 1, row, :]
                resid = r_ref[p, rows, :] - alpha * q_ref[p, rows, :]
                r_ref[p, rows, :] = resid
                acc_z = acc_z + resid * (resid / d_ref[p, rows, :])
                acc_r = acc_r + resid * resid
            return acc_z, acc_r

        rho_new, rr = reduce(0, lax.fori_loop(0, NP, update, zero_tiles(2)))
        beta = jnp.broadcast_to(rho_new / rho, TILE)

        def turn(p, carry):
            for t in range(ROWS):
                row = own(t)
                rows = tile(t)
                p_ref[p + 1, row, :] = r_ref[p, rows, :] / d_ref[p, rows, :] + beta * p_ref[p + 1, row, :]
            return carry

        lax.fori_loop(0, NP, turn, 0)
        hist = jnp.where(lane_iota(1) == it, jnp.broadcast_to(rr, (1, LANES)), hist)
        return rho_new, hist

    _, hist = lax.fori_loop(0, CG_ITERS, iteration, (rho, jnp.zeros((1, LANES), F32)))
    h_ref[...] = hist

    def finish(p, carry):
        write_plane(u_out, p, u_ref[p + 1, R0:R0 + NY, :])
        write_plane(r_out, p, r_ref[p])
        return carry

    lax.fori_loop(0, NP, finish, 0)
    for rnd in range(2):
        for face in range(FACES):
            comm.wait_send(rnd, face)


def scratch_for(kind, counts):
    field = (NP + 2, NY + 16, LANES)
    block = (NP, NY, LANES)
    vm = lambda *shape: pltpu.VMEM(shape, F32)
    raws = [vm(NX, NY, NZ)] * 3 + [vm(NY, LANES), vm(NX, LANES), vm(NX, LANES)]
    if kind == 'basis':
        rounds, reds = CG_ITERS + 2, ()
        work = [vm(*field), vm(*field), vm(NB + 1, *field), vm(NP, ROWS, FACES, *TILE), vm(*block), vm(LANES, LANES),
                vm(40, LANES), vm(32, LANES), vm(CG_ITERS, 16, LANES), vm(NB, 16, LANES), vm(2, 16, LANES), vm(*block), vm(*block)]
    else:
        rounds, reds = 3, (2,)
        work = [vm(*field), vm(*field), vm(*field), vm(*block), vm(*block), vm(NP, ROWS, FACES, *TILE), vm(*block)]
    work += [vm(NP, FOLD, LANES), vm(LANES, LANES), vm(*block), vm(*block)]
    sides = [vm(rounds, 2, FOLD, LANES), vm(rounds, 2, NP, 1, LANES)]
    faces = sides + [vm(rounds, FOLD, LANES)] + sides + [vm(rounds, 2, FOLD, LANES)]
    sizes = [counts[0], counts[1] * counts[2]]
    rows = [vm(*reds, 2, 1, LANES)] + [vm(*reds, n, 1, LANES) for n in sizes]
    dma = pltpu.SemaphoreType.DMA
    sems = [dma((6,)), dma((rounds, 6)), dma((rounds, 6)), dma((*reds, 2, max(sizes))), dma((*reds, 2, max(sizes)))]
    return raws + work + faces + rows + sems


def solution(mesh):
    counts = tuple(mesh.shape[name] for name in AXES)
    grid_spec = P(*AXES)
    block = jax.ShapeDtypeStruct((NX, NY, NZ), F32)

    def call(kernel, kind, ident, *more):
        hbm, vmem = pl.BlockSpec(memory_space=pltpu.HBM), pl.BlockSpec(memory_space=pltpu.VMEM)
        smem = [pl.BlockSpec(memory_space=pltpu.SMEM)] * len(more)
        return pl.pallas_call(
            functools.partial(kernel, counts),
            out_shape=(block, block, jax.ShapeDtypeStruct((1, LANES), F32), *more),
            in_specs=[hbm] * 4,
            out_specs=(vmem, vmem, vmem, *smem),
            scratch_shapes=scratch_for(kind, counts),
            compiler_params=pltpu.CompilerParams(collective_id=ident, has_side_effects=True, vmem_limit_bytes=VMEM_BYTES),
            name=kind,
        )

    def local_solve(k_cell, k_ghost, f_rhs, u_init):
        args = (k_cell, k_ghost, f_rhs, u_init)
        *fast, ok = call(basis_kernel, 'basis', 0, jax.ShapeDtypeStruct((1, 1), jnp.int32))(*args)
        u_out, r_out, row = lax.cond(ok[0, 0] > 0, lambda: tuple(fast),
                                     lambda: tuple(call(plain_kernel, 'plain', 1)(*args)))
        return u_out, r_out, row[0, 0:CG_ITERS]

    return jax.shard_map(local_solve, mesh=mesh, in_specs=(grid_spec, P(), grid_spec, grid_spec),
                         out_specs=(grid_spec, grid_spec, P()), check_vma=False)
```

```python
import functools

import jax
import jax.numpy as jnp
from jax import lax
from jax.experimental import pallas as pl
from jax.experimental.pallas import tpu as pltpu
from jax.sharding import PartitionSpec as P

CG_ITERS = 8
NB = CG_ITERS + 1
NX, NY, NZ = 32, 64, 64
NP = NX // 2
R0 = 8
MESH = pl.DeviceIdType.MESH
AXES = ('gx', 'gy', 'gz')
BOUND = 4096.0
GRAM = 2 * NB
VMEM_BYTES = 60_000_000
F32 = jnp.float32
SUB, LANES, HALF, LOW = 8, 128, 64, 63
ROWS = NY // SUB
TILE = (SUB, LANES)
WIDE = (2 * SUB, LANES)
FACES = 6
FOLD = NY // 2
TURNS = (4, 8, 16, 32)


def own(t):
    return slice(R0 + SUB * t, R0 + SUB * t + SUB)


def tile(t):
    return slice(SUB * t, SUB * t + SUB)


def one(i):
    return slice(i, i + 1)


def spin(values, by):
    return pltpu.roll(values, by, 1)


def turn_half(values):
    return spin(values, HALF)


def row_sum(values):
    return jnp.sum(values, axis=0, keepdims=True)


def lane_sum(values):
    return jnp.sum(values, axis=1, keepdims=True)


def total_of(parts):
    parts = list(parts)
    while len(parts) > 1:
        parts = [sum(parts[i + 1:i + 2], parts[i]) for i in range(0, len(parts), 2)]
    return parts[0]


def lane_iota(rows=8):
    return lax.broadcasted_iota(jnp.int32, (rows, LANES), 1)


def row_iota(rows):
    return lax.broadcasted_iota(jnp.int32, (rows, LANES), 0)


class Comm:
    def __init__(self, counts, bufs):
        self.counts = counts
        self.pos = [lax.axis_index(name) for name in AXES]
        self.has = []
        for axis in range(3):
            self.has.append(self.pos[axis] > 0)
            self.has.append(self.pos[axis] < counts[axis] - 1)
        (self.xs, self.ys, self.zs, self.xr, self.yr, self.zr, self.send_sem, self.recv_sem) = bufs

    def neighbour(self, face):
        return {AXES[face // 2]: self.pos[face // 2] + (1 if face % 2 else -1)}

    def source(self, rnd, face):
        axis, high = face // 2, face % 2
        return self.zs.at[rnd] if axis == 2 else (self.xs, self.ys)[axis].at[rnd, high]

    def copies(self, rnd, face):
        axis, high = face // 2, face % 2
        src = self.source(rnd, face)
        dst = (self.xr, self.yr, self.zr)[axis]
        return pltpu.make_async_remote_copy(
            src_ref=src, dst_ref=dst.at[rnd, 1 - high],
            send_sem=self.send_sem.at[rnd, face], recv_sem=self.recv_sem.at[rnd, face ^ 1],
            device_id=self.neighbour(face), device_id_type=MESH)

    def send(self, rnd, face):
        @pl.when(self.has[face])
        def _():
            self.copies(rnd, face).start()

    def wait_recv(self, rnd, face):
        axis, high = face // 2, face % 2
        src = self.source(rnd, face)
        dst = (self.xr, self.yr, self.zr)[axis]

        @pl.when(self.has[face])
        def _():
            pltpu.make_async_remote_copy(
                src_ref=src, dst_ref=dst.at[rnd, high],
                send_sem=self.send_sem.at[rnd, face], recv_sem=self.recv_sem.at[rnd, face],
                device_id=self.neighbour(face), device_id_type=MESH).wait_recv()

    def wait_send(self, rnd, face):
        @pl.when(self.has[face])
        def _():
            self.copies(rnd, face).wait_send()


GROUPS = (('gx',), ('gy', 'gz'))


def group_of(comm, group):
    sizes = [comm.counts[AXES.index(name)] for name in group]
    size, rank = 1, 0
    for name, n in zip(group, sizes):
        size, rank = size * n, rank * n + comm.pos[AXES.index(name)]

    def peer(off):
        left, where = lax.rem(rank + off, size), {}
        for name, n in reversed(tuple(zip(group, sizes))):
            where[name], left = lax.rem(left, n), lax.div(left, n)
        return where
    return size, rank, peer


def greet_faces(comm):
    sem = pltpu.get_barrier_semaphore()
    for face in range(FACES):
        @pl.when(comm.has[face])
        def _():
            pl.semaphore_signal(sem, inc=1, device_id=comm.neighbour(face), device_id_type=MESH)
    return sem, sum(flag.astype(jnp.int32) for flag in comm.has)


def greet_groups(comm):
    sem, total = pltpu.get_barrier_semaphore(), 0
    for group in GROUPS:
        size, _, peer = group_of(comm, group)
        for off in range(1, size):
            pl.semaphore_signal(sem, inc=1, device_id=peer(off), device_id_type=MESH)
        total += size - 1
    return sem, total


class Reducer:
    def __init__(self, comm, send_row, recv_rows, send_sem, recv_sem):
        self.comm, self.send_row, self.recv_rows, self.ss, self.rs = comm, send_row, recv_rows, send_sem, recv_sem

    def run(self, row):
        for stage, group in enumerate(GROUPS):
            size, rank, peer = group_of(self.comm, group)
            rows = self.recv_rows[stage]
            self.send_row[stage] = row
            copies = [pltpu.make_async_remote_copy(
                src_ref=self.send_row.at[stage], dst_ref=rows.at[rank], send_sem=self.ss.at[stage, off],
                recv_sem=self.rs.at[stage, off], device_id=peer(off), device_id_type=MESH) for off in range(1, size)]
            for copy in copies:
                copy.start()
            rows[rank] = row
            for copy in copies:
                copy.wait()
            row = total_of(rows[i] for i in range(size))
        return row


def store_plane_faces(comm, rnd, ref, p):
    comm.ys[rnd, 0, p] = ref[p + 1, R0:R0 + 1, :]
    comm.ys[rnd, 1, p] = ref[p + 1, R0 + NY - 1:R0 + NY, :]


def pack_x_faces(comm, rnd, ref):
    half = FOLD
    lane = lane_iota(half)
    a, b = ref[1, R0:R0 + half, :], ref[1, R0 + half:R0 + NY, :]
    comm.xs[rnd, 0] = jnp.where(lane < HALF, a, turn_half(b))
    a, b = ref[NP, R0:R0 + half, :], ref[NP, R0 + half:R0 + NY, :]
    comm.xs[rnd, 1] = jnp.where(lane < HALF, turn_half(a), b)


def face_mask(turn, rows=FOLD):
    return ((lane_iota(rows) + 1) & LOW) < turn


def pack_z(comm, rnd, ref, tree):
    def fold(p, carry):
        low, high = ref[p + 1, R0:R0 + FOLD, :], ref[p + 1, R0 + FOLD:R0 + NY, :]
        tree[p] = jnp.where(face_mask(2), low, spin(high, 2))
        return carry
    lax.fori_loop(0, NP, fold, 0, unroll=NP)
    join_z(comm, rnd, tree)


def join_z(comm, rnd, tree):
    parts = [tree[p] for p in range(NP)]
    for turn in TURNS:
        parts = [jnp.where(face_mask(turn), parts[i], spin(parts[i + 1], turn)) for i in range(0, len(parts), 2)]
    comm.zs[rnd] = parts[0]


def unpack_z(comm, rnd, tree):
    odd = (lane_iota(FOLD) & 1) == 1
    parts = [jnp.where(odd, spin(comm.zr[rnd, 1], LOW - 2), spin(comm.zr[rnd, 0], HALF - 1))]
    for turn in reversed(TURNS):
        parts = [q for part in parts for q in (part, spin(part, LANES - turn))]
    for p in range(NP):
        tree[p] = parts[p]


def spread_z(comm, rnd, tree, ghost):
    unpack_z(comm, rnd, tree)

    def fold(p, carry):
        ghost[p, 0:FOLD, :] = spin(tree[p], 2)
        ghost[p, FOLD:NY, :] = tree[p]
        return carry
    lax.fori_loop(0, NP, fold, 0, unroll=NP)


def inner_planes(ref):
    low = lane_iota(NY) < HALF
    ref[0, R0:R0 + NY, :] = jnp.where(low, 0.0, turn_half(ref[NP, R0:R0 + NY, :]))
    ref[NP + 1, R0:R0 + NY, :] = jnp.where(low, turn_half(ref[1, R0:R0 + NY, :]), 0.0)


def x_ghosts(comm, rnd):
    low = lane_iota(FOLD) < HALF
    lo, hi = comm.xr[rnd, 0], comm.xr[rnd, 1]
    below = [jnp.where(low, lo, 0.0), jnp.where(low, turn_half(lo), 0.0)]
    above = [jnp.where(low, 0.0, turn_half(hi)), jnp.where(low, 0.0, hi)]
    return below, above


def outer_layers(comm, rnd, ref):
    inner_planes(ref)
    below, above = x_ghosts(comm, rnd)
    for i in range(2):
        rows = slice(R0 + FOLD * i, R0 + FOLD * i + FOLD)
        ref[0, rows, :] = ref[0, rows, :] + below[i]
        ref[NP + 1, rows, :] = ref[NP + 1, rows, :] + above[i]
    for p in range(NP):
        ref[p + 1, R0 - 1:R0, :] = comm.yr[rnd, 0, p]
        ref[p + 1, R0 + NY:R0 + NY + 1, :] = comm.yr[rnd, 1, p]


def blank_rows(ref):
    for p in range(NP):
        ref[p + 1, R0 - 1:R0, :] = jnp.zeros((1, LANES), F32)
        ref[p + 1, R0 + NY:R0 + NY + 1, :] = jnp.zeros((1, LANES), F32)


def neighbours(ref, p, t, ghost=None):
    row = R0 + SUB * t
    lane = lane_iota() & LOW
    centre = ref[p + 1, own(t), :]
    xm = ref[p, own(t), :]
    xp = ref[p + 2, own(t), :]
    ym = ref[p + 1, row - 1:row + SUB - 1, :]
    yp = ref[p + 1, row + 1:row + SUB + 1, :]
    zm, zp = spin(centre, 1), spin(centre, LANES - 1)
    if ghost is not None:
        edge = ghost[p, tile(t), :]
        zm, zp = jnp.where(lane == 0, edge, zm), jnp.where(lane == LOW, edge, zp)
    return centre, (xm, xp, ym, yp, zm, zp)


def sweep(body, state=(), unroll=2):
    def plane(p, carry):
        carry = list(carry)
        body(p, carry)
        return tuple(carry)
    return lax.fori_loop(0, NP, plane, tuple(state), unroll=unroll)


def zero_tiles(n):
    return tuple(jnp.zeros(TILE, F32) for _ in range(n))


def send_faces(comm, rnd, ref, tree, folded=False):
    (join_z if folded else functools.partial(pack_z, ref=ref))(comm, rnd, tree=tree)
    for face in (4, 5):
        comm.send(rnd, face)
    pack_x_faces(comm, rnd, ref)
    for p in range(NP):
        store_plane_faces(comm, rnd, ref, p)
    for face in range(4):
        comm.send(rnd, face)


def load_field(raw, ref):
    def body(p, state):
        ref[p + 1, R0:R0 + NY, :] = jnp.concatenate([raw[p], raw[p + NP]], axis=1)
    sweep(body, unroll=NP)


def fill_ghost_conductivity(comm, square, gx_slab, gy_slab, gz_slab):
    px, py, pz = comm.pos
    half = FOLD
    turn = 64 * lax.rem(pz, 2)
    lane = lane_iota(half)
    a, b = pltpu.roll(gx_slab[0:half, :], turn, 1), pltpu.roll(gx_slab[half:NY, :], turn, 1)
    x_face = jnp.where(lane < HALF, a, turn_half(b))
    for end in range(2):
        @pl.when(jnp.logical_not(comm.has[end]))
        def _():
            comm.xr[0, end] = x_face
    rows = pltpu.roll(gy_slab[...], turn, 1)
    y_face = jnp.where(lane_iota(NP) < HALF, rows[0:NP], turn_half(rows[NP:NX]))
    for end in range(2):
        @pl.when(jnp.logical_not(comm.has[2 + end]))
        def _():
            for p in range(NP):
                comm.yr[0, end, p] = y_face[one(p)]
    for end in range(2):
        @pl.when(jnp.logical_not(comm.has[4 + end]))
        def _():
            cols = spin(gz_slab[...], HALF * lax.rem(py, 2))
            shift = 0 if end else LOW
            square[...] = jnp.zeros(square.shape, F32)
            for x in range(NX):
                for c in range(2):
                    square[one((4 * (x % NP) + 2 * c + HALF * (x // NP) + shift) % LANES)] = cols[one(x)]
            turned = square[...].T
            second = ((lane_iota(FOLD) - shift) & 3) == 2
            comm.zr[0, end] = jnp.where(second, turned[FOLD:NY], turned[:FOLD])


def zero_ends(comm, rounds):
    for face in range(FACES):
        @pl.when(jnp.logical_not(comm.has[face]))
        def _():
            buf = (comm.xr, comm.yr, comm.zr)[face // 2]

            def clear(rnd, carry):
                buf[rnd, face % 2] = jnp.zeros(buf.shape[2:], F32)
                return carry
            lax.fori_loop(1, rounds, clear, 0)


def lanes_of(pos):
    return pl.ds(pl.multiple_of(lax.div(pos, 2) * LANES, LANES), LANES)


def start_up(comm, ins, raws, slabs, load_sem):
    k_hbm, g_hbm, f_hbm, u_hbm = ins
    px, py, pz = comm.pos
    loads = [pltpu.make_async_copy(k_hbm, raws[0], load_sem.at[0]),
             pltpu.make_async_copy(u_hbm, raws[1], load_sem.at[1])]
    x_row = jnp.where(comm.has[1], 0, 1)
    y_row = jnp.where(comm.has[3], 2, 3)
    z_row = jnp.where(comm.has[5], 4, 5)
    z_lanes = lanes_of(pz)
    y_lanes = lanes_of(py)
    loads.append(pltpu.make_async_copy(
        g_hbm.at[x_row, pl.ds(pl.multiple_of(py * NY, NY), NY), z_lanes], slabs[0], load_sem.at[2]))
    loads.append(pltpu.make_async_copy(
        g_hbm.at[y_row, pl.ds(pl.multiple_of(px * NX, NX), NX), z_lanes], slabs[1], load_sem.at[3]))
    loads.append(pltpu.make_async_copy(
        g_hbm.at[z_row, pl.ds(pl.multiple_of(px * NX, NX), NX), y_lanes], slabs[2], load_sem.at[4]))
    loads.append(pltpu.make_async_copy(f_hbm, raws[2], load_sem.at[5]))
    for load in loads:
        load.start()
    return loads


def first_exchange(comm, loads, greet, raws, slabs, k_ref, u_ref, tree, square, k_ghost, u_ghost):
    sem, total = greet
    loads[0].wait()
    load_field(raws[0], k_ref)
    pl.semaphore_wait(sem, total)
    send_faces(comm, 0, k_ref, tree)
    loads[1].wait()
    load_field(raws[1], u_ref)
    send_faces(comm, 1, u_ref, tree)
    for load in loads[2:]:
        load.wait()
    fill_ghost_conductivity(comm, square, *slabs)
    for rnd, ref, ghost in ((0, k_ref, k_ghost), (1, u_ref, u_ghost)):
        for face in range(FACES):
            comm.wait_recv(rnd, face)
        outer_layers(comm, rnd, ref)
        spread_z(comm, rnd, tree, ghost)


def first_residual(raw_f, k_ref, u_ref, k_ghost, u_ghost, p, t, d_ref):
    centre, others = neighbours(k_ref, p, t, k_ghost)
    u_own, u_others = neighbours(u_ref, p, t, u_ghost)
    twice = centre + centre
    weights = [twice * other / (centre + other) for other in others]
    diag = total_of(weights)
    au = total_of([w * (u_own - other) for w, other in zip(weights, u_others)])
    f_tile = jnp.concatenate([raw_f[p, tile(t), :], raw_f[p + NP, tile(t), :]], axis=1)
    d_ref[p, tile(t), :] = diag
    return weights, f_tile - au, 1.0 / diag


def write_plane(raw_ref, p, values):
    raw_ref[p] = values[:, :HALF]
    raw_ref[p + NP] = turn_half(values)[:, :HALF]


def dot_rows(a, b):
    prod = a[:2 * SUB] * b[:2 * SUB]
    return row_sum(prod[:SUB] + prod[SUB:])


def solve_coefficients(row, mom_ref, pc_ref, hist_ref, full_ref):
    lane24, line24 = lane_iota(24), row_iota(24)
    wide = jnp.broadcast_to(row, (24, LANES))
    base = lane_sum(jnp.where((lane24 == line24 + 1) & (line24 < 17), wide, 0.0))
    base = jnp.broadcast_to(base, (24, LANES))
    first, second = base[0:1], base[1:2]
    even = (line24 & 1) == 0
    mom = jnp.where(line24 >= 2, 2.0 * base - jnp.where(even, first, second), base)
    mom = jnp.where(line24 < 17, mom, 0.0)
    lane16, line16 = lane_iota(16), row_iota(16)
    wide = jnp.broadcast_to(row, WIDE)
    for k in range(NB):
        big = jnp.maximum(line16, k)
        small = jnp.minimum(line16, k)
        want = GRAM + NB * big + small
        col = lane_sum(jnp.where((lane16 == want) & (line16 < NB), wide, 0.0))
        full_ref[k] = jnp.broadcast_to(col, WIDE)
    zeros8 = jnp.zeros(TILE, F32)
    mom_ref[:SUB] = zeros8
    mom_ref[32:40] = zeros8
    pc_ref[:SUB] = zeros8
    pc_ref[24:32] = zeros8
    unit = jnp.where(line16 == 0, 1.0, 0.0)
    cvec, pvec, avec = unit, unit, jnp.zeros(WIDE, F32)
    rvec, mvec = mom, mom
    mu0 = mom[0:1]
    rho = dot_rows(cvec, rvec)
    ok = jnp.where(rho > 0.0, 1.0, 0.0)
    two_one = jnp.where(line16 == 1, 2.0, 1.0)
    for t in range(CG_ITERS):
        mom_ref[8:32] = mvec
        mom_ref[7:8] = mvec[1:2]
        pc_ref[8:24] = pvec
        qvec = mvec - 0.5 * (mom_ref[9:33] + mom_ref[7:31])
        npvec = 0.5 * (two_one * pc_ref[7:23] + pc_ref[9:25])
        curv = dot_rows(pvec, qvec)
        size = row_sum(jnp.abs(pvec))
        ok = jnp.where(size * size * mu0 < BOUND * curv, ok, 0.0)
        alpha = rho / curv
        avec = avec + alpha * pvec
        cvec = cvec - alpha * (pvec - npvec)
        rvec = rvec - alpha * qvec
        hist_ref[t] = cvec
        rho_new = dot_rows(cvec, rvec)
        size = row_sum(jnp.abs(cvec))
        ok = jnp.where(size * size * mu0 < BOUND * rho_new, ok, 0.0)
        beta = rho_new / rho
        pvec = cvec + beta * pvec
        mvec = rvec + beta * mvec
        rho = rho_new
    return avec, cvec, ok


def squares_row(hist_ref, full_ref):
    lane = lane_iota(1)
    out = jnp.zeros((1, LANES), F32)
    for t in range(CG_ITERS):
        cvec = hist_ref[t]
        acc = full_ref[0] * hist_ref[t, one(0)]
        for j in range(1, NB):
            acc = acc + full_ref[j] * hist_ref[t, one(j)]
        out = jnp.where(lane == t, dot_rows(acc, cvec), out)
    return out


def basis_kernel(counts, k_hbm, g_hbm, f_hbm, u_hbm, u_out, r_out, h_ref, ok_ref,
                 raw_k, raw_u, raw_f, slab_x, slab_y, slab_z, k_ref, u_ref, z_ref, coef_ref, d_ref, sums_ref,
                 mom_ref, pc_ref, hist_ref, full_ref, comb_ref, edge_ref, part_ref, tree, square, k_ghost, u_ghost,
                 xs, ys, zs, xr, yr, zr, send_row, rows_a, rows_b,
                 load_sem, send_sem, recv_sem, red_ss, red_rs):
    comm = Comm(counts, (xs, ys, zs, xr, yr, zr, send_sem, recv_sem))
    raws, slabs = (raw_k, raw_u, raw_f), (slab_x, slab_y, slab_z)
    loads = start_up(comm, (k_hbm, g_hbm, f_hbm, u_hbm), raws, slabs, load_sem)
    greet = greet_faces(comm)
    zero_ends(comm, CG_ITERS + 2)
    sums_ref[...] = jnp.zeros(sums_ref.shape, F32)

    def blank(k, carry):
        blank_rows(z_ref.at[k + 1])
        return carry
    lax.fori_loop(0, CG_ITERS, blank, 0)

    def nothing(p, state):
        z_ref[0, p + 1, R0:R0 + NY, :] = jnp.zeros((NY, LANES), F32)
    sweep(nothing, unroll=4)
    first_exchange(comm, loads, greet, raws, slabs, k_ref, u_ref, tree, square, k_ghost, u_ghost)

    def first(p, state):
        lane = lane_iota() & LOW
        for t in range(ROWS):
            weights, resid, inv = first_residual(raw_f, k_ref, u_ref, k_ghost, u_ghost, p, t, d_ref)
            factor = inv + inv
            scaled = [w * factor for w in weights]
            low, high = scaled[4:]
            edge_ref[p, tile(t), :] = jnp.where(lane == 0, low, jnp.where(lane == LOW, high, 0.0))
            scaled[4:] = jnp.where(lane == 0, 0.0, low), jnp.where(lane == LOW, 0.0, high)
            for i in range(FACES):
                coef_ref[p, t, i] = scaled[i]
            z_ref[1, p + 1, own(t), :] = resid * inv

    sweep(first, unroll=4)
    send_faces(comm, 2, z_ref.at[1], tree)

    def products(k):
        def body(p, accs):
            for t in range(ROWS):
                d = d_ref[p, tile(t), :]
                z_k = z_ref[k + 1, p + 1, own(t), :]
                dz = d * z_k
                ddz = d * dz
                for i in range(NB):
                    accs[i] = accs[i] + ddz * z_ref[i + 1, p + 1, own(t), :]
                accs[NB] = accs[NB] + dz * z_k
                accs[NB + 1] = accs[NB + 1] + dz * z_ref[k, p + 1, own(t), :]
        accs = sweep(body, zero_tiles(NB + 2))
        rows = [GRAM + NB * k + i for i in range(NB)] + [2 * k + 1, 2 * k]
        for row, acc in zip(rows, accs):
            sums_ref[pl.ds(row, 1), :] = row_sum(acc)

    def weight(k):
        return jnp.where(k == 0, 0.5, 1.0)

    def late_terms(k, rnd):
        ref, factor = z_ref.at[k + 2], weight(k)
        unpack_z(comm, rnd, tree)
        below, above = x_ghosts(comm, rnd)
        for t in range(ROWS):
            part = slice(SUB * (t % 4), SUB * (t % 4) + SUB)
            for plane, face, layer in ((1, 0, below), (NP, 1, above)):
                term = coef_ref[plane - 1, t, face] * layer[t // 4][part]
                part_ref[plane - 1, tile(t), :] = part_ref[plane - 1, tile(t), :] + factor * term

        first, last = row_iota(SUB) == 0, row_iota(SUB) == SUB - 1

        def body(p, state):
            turned = [spin(tree[p], 2), tree[p]]
            news = []
            for t in range(ROWS):
                part = slice(SUB * (t % 4), SUB * (t % 4) + SUB)
                term = edge_ref[p, tile(t), :] * turned[t // 4][part]
                for end, at, sub, mask in ((0, 0, 0, first), (1, ROWS - 1, SUB - 1, last)):
                    if t == at:
                        line = coef_ref[p, t, 2 + end, one(sub), :] * comm.yr[rnd, end, p]
                        term = term + jnp.where(mask, line, 0.0)
                news.append(part_ref[p, tile(t), :] + factor * term)
                ref[p + 1, own(t), :] = news[t]
            for t in range(4):
                tree[p, tile(t), :] = jnp.where(face_mask(2, SUB), news[t], spin(news[t + 4], 2))
        sweep(body, unroll=NP)

    def apply(k, carry):
        rnd, factor = k + 2, weight(k)
        ref = z_ref.at[k + 1]
        inner_planes(ref)

        def step(p, state):
            for t in range(ROWS):
                _, others = neighbours(ref, p, t)
                total = total_of(coef_ref[p, t, i] * others[i] for i in range(FACES))
                part_ref[p, tile(t), :] = factor * total - z_ref[k, p + 1, own(t), :]

        sweep(step)
        products(k)
        for face in range(FACES):
            comm.wait_recv(rnd, face)
        late_terms(k, rnd)

        @pl.when(k < CG_ITERS - 1)
        def _():
            send_faces(comm, rnd + 1, z_ref.at[k + 2], tree, folded=True)
        return carry

    lax.fori_loop(0, CG_ITERS, apply, 0)
    products(CG_ITERS)

    total = jnp.broadcast_to(lane_sum(sums_ref[...]), (LANES, LANES))
    row = row_sum(jnp.where(lane_iota(LANES) == row_iota(LANES), total, 0.0))
    red = Reducer(comm, send_row, (rows_a, rows_b), red_ss, red_rs)
    row = red.run(row)
    avec, cvec, ok = solve_coefficients(row, mom_ref, pc_ref, hist_ref, full_ref)
    comb_ref[0] = avec
    comb_ref[1] = cvec

    a_co = [jnp.broadcast_to(comb_ref[0, one(i)], TILE) for i in range(CG_ITERS)]
    c_co = [jnp.broadcast_to(comb_ref[1, one(i)], TILE) for i in range(NB)]

    def combine(p, carry):
        for t in range(ROWS):
            row = own(t)
            rows = tile(t)
            basis = [z_ref[i + 1, p + 1, row, :] for i in range(NB)]
            ut, rt = a_co[0] * basis[0], c_co[0] * basis[0]
            for i in range(1, NB):
                if i < CG_ITERS:
                    ut = ut + a_co[i] * basis[i]
                rt = rt + c_co[i] * basis[i]
            ut = u_ref[p + 1, row, :] + ut
            rt = d_ref[p, rows, :] * rt
            u_out[p, rows, :] = ut[:, :HALF]
            u_out[p + NP, rows, :] = turn_half(ut)[:, :HALF]
            r_out[p, rows, :] = rt[:, :HALF]
            r_out[p + NP, rows, :] = turn_half(rt)[:, :HALF]
        return carry

    lax.fori_loop(0, NP, combine, 0, unroll=4)
    h_ref[...] = squares_row(hist_ref, full_ref)
    ok_ref[0, 0] = ok[0, 0].astype(jnp.int32)

    def drain(rnd, carry):
        for face in range(FACES):
            comm.wait_send(rnd, face)
        return carry
    lax.fori_loop(0, CG_ITERS + 2, drain, 0)


def plain_kernel(counts, k_hbm, g_hbm, f_hbm, u_hbm, u_out, r_out, h_ref,
                 raw_k, raw_u, raw_f, slab_x, slab_y, slab_z, k_ref, u_ref, p_ref, q_ref, r_ref, coef_ref, d_ref, tree, square, k_ghost, u_ghost,
                 xs, ys, zs, xr, yr, zr, send_row, rows_a, rows_b,
                 load_sem, send_sem, recv_sem, red_ss, red_rs):
    comm = Comm(counts, (xs, ys, zs, xr, yr, zr, send_sem, recv_sem))
    raws, slabs = (raw_k, raw_u, raw_f), (slab_x, slab_y, slab_z)
    loads = start_up(comm, (k_hbm, g_hbm, f_hbm, u_hbm), raws, slabs, load_sem)
    greet = greet_groups(comm)
    zero_ends(comm, 3)
    first_exchange(comm, loads, greet, raws, slabs, k_ref, u_ref, tree, square, k_ghost, u_ghost)
    red = [Reducer(comm, send_row.at[i], (rows_a.at[i], rows_b.at[i]), red_ss.at[i], red_rs.at[i]) for i in range(2)]

    def reduce(which, accs):
        lane = lane_iota(1)
        row = jnp.zeros((1, LANES), F32)
        for i, acc in enumerate(accs):
            total = row_sum(lane_sum(acc))
            row = jnp.where(lane == i, jnp.broadcast_to(total, (1, LANES)), row)
        row = red[which].run(row)
        return [lane_sum(jnp.where(lane == i, row, 0.0)) for i in range(len(accs))]

    def first(p, state):
        for t in range(ROWS):
            weights, resid, inv = first_residual(raw_f, k_ref, u_ref, k_ghost, u_ghost, p, t, d_ref)
            for i in range(FACES):
                coef_ref[p, t, i] = weights[i]
            r_ref[p, tile(t), :] = resid
            z_new = resid * inv
            p_ref[p + 1, own(t), :] = z_new
            state[0] = state[0] + resid * z_new

    rho, = reduce(0, sweep(first, zero_tiles(1)))

    def iteration(it, carry):
        rho, hist = carry

        send_faces(comm, 2, p_ref, tree)
        for face in range(FACES):
            comm.wait_recv(2, face)
            comm.wait_send(2, face)
        outer_layers(comm, 2, p_ref)
        spread_z(comm, 2, tree, k_ghost)

        def apply(p, state):
            for t in range(ROWS):
                centre, others = neighbours(p_ref, p, t, k_ghost)
                q = total_of(coef_ref[p, t, i] * (centre - others[i]) for i in range(FACES))
                q_ref[p, tile(t), :] = q
                state[0] = state[0] + centre * q

        curv, = reduce(1, sweep(apply, zero_tiles(1)))
        alpha = jnp.broadcast_to(rho / curv, TILE)

        def update(p, accs):
            acc_z, acc_r = accs
            for t in range(ROWS):
                row = own(t)
                rows = tile(t)
                u_ref[p + 1, row, :] = u_ref[p + 1, row, :] + alpha * p_ref[p + 1, row, :]
                resid = r_ref[p, rows, :] - alpha * q_ref[p, rows, :]
                r_ref[p, rows, :] = resid
                acc_z = acc_z + resid * (resid / d_ref[p, rows, :])
                acc_r = acc_r + resid * resid
            return acc_z, acc_r

        rho_new, rr = reduce(0, lax.fori_loop(0, NP, update, zero_tiles(2)))
        beta = jnp.broadcast_to(rho_new / rho, TILE)

        def turn(p, carry):
            for t in range(ROWS):
                row = own(t)
                rows = tile(t)
                p_ref[p + 1, row, :] = r_ref[p, rows, :] / d_ref[p, rows, :] + beta * p_ref[p + 1, row, :]
            return carry

        lax.fori_loop(0, NP, turn, 0)
        hist = jnp.where(lane_iota(1) == it, jnp.broadcast_to(rr, (1, LANES)), hist)
        return rho_new, hist

    _, hist = lax.fori_loop(0, CG_ITERS, iteration, (rho, jnp.zeros((1, LANES), F32)))
    h_ref[...] = hist

    def finish(p, carry):
        write_plane(u_out, p, u_ref[p + 1, R0:R0 + NY, :])
        write_plane(r_out, p, r_ref[p])
        return carry

    lax.fori_loop(0, NP, finish, 0)
    for rnd in range(2):
        for face in range(FACES):
            comm.wait_send(rnd, face)


def finish_kernel(u_in, r_in, u_hbm, r_hbm, sems):
    copies = [pltpu.make_async_copy(u_in, u_hbm, sems.at[0]), pltpu.make_async_copy(r_in, r_hbm, sems.at[1])]
    for copy in copies:
        copy.start()
    for copy in copies:
        copy.wait()


def scratch_for(kind, counts):
    field = (NP + 2, NY + 16, LANES)
    block = (NP, NY, LANES)
    vm = lambda *shape: pltpu.VMEM(shape, F32)
    raws = [vm(NX, NY, NZ)] * 3 + [vm(NY, LANES), vm(NX, LANES), vm(NX, LANES)]
    if kind == 'basis':
        rounds, reds = CG_ITERS + 2, ()
        work = [vm(*field), vm(*field), vm(NB + 1, *field), vm(NP, ROWS, FACES, *TILE), vm(*block), vm(LANES, LANES),
                vm(40, LANES), vm(32, LANES), vm(CG_ITERS, 16, LANES), vm(NB, 16, LANES), vm(2, 16, LANES), vm(*block), vm(*block)]
    else:
        rounds, reds = 3, (2,)
        work = [vm(*field), vm(*field), vm(*field), vm(*block), vm(*block), vm(NP, ROWS, FACES, *TILE), vm(*block)]
    work += [vm(NP, FOLD, LANES), vm(LANES, LANES), vm(*block), vm(*block)]
    sides = [vm(rounds, 2, FOLD, LANES), vm(rounds, 2, NP, 1, LANES)]
    faces = sides + [vm(rounds, FOLD, LANES)] + sides + [vm(rounds, 2, FOLD, LANES)]
    sizes = [counts[0], counts[1] * counts[2]]
    rows = [vm(*reds, 2, 1, LANES)] + [vm(*reds, n, 1, LANES) for n in sizes]
    dma = pltpu.SemaphoreType.DMA
    sems = [dma((6,)), dma((rounds, 6)), dma((rounds, 6)), dma((*reds, 2, max(sizes))), dma((*reds, 2, max(sizes)))]
    return raws + work + faces + rows + sems


def solution(mesh):
    counts = tuple(mesh.shape[name] for name in AXES)
    grid_spec = P(*AXES)
    block = jax.ShapeDtypeStruct((NX, NY, NZ), F32)

    def call(kernel, kind, ident, *more):
        hbm, vmem = pl.BlockSpec(memory_space=pltpu.HBM), pl.BlockSpec(memory_space=pltpu.VMEM)
        smem = [pl.BlockSpec(memory_space=pltpu.SMEM)] * len(more)
        return pl.pallas_call(
            functools.partial(kernel, counts),
            out_shape=(block, block, jax.ShapeDtypeStruct((1, LANES), F32), *more),
            in_specs=[hbm] * 4,
            out_specs=(vmem, vmem, vmem, *smem),
            scratch_shapes=scratch_for(kind, counts),
            compiler_params=pltpu.CompilerParams(collective_id=ident, has_side_effects=True, vmem_limit_bytes=VMEM_BYTES),
            name=kind,
        )

    def local_solve(k_cell, k_ghost, f_rhs, u_init):
        args = (k_cell, k_ghost, f_rhs, u_init)
        *fast, ok = call(basis_kernel, 'basis', 0, jax.ShapeDtypeStruct((1, 1), jnp.int32))(*args)
        u_out, r_out, row = lax.cond(ok[0, 0] > 0, lambda: tuple(fast),
                                     lambda: tuple(call(plain_kernel, 'plain', 1)(*args)))
        u_out, r_out = pl.pallas_call(
            finish_kernel,
            out_shape=(block, block),
            in_specs=[pl.BlockSpec(memory_space=pltpu.VMEM)] * 2,
            out_specs=(pl.BlockSpec(memory_space=pltpu.HBM),) * 2,
            scratch_shapes=[pltpu.SemaphoreType.DMA((2,))],
            compiler_params=pltpu.CompilerParams(vmem_limit_bytes=VMEM_BYTES),
            name='finish',
        )(u_out, r_out)
        return u_out, r_out, row[0, 0:CG_ITERS]

    return jax.shard_map(local_solve, mesh=mesh, in_specs=(grid_spec, P(), grid_spec, grid_spec),
                         out_specs=(grid_spec, grid_spec, P()), check_vma=False)
```

```python
import functools

import jax
import jax.numpy as jnp
from jax import lax
from jax.experimental import pallas as pl
from jax.experimental.pallas import tpu as pltpu
from jax.sharding import PartitionSpec as P

CG_ITERS = 8
NB = CG_ITERS + 1
NX, NY, NZ = 32, 64, 64
NP = NX // 2
R0 = 8
MESH = pl.DeviceIdType.MESH
AXES = ('gx', 'gy', 'gz')
BOUND = 4096.0
GRAM = 2 * NB
VMEM_BYTES = 60_000_000
F32 = jnp.float32
SUB, LANES, HALF, LOW = 8, 128, 64, 63
ROWS = NY // SUB
TILE = (SUB, LANES)
WIDE = (2 * SUB, LANES)
FACES = 6
FOLD = NY // 2
TURNS = ((4, 8, 12), (16, 32, 48))


def own(t):
    return slice(R0 + SUB * t, R0 + SUB * t + SUB)


def tile(t):
    return slice(SUB * t, SUB * t + SUB)


def one(i):
    return slice(i, i + 1)


def spin(values, by):
    return pltpu.roll(values, by, 1)


def turn_half(values):
    return spin(values, HALF)


def row_sum(values):
    return jnp.sum(values, axis=0, keepdims=True)


def lane_sum(values):
    return jnp.sum(values, axis=1, keepdims=True)


def total_of(parts):
    parts = list(parts)
    while len(parts) > 1:
        parts = [sum(parts[i + 1:i + 2], parts[i]) for i in range(0, len(parts), 2)]
    return parts[0]


def lane_iota(rows=8):
    return lax.broadcasted_iota(jnp.int32, (rows, LANES), 1)


def row_iota(rows):
    return lax.broadcasted_iota(jnp.int32, (rows, LANES), 0)


class Comm:
    def __init__(self, counts, bufs):
        self.counts = counts
        self.pos = [lax.axis_index(name) for name in AXES]
        self.has = []
        for axis in range(3):
            self.has.append(self.pos[axis] > 0)
            self.has.append(self.pos[axis] < counts[axis] - 1)
        (self.xs, self.ys, self.zs, self.xr, self.yr, self.zr, self.send_sem, self.recv_sem) = bufs

    def neighbour(self, face):
        return {AXES[face // 2]: self.pos[face // 2] + (1 if face % 2 else -1)}

    def source(self, rnd, face):
        axis, high = face // 2, face % 2
        return (self.xs, self.ys, self.zs)[axis].at[rnd, high]

    def copies(self, rnd, face):
        axis, high = face // 2, face % 2
        src = self.source(rnd, face)
        dst = (self.xr, self.yr, self.zr)[axis]
        return pltpu.make_async_remote_copy(
            src_ref=src, dst_ref=dst.at[rnd, 1 - high],
            send_sem=self.send_sem.at[rnd, face], recv_sem=self.recv_sem.at[rnd, face ^ 1],
            device_id=self.neighbour(face), device_id_type=MESH)

    def send(self, rnd, face):
        @pl.when(self.has[face])
        def _():
            self.copies(rnd, face).start()

    def wait_recv(self, rnd, face):
        axis, high = face // 2, face % 2
        src = self.source(rnd, face)
        dst = (self.xr, self.yr, self.zr)[axis]

        @pl.when(self.has[face])
        def _():
            pltpu.make_async_remote_copy(
                src_ref=src, dst_ref=dst.at[rnd, high],
                send_sem=self.send_sem.at[rnd, face], recv_sem=self.recv_sem.at[rnd, face],
                device_id=self.neighbour(face), device_id_type=MESH).wait_recv()

    def wait_send(self, rnd, face):
        @pl.when(self.has[face])
        def _():
            self.copies(rnd, face).wait_send()


GROUPS = (('gx',), ('gy', 'gz'))


def group_of(comm, group):
    sizes = [comm.counts[AXES.index(name)] for name in group]
    size, rank = 1, 0
    for name, n in zip(group, sizes):
        size, rank = size * n, rank * n + comm.pos[AXES.index(name)]

    def peer(off):
        left, where = lax.rem(rank + off, size), {}
        for name, n in reversed(tuple(zip(group, sizes))):
            where[name], left = lax.rem(left, n), lax.div(left, n)
        return where
    return size, rank, peer


def greet_faces(comm):
    sem = pltpu.get_barrier_semaphore()
    for face in range(FACES):
        @pl.when(comm.has[face])
        def _():
            pl.semaphore_signal(sem, inc=1, device_id=comm.neighbour(face), device_id_type=MESH)
    return sem, sum(flag.astype(jnp.int32) for flag in comm.has)


def greet_groups(comm):
    sem, total = pltpu.get_barrier_semaphore(), 0
    for group in GROUPS:
        size, _, peer = group_of(comm, group)
        for off in range(1, size):
            pl.semaphore_signal(sem, inc=1, device_id=peer(off), device_id_type=MESH)
        total += size - 1
    return sem, total


class Reducer:
    def __init__(self, comm, send_row, recv_rows, send_sem, recv_sem):
        self.comm, self.send_row, self.recv_rows, self.ss, self.rs = comm, send_row, recv_rows, send_sem, recv_sem

    def run(self, row):
        for stage, group in enumerate(GROUPS):
            size, rank, peer = group_of(self.comm, group)
            rows = self.recv_rows[stage]
            self.send_row[stage] = row
            copies = [pltpu.make_async_remote_copy(
                src_ref=self.send_row.at[stage], dst_ref=rows.at[rank], send_sem=self.ss.at[stage, off],
                recv_sem=self.rs.at[stage, off], device_id=peer(off), device_id_type=MESH) for off in range(1, size)]
            for copy in copies:
                copy.start()
            rows[rank] = row
            for copy in copies:
                copy.wait()
            row = total_of(rows[i] for i in range(size))
        return row


def store_plane_faces(comm, rnd, ref, p):
    comm.ys[rnd, 0, p] = ref[p + 1, R0:R0 + 1, :]
    comm.ys[rnd, 1, p] = ref[p + 1, R0 + NY - 1:R0 + NY, :]


def pack_x_faces(comm, rnd, ref):
    half = FOLD
    lane = lane_iota(half)
    a, b = ref[1, R0:R0 + half, :], ref[1, R0 + half:R0 + NY, :]
    comm.xs[rnd, 0] = jnp.where(lane < HALF, a, turn_half(b))
    a, b = ref[NP, R0:R0 + half, :], ref[NP, R0 + half:R0 + NY, :]
    comm.xs[rnd, 1] = jnp.where(lane < HALF, turn_half(a), b)


def face_mask(turn, rows=FOLD):
    return ((lane_iota(rows) + 1) & LOW) < turn


def pack_z(comm, rnd, ref, tree):
    def fold(p, carry):
        low, high = ref[p + 1, R0:R0 + FOLD, :], ref[p + 1, R0 + FOLD:R0 + NY, :]
        tree[p] = jnp.where(face_mask(2), low, spin(high, 2))
        return carry
    lax.fori_loop(0, NP, fold, 0, unroll=NP)
    join_z(comm, rnd, tree)


def join_z(comm, rnd, tree):
    parts = [tree[p] for p in range(NP)]
    for turns in TURNS:
        merged = []
        for i in range(0, NP, 4)[:len(parts) // 4]:
            out = spin(parts[i + 3], turns[-1])
            for n in (2, 1):
                out = jnp.where(face_mask(turns[n]), spin(parts[i + n], turns[n - 1]), out)
            merged.append(jnp.where(face_mask(turns[0]), parts[i], out))
        parts = merged
    for end in range(2):
        comm.zs[rnd, end] = halve_z(parts[0], 1 - end)


def halve_z(packed, keep):
    even = (lane_iota(NP) & 1) == 1 - keep
    return jnp.where(even, packed[:NP], spin(packed[NP:], 1 if keep else LANES - 1))


def unpack_z(comm, rnd, tree):
    odd = (lane_iota(NP) & 1) == 1
    low, high = comm.zr[rnd, 0], comm.zr[rnd, 1]
    parts = [jnp.concatenate([jnp.where(odd, spin(high, LOW - 2 - i), spin(low, LOW + i)) for i in range(2)], axis=0)]
    for turns in reversed(TURNS):
        parts = [q for part in parts for q in (part, *(spin(part, LANES - turn) for turn in turns))]
    for p in range(NP):
        tree[p] = parts[p]


def spread_z(comm, rnd, tree, ghost):
    unpack_z(comm, rnd, tree)

    def fold(p, carry):
        ghost[p, 0:FOLD, :] = spin(tree[p], 2)
        ghost[p, FOLD:NY, :] = tree[p]
        return carry
    lax.fori_loop(0, NP, fold, 0, unroll=NP)


def inner_planes(ref):
    low = lane_iota(NY) < HALF
    ref[0, R0:R0 + NY, :] = jnp.where(low, 0.0, turn_half(ref[NP, R0:R0 + NY, :]))
    ref[NP + 1, R0:R0 + NY, :] = jnp.where(low, turn_half(ref[1, R0:R0 + NY, :]), 0.0)


def x_ghosts(comm, rnd):
    low = lane_iota(FOLD) < HALF
    lo, hi = comm.xr[rnd, 0], comm.xr[rnd, 1]
    below = [jnp.where(low, lo, 0.0), jnp.where(low, turn_half(lo), 0.0)]
    above = [jnp.where(low, 0.0, turn_half(hi)), jnp.where(low, 0.0, hi)]
    return below, above


def outer_layers(comm, rnd, ref):
    inner_planes(ref)
    below, above = x_ghosts(comm, rnd)
    for i in range(2):
        rows = slice(R0 + FOLD * i, R0 + FOLD * i + FOLD)
        ref[0, rows, :] = ref[0, rows, :] + below[i]
        ref[NP + 1, rows, :] = ref[NP + 1, rows, :] + above[i]
    for p in range(NP):
        ref[p + 1, R0 - 1:R0, :] = comm.yr[rnd, 0, p]
        ref[p + 1, R0 + NY:R0 + NY + 1, :] = comm.yr[rnd, 1, p]


def blank_rows(ref):
    for p in range(NP):
        ref[p + 1, R0 - 1:R0, :] = jnp.zeros((1, LANES), F32)
        ref[p + 1, R0 + NY:R0 + NY + 1, :] = jnp.zeros((1, LANES), F32)


def neighbours(ref, p, t, ghost=None):
    row = R0 + SUB * t
    lane = lane_iota() & LOW
    centre = ref[p + 1, own(t), :]
    xm = ref[p, own(t), :]
    xp = ref[p + 2, own(t), :]
    ym = ref[p + 1, row - 1:row + SUB - 1, :]
    yp = ref[p + 1, row + 1:row + SUB + 1, :]
    zm, zp = spin(centre, 1), spin(centre, LANES - 1)
    if ghost is not None:
        edge = ghost[p, tile(t), :]
        zm, zp = jnp.where(lane == 0, edge, zm), jnp.where(lane == LOW, edge, zp)
    return centre, (xm, xp, ym, yp, zm, zp)


def sweep(body, state=(), unroll=2):
    def plane(p, carry):
        carry = list(carry)
        body(p, carry)
        return tuple(carry)
    return lax.fori_loop(0, NP, plane, tuple(state), unroll=unroll)


def zero_tiles(n):
    return tuple(jnp.zeros(TILE, F32) for _ in range(n))


def send_faces(comm, rnd, ref, tree, folded=False):
    if not folded:
        for p in range(NP):
            store_plane_faces(comm, rnd, ref, p)
    for face in (2, 3):
        comm.send(rnd, face)
    (join_z if folded else functools.partial(pack_z, ref=ref))(comm, rnd, tree=tree)
    for face in (4, 5):
        comm.send(rnd, face)
    pack_x_faces(comm, rnd, ref)
    for face in (0, 1):
        comm.send(rnd, face)


def load_field(raw, ref):
    def body(p, state):
        ref[p + 1, R0:R0 + NY, :] = jnp.concatenate([raw[p], raw[p + NP]], axis=1)
    sweep(body, unroll=NP)


def fill_ghost_conductivity(comm, square, gx_slab, gy_slab, gz_slab):
    px, py, pz = comm.pos
    half = FOLD
    turn = 64 * lax.rem(pz, 2)
    lane = lane_iota(half)
    a, b = pltpu.roll(gx_slab[0:half, :], turn, 1), pltpu.roll(gx_slab[half:NY, :], turn, 1)
    x_face = jnp.where(lane < HALF, a, turn_half(b))
    for end in range(2):
        @pl.when(jnp.logical_not(comm.has[end]))
        def _():
            comm.xr[0, end] = x_face
    rows = pltpu.roll(gy_slab[...], turn, 1)
    y_face = jnp.where(lane_iota(NP) < HALF, rows[0:NP], turn_half(rows[NP:NX]))
    for end in range(2):
        @pl.when(jnp.logical_not(comm.has[2 + end]))
        def _():
            for p in range(NP):
                comm.yr[0, end, p] = y_face[one(p)]
    for end in range(2):
        @pl.when(jnp.logical_not(comm.has[4 + end]))
        def _():
            cols = spin(gz_slab[...], HALF * lax.rem(py, 2))
            shift = 0 if end else LOW
            square[...] = jnp.zeros(square.shape, F32)
            for x in range(NX):
                for c in range(2):
                    square[one((4 * (x % NP) + 2 * c + HALF * (x // NP) + shift) % LANES)] = cols[one(x)]
            turned = square[...].T
            second = ((lane_iota(FOLD) - shift) & 3) == 2
            comm.zr[0, end] = halve_z(jnp.where(second, turned[FOLD:NY], turned[:FOLD]), end)


def zero_ends(comm, rounds):
    for face in range(FACES):
        @pl.when(jnp.logical_not(comm.has[face]))
        def _():
            buf = (comm.xr, comm.yr, comm.zr)[face // 2]

            def clear(rnd, carry):
                buf[rnd, face % 2] = jnp.zeros(buf.shape[2:], F32)
                return carry
            lax.fori_loop(1, rounds, clear, 0)


def lanes_of(pos):
    return pl.ds(pl.multiple_of(lax.div(pos, 2) * LANES, LANES), LANES)


def start_up(comm, ins, raws, slabs, load_sem):
    k_hbm, g_hbm, f_hbm, u_hbm = ins
    px, py, pz = comm.pos
    loads = [pltpu.make_async_copy(k_hbm, raws[0], load_sem.at[0]),
             pltpu.make_async_copy(u_hbm, raws[1], load_sem.at[1])]
    x_row = jnp.where(comm.has[1], 0, 1)
    y_row = jnp.where(comm.has[3], 2, 3)
    z_row = jnp.where(comm.has[5], 4, 5)
    z_lanes = lanes_of(pz)
    y_lanes = lanes_of(py)
    loads.append(pltpu.make_async_copy(
        g_hbm.at[x_row, pl.ds(pl.multiple_of(py * NY, NY), NY), z_lanes], slabs[0], load_sem.at[2]))
    loads.append(pltpu.make_async_copy(
        g_hbm.at[y_row, pl.ds(pl.multiple_of(px * NX, NX), NX), z_lanes], slabs[1], load_sem.at[3]))
    loads.append(pltpu.make_async_copy(
        g_hbm.at[z_row, pl.ds(pl.multiple_of(px * NX, NX), NX), y_lanes], slabs[2], load_sem.at[4]))
    loads.append(pltpu.make_async_copy(f_hbm, raws[2], load_sem.at[5]))
    for load in loads:
        load.start()
    return loads


def first_exchange(comm, loads, greet, raws, slabs, k_ref, u_ref, tree, square, k_ghost, u_ghost):
    sem, total = greet
    loads[0].wait()
    load_field(raws[0], k_ref)
    pl.semaphore_wait(sem, total)
    send_faces(comm, 0, k_ref, tree)
    loads[1].wait()
    load_field(raws[1], u_ref)
    send_faces(comm, 1, u_ref, tree)
    for load in loads[2:]:
        load.wait()
    fill_ghost_conductivity(comm, square, *slabs)
    for rnd, ref, ghost in ((0, k_ref, k_ghost), (1, u_ref, u_ghost)):
        for face in range(FACES):
            comm.wait_recv(rnd, face)
        outer_layers(comm, rnd, ref)
        spread_z(comm, rnd, tree, ghost)


def first_residual(raw_f, k_ref, u_ref, k_ghost, u_ghost, p, t, d_ref):
    centre, others = neighbours(k_ref, p, t, k_ghost)
    u_own, u_others = neighbours(u_ref, p, t, u_ghost)
    twice = centre + centre
    weights = [twice * other / (centre + other) for other in others]
    diag = total_of(weights)
    au = total_of([w * (u_own - other) for w, other in zip(weights, u_others)])
    f_tile = jnp.concatenate([raw_f[p, tile(t), :], raw_f[p + NP, tile(t), :]], axis=1)
    d_ref[p, tile(t), :] = diag
    return weights, f_tile - au, 1.0 / diag


def write_plane(raw_ref, p, values):
    raw_ref[p] = values[:, :HALF]
    raw_ref[p + NP] = turn_half(values)[:, :HALF]


def dot_rows(a, b):
    prod = a[:2 * SUB] * b[:2 * SUB]
    return row_sum(prod[:SUB] + prod[SUB:])


def solve_coefficients(row, mom_ref, pc_ref, hist_ref, full_ref):
    lane24, line24 = lane_iota(24), row_iota(24)
    wide = jnp.broadcast_to(row, (24, LANES))
    base = lane_sum(jnp.where((lane24 == line24 + 1) & (line24 < 17), wide, 0.0))
    base = jnp.broadcast_to(base, (24, LANES))
    first, second = base[0:1], base[1:2]
    even = (line24 & 1) == 0
    mom = jnp.where(line24 >= 2, 2.0 * base - jnp.where(even, first, second), base)
    mom = jnp.where(line24 < 17, mom, 0.0)
    lane16, line16 = lane_iota(16), row_iota(16)
    wide = jnp.broadcast_to(row, WIDE)
    for k in range(NB):
        big = jnp.maximum(line16, k)
        small = jnp.minimum(line16, k)
        want = GRAM + NB * big + small
        col = lane_sum(jnp.where((lane16 == want) & (line16 < NB), wide, 0.0))
        full_ref[k] = jnp.broadcast_to(col, WIDE)
    zeros8 = jnp.zeros(TILE, F32)
    mom_ref[:SUB] = zeros8
    mom_ref[32:40] = zeros8
    pc_ref[:SUB] = zeros8
    pc_ref[24:32] = zeros8
    unit = jnp.where(line16 == 0, 1.0, 0.0)
    cvec, pvec, avec = unit, unit, jnp.zeros(WIDE, F32)
    rvec, mvec = mom, mom
    mu0 = mom[0:1]
    rho = dot_rows(cvec, rvec)
    ok = jnp.where(rho > 0.0, 1.0, 0.0)
    two_one = jnp.where(line16 == 1, 2.0, 1.0)
    for t in range(CG_ITERS):
        mom_ref[8:32] = mvec
        mom_ref[7:8] = mvec[1:2]
        pc_ref[8:24] = pvec
        qvec = mvec - 0.5 * (mom_ref[9:33] + mom_ref[7:31])
        npvec = 0.5 * (two_one * pc_ref[7:23] + pc_ref[9:25])
        curv = dot_rows(pvec, qvec)
        size = row_sum(jnp.abs(pvec))
        ok = jnp.where(size * size * mu0 < BOUND * curv, ok, 0.0)
        alpha = rho / curv
        avec = avec + alpha * pvec
        cvec = cvec - alpha * (pvec - npvec)
        rvec = rvec - alpha * qvec
        hist_ref[t] = cvec
        rho_new = dot_rows(cvec, rvec)
        size = row_sum(jnp.abs(cvec))
        ok = jnp.where(size * size * mu0 < BOUND * rho_new, ok, 0.0)
        beta = rho_new / rho
        pvec = cvec + beta * pvec
        mvec = rvec + beta * mvec
        rho = rho_new
    return avec, cvec, ok


def squares_row(hist_ref, full_ref):
    lane = lane_iota(1)
    out = jnp.zeros((1, LANES), F32)
    for t in range(CG_ITERS):
        cvec = hist_ref[t]
        acc = full_ref[0] * hist_ref[t, one(0)]
        for j in range(1, NB):
            acc = acc + full_ref[j] * hist_ref[t, one(j)]
        out = jnp.where(lane == t, dot_rows(acc, cvec), out)
    return out


def basis_kernel(counts, k_hbm, g_hbm, f_hbm, u_hbm, u_out, r_out, h_ref, ok_ref,
                 raw_k, raw_u, raw_f, slab_x, slab_y, slab_z, k_ref, u_ref, z_ref, coef_ref, d_ref, sums_ref,
                 mom_ref, pc_ref, hist_ref, full_ref, comb_ref, edge_ref, part_ref, tree, square, k_ghost, u_ghost,
                 xs, ys, zs, xr, yr, zr, send_row, rows_a, rows_b,
                 load_sem, send_sem, recv_sem, red_ss, red_rs):
    comm = Comm(counts, (xs, ys, zs, xr, yr, zr, send_sem, recv_sem))
    raws, slabs = (raw_k, raw_u, raw_f), (slab_x, slab_y, slab_z)
    loads = start_up(comm, (k_hbm, g_hbm, f_hbm, u_hbm), raws, slabs, load_sem)
    greet = greet_faces(comm)
    zero_ends(comm, CG_ITERS + 2)
    sums_ref[...] = jnp.zeros(sums_ref.shape, F32)

    def blank(k, carry):
        blank_rows(z_ref.at[k + 1])
        return carry
    lax.fori_loop(0, CG_ITERS, blank, 0)

    def nothing(p, state):
        z_ref[0, p + 1, R0:R0 + NY, :] = jnp.zeros((NY, LANES), F32)
    sweep(nothing, unroll=4)
    first_exchange(comm, loads, greet, raws, slabs, k_ref, u_ref, tree, square, k_ghost, u_ghost)

    def first(p, state):
        lane = lane_iota() & LOW
        for t in range(ROWS):
            weights, resid, inv = first_residual(raw_f, k_ref, u_ref, k_ghost, u_ghost, p, t, d_ref)
            factor = inv + inv
            scaled = [w * factor for w in weights]
            low, high = scaled[4:]
            edge_ref[p, tile(t), :] = jnp.where(lane == 0, low, jnp.where(lane == LOW, high, 0.0))
            scaled[4:] = jnp.where(lane == 0, 0.0, low), jnp.where(lane == LOW, 0.0, high)
            for i in range(FACES):
                coef_ref[p, t, i] = scaled[i]
            z_ref[1, p + 1, own(t), :] = resid * inv

    sweep(first, unroll=4)
    send_faces(comm, 2, z_ref.at[1], tree)

    def products(k):
        def body(p, accs):
            for t in range(ROWS):
                d = d_ref[p, tile(t), :]
                z_k = z_ref[k + 1, p + 1, own(t), :]
                dz = d * z_k
                ddz = d * dz
                for i in range(NB):
                    accs[i] = accs[i] + ddz * z_ref[i + 1, p + 1, own(t), :]
                accs[NB] = accs[NB] + dz * z_k
                accs[NB + 1] = accs[NB + 1] + dz * z_ref[k, p + 1, own(t), :]
        accs = sweep(body, zero_tiles(NB + 2))
        rows = [GRAM + NB * k + i for i in range(NB)] + [2 * k + 1, 2 * k]
        for row, acc in zip(rows, accs):
            sums_ref[pl.ds(row, 1), :] = row_sum(acc)

    def weight(k):
        return jnp.where(k == 0, 0.5, 1.0)

    def x_terms(k, rnd):
        factor = weight(k)
        below, above = x_ghosts(comm, rnd)
        for t in range(ROWS):
            part = slice(SUB * (t % 4), SUB * (t % 4) + SUB)
            for plane, face, layer in ((0, 0, below), (NP - 1, 1, above)):
                term = coef_ref[plane, t, face] * layer[t // 4][part]
                part_ref[plane, tile(t), :] = part_ref[plane, tile(t), :] + factor * term

    def late_terms(k, rnd):
        ref, factor = z_ref.at[k + 2], weight(k)
        unpack_z(comm, rnd, tree)
        first, last = row_iota(SUB) == 0, row_iota(SUB) == SUB - 1

        def body(p, state):
            turned = [spin(tree[p], 2), tree[p]]
            news = []
            for t in range(ROWS):
                part = slice(SUB * (t % 4), SUB * (t % 4) + SUB)
                term = edge_ref[p, tile(t), :] * turned[t // 4][part]
                for end, at, sub, mask in ((0, 0, 0, first), (1, ROWS - 1, SUB - 1, last)):
                    if t == at:
                        line = coef_ref[p, t, 2 + end, one(sub), :] * comm.yr[rnd, end, p]
                        term = term + jnp.where(mask, line, 0.0)
                news.append(part_ref[p, tile(t), :] + factor * term)
                ref[p + 1, own(t), :] = news[t]
            comm.ys[rnd + 1, 0, p] = news[0][:1]
            comm.ys[rnd + 1, 1, p] = news[ROWS - 1][SUB - 1:]
            for t in range(4):
                tree[p, tile(t), :] = jnp.where(face_mask(2, SUB), news[t], spin(news[t + 4], 2))
        sweep(body, unroll=NP)

    def apply(k, carry):
        rnd, factor = k + 2, weight(k)
        ref = z_ref.at[k + 1]
        inner_planes(ref)

        def step(p, state):
            for t in range(ROWS):
                _, others = neighbours(ref, p, t)
                total = total_of(coef_ref[p, t, i] * others[i] for i in range(FACES))
                part_ref[p, tile(t), :] = factor * total - z_ref[k, p + 1, own(t), :]

        sweep(step)
        products(k)
        for face in range(FACES):
            comm.wait_recv(rnd, face)
            if face == 1:
                x_terms(k, rnd)
        late_terms(k, rnd)

        @pl.when(k < CG_ITERS - 1)
        def _():
            send_faces(comm, rnd + 1, z_ref.at[k + 2], tree, folded=True)
        return carry

    lax.fori_loop(0, CG_ITERS, apply, 0)
    products(CG_ITERS)

    total = jnp.broadcast_to(lane_sum(sums_ref[...]), (LANES, LANES))
    row = row_sum(jnp.where(lane_iota(LANES) == row_iota(LANES), total, 0.0))
    red = Reducer(comm, send_row, (rows_a, rows_b), red_ss, red_rs)
    row = red.run(row)
    avec, cvec, ok = solve_coefficients(row, mom_ref, pc_ref, hist_ref, full_ref)
    comb_ref[0] = avec
    comb_ref[1] = cvec

    a_co = [jnp.broadcast_to(comb_ref[0, one(i)], TILE) for i in range(CG_ITERS)]
    c_co = [jnp.broadcast_to(comb_ref[1, one(i)], TILE) for i in range(NB)]

    def combine(p, carry):
        for t in range(ROWS):
            row = own(t)
            rows = tile(t)
            basis = [z_ref[i + 1, p + 1, row, :] for i in range(NB)]
            ut, rt = a_co[0] * basis[0], c_co[0] * basis[0]
            for i in range(1, NB):
                if i < CG_ITERS:
                    ut = ut + a_co[i] * basis[i]
                rt = rt + c_co[i] * basis[i]
            ut = u_ref[p + 1, row, :] + ut
            rt = d_ref[p, rows, :] * rt
            u_out[p, rows, :] = ut[:, :HALF]
            u_out[p + NP, rows, :] = turn_half(ut)[:, :HALF]
            r_out[p, rows, :] = rt[:, :HALF]
            r_out[p + NP, rows, :] = turn_half(rt)[:, :HALF]
        return carry

    lax.fori_loop(0, NP, combine, 0, unroll=4)
    h_ref[...] = squares_row(hist_ref, full_ref)
    ok_ref[0, 0] = ok[0, 0].astype(jnp.int32)

    def drain(rnd, carry):
        for face in range(FACES):
            comm.wait_send(rnd, face)
        return carry
    lax.fori_loop(0, CG_ITERS + 2, drain, 0)


def plain_kernel(counts, k_hbm, g_hbm, f_hbm, u_hbm, u_out, r_out, h_ref,
                 raw_k, raw_u, raw_f, slab_x, slab_y, slab_z, k_ref, u_ref, p_ref, q_ref, r_ref, coef_ref, d_ref, tree, square, k_ghost, u_ghost,
                 xs, ys, zs, xr, yr, zr, send_row, rows_a, rows_b,
                 load_sem, send_sem, recv_sem, red_ss, red_rs):
    comm = Comm(counts, (xs, ys, zs, xr, yr, zr, send_sem, recv_sem))
    raws, slabs = (raw_k, raw_u, raw_f), (slab_x, slab_y, slab_z)
    loads = start_up(comm, (k_hbm, g_hbm, f_hbm, u_hbm), raws, slabs, load_sem)
    greet = greet_groups(comm)
    zero_ends(comm, 3)
    first_exchange(comm, loads, greet, raws, slabs, k_ref, u_ref, tree, square, k_ghost, u_ghost)
    red = [Reducer(comm, send_row.at[i], (rows_a.at[i], rows_b.at[i]), red_ss.at[i], red_rs.at[i]) for i in range(2)]

    def reduce(which, accs):
        lane = lane_iota(1)
        row = jnp.zeros((1, LANES), F32)
        for i, acc in enumerate(accs):
            total = row_sum(lane_sum(acc))
            row = jnp.where(lane == i, jnp.broadcast_to(total, (1, LANES)), row)
        row = red[which].run(row)
        return [lane_sum(jnp.where(lane == i, row, 0.0)) for i in range(len(accs))]

    def first(p, state):
        for t in range(ROWS):
            weights, resid, inv = first_residual(raw_f, k_ref, u_ref, k_ghost, u_ghost, p, t, d_ref)
            for i in range(FACES):
                coef_ref[p, t, i] = weights[i]
            r_ref[p, tile(t), :] = resid
            z_new = resid * inv
            p_ref[p + 1, own(t), :] = z_new
            state[0] = state[0] + resid * z_new

    rho, = reduce(0, sweep(first, zero_tiles(1)))

    def iteration(it, carry):
        rho, hist = carry

        send_faces(comm, 2, p_ref, tree)
        for face in range(FACES):
            comm.wait_recv(2, face)
            comm.wait_send(2, face)
        outer_layers(comm, 2, p_ref)
        spread_z(comm, 2, tree, k_ghost)

        def apply(p, state):
            for t in range(ROWS):
                centre, others = neighbours(p_ref, p, t, k_ghost)
                q = total_of(coef_ref[p, t, i] * (centre - others[i]) for i in range(FACES))
                q_ref[p, tile(t), :] = q
                state[0] = state[0] + centre * q

        curv, = reduce(1, sweep(apply, zero_tiles(1)))
        alpha = jnp.broadcast_to(rho / curv, TILE)

        def update(p, accs):
            acc_z, acc_r = accs
            for t in range(ROWS):
                row = own(t)
                rows = tile(t)
                u_ref[p + 1, row, :] = u_ref[p + 1, row, :] + alpha * p_ref[p + 1, row, :]
                resid = r_ref[p, rows, :] - alpha * q_ref[p, rows, :]
                r_ref[p, rows, :] = resid
                acc_z = acc_z + resid * (resid / d_ref[p, rows, :])
                acc_r = acc_r + resid * resid
            return acc_z, acc_r

        rho_new, rr = reduce(0, lax.fori_loop(0, NP, update, zero_tiles(2)))
        beta = jnp.broadcast_to(rho_new / rho, TILE)

        def turn(p, carry):
            for t in range(ROWS):
                row = own(t)
                rows = tile(t)
                p_ref[p + 1, row, :] = r_ref[p, rows, :] / d_ref[p, rows, :] + beta * p_ref[p + 1, row, :]
            return carry

        lax.fori_loop(0, NP, turn, 0)
        hist = jnp.where(lane_iota(1) == it, jnp.broadcast_to(rr, (1, LANES)), hist)
        return rho_new, hist

    _, hist = lax.fori_loop(0, CG_ITERS, iteration, (rho, jnp.zeros((1, LANES), F32)))
    h_ref[...] = hist

    def finish(p, carry):
        write_plane(u_out, p, u_ref[p + 1, R0:R0 + NY, :])
        write_plane(r_out, p, r_ref[p])
        return carry

    lax.fori_loop(0, NP, finish, 0)
    for rnd in range(2):
        for face in range(FACES):
            comm.wait_send(rnd, face)


def finish_kernel(u_in, r_in, u_hbm, r_hbm, sems):
    copies = [pltpu.make_async_copy(u_in, u_hbm, sems.at[0]), pltpu.make_async_copy(r_in, r_hbm, sems.at[1])]
    for copy in copies:
        copy.start()
    for copy in copies:
        copy.wait()


def scratch_for(kind, counts):
    field = (NP + 2, NY + 16, LANES)
    block = (NP, NY, LANES)
    vm = lambda *shape: pltpu.VMEM(shape, F32)
    raws = [vm(NX, NY, NZ)] * 3 + [vm(NY, LANES), vm(NX, LANES), vm(NX, LANES)]
    if kind == 'basis':
        rounds, reds = CG_ITERS + 2, ()
        work = [vm(*field), vm(*field), vm(NB + 1, *field), vm(NP, ROWS, FACES, *TILE), vm(*block), vm(LANES, LANES),
                vm(40, LANES), vm(32, LANES), vm(CG_ITERS, 16, LANES), vm(NB, 16, LANES), vm(2, 16, LANES), vm(*block), vm(*block)]
    else:
        rounds, reds = 3, (2,)
        work = [vm(*field), vm(*field), vm(*field), vm(*block), vm(*block), vm(NP, ROWS, FACES, *TILE), vm(*block)]
    work += [vm(NP, FOLD, LANES), vm(LANES, LANES), vm(*block), vm(*block)]
    x_side, y_side = vm(rounds, 2, FOLD, LANES), vm(rounds + 1, 2, NP, 1, LANES)
    faces = [x_side, y_side, vm(rounds, 2, NP, LANES)] * 2
    sizes = [counts[0], counts[1] * counts[2]]
    rows = [vm(*reds, 2, 1, LANES)] + [vm(*reds, n, 1, LANES) for n in sizes]
    dma = pltpu.SemaphoreType.DMA
    sems = [dma((6,)), dma((rounds, 6)), dma((rounds, 6)), dma((*reds, 2, max(sizes))), dma((*reds, 2, max(sizes)))]
    return raws + work + faces + rows + sems


def solution(mesh):
    counts = tuple(mesh.shape[name] for name in AXES)
    grid_spec = P(*AXES)
    block = jax.ShapeDtypeStruct((NX, NY, NZ), F32)

    def call(kernel, kind, ident, *more):
        hbm, vmem = pl.BlockSpec(memory_space=pltpu.HBM), pl.BlockSpec(memory_space=pltpu.VMEM)
        smem = [pl.BlockSpec(memory_space=pltpu.SMEM)] * len(more)
        return pl.pallas_call(
            functools.partial(kernel, counts),
            out_shape=(block, block, jax.ShapeDtypeStruct((1, LANES), F32), *more),
            in_specs=[hbm] * 4,
            out_specs=(vmem, vmem, vmem, *smem),
            scratch_shapes=scratch_for(kind, counts),
            compiler_params=pltpu.CompilerParams(collective_id=ident, has_side_effects=True, vmem_limit_bytes=VMEM_BYTES),
            name=kind,
        )

    def local_solve(k_cell, k_ghost, f_rhs, u_init):
        args = (k_cell, k_ghost, f_rhs, u_init)
        *fast, ok = call(basis_kernel, 'basis', 0, jax.ShapeDtypeStruct((1, 1), jnp.int32))(*args)
        u_out, r_out, row = lax.cond(ok[0, 0] > 0, lambda: tuple(fast),
                                     lambda: tuple(call(plain_kernel, 'plain', 1)(*args)))
        u_out, r_out = pl.pallas_call(
            finish_kernel,
            out_shape=(block, block),
            in_specs=[pl.BlockSpec(memory_space=pltpu.VMEM)] * 2,
            out_specs=(pl.BlockSpec(memory_space=pltpu.HBM),) * 2,
            scratch_shapes=[pltpu.SemaphoreType.DMA((2,))],
            compiler_params=pltpu.CompilerParams(vmem_limit_bytes=VMEM_BYTES),
            name='finish',
        )(u_out, r_out)
        return u_out, r_out, row[0, 0:CG_ITERS]

    return jax.shard_map(local_solve, mesh=mesh, in_specs=(grid_spec, P(), grid_spec, grid_spec),
                         out_specs=(grid_spec, grid_spec, P()), check_vma=False)
```

```python
import functools

import jax
import jax.numpy as jnp
from jax import lax
from jax.experimental import pallas as pl
from jax.experimental.pallas import tpu as pltpu
from jax.sharding import PartitionSpec as P

CG_ITERS = 8
NB = CG_ITERS + 1
NX, NY, NZ = 32, 64, 64
NP = NX // 2
R0 = 8
MESH = pl.DeviceIdType.MESH
AXES = ('gx', 'gy', 'gz')
BOUND = 4096.0
GRAM = 2 * NB
VMEM_BYTES = 60_000_000
F32 = jnp.float32
SUB, LANES, HALF, LOW = 8, 128, 64, 63
ROWS = NY // SUB
TILE = (SUB, LANES)
WIDE = (2 * SUB, LANES)
FACES = 6
FOLD = NY // 2
TURNS = ((4, 8, 12), (16, 32, 48))


def own(t):
    return slice(R0 + SUB * t, R0 + SUB * t + SUB)


def tile(t):
    return slice(SUB * t, SUB * t + SUB)


def one(i):
    return slice(i, i + 1)


def spin(values, by):
    return pltpu.roll(values, by, 1)


def turn_half(values):
    return spin(values, HALF)


def row_sum(values):
    return jnp.sum(values, axis=0, keepdims=True)


def lane_sum(values):
    return jnp.sum(values, axis=1, keepdims=True)


def total_of(parts):
    parts = list(parts)
    while len(parts) > 1:
        parts = [sum(parts[i + 1:i + 2], parts[i]) for i in range(0, len(parts), 2)]
    return parts[0]


def lane_iota(rows=8):
    return lax.broadcasted_iota(jnp.int32, (rows, LANES), 1)


def row_iota(rows):
    return lax.broadcasted_iota(jnp.int32, (rows, LANES), 0)


class Comm:
    def __init__(self, counts, bufs):
        self.counts = counts
        self.pos = [lax.axis_index(name) for name in AXES]
        self.has = []
        for axis in range(3):
            self.has.append(self.pos[axis] > 0)
            self.has.append(self.pos[axis] < counts[axis] - 1)
        (self.xs, self.ys, self.zs, self.xr, self.yr, self.zr, self.send_sem, self.recv_sem) = bufs

    def neighbour(self, face):
        return {AXES[face // 2]: self.pos[face // 2] + (1 if face % 2 else -1)}

    def source(self, rnd, face):
        axis, high = face // 2, face % 2
        return (self.xs, self.ys, self.zs)[axis].at[rnd, high]

    def copies(self, rnd, face):
        axis, high = face // 2, face % 2
        src = self.source(rnd, face)
        dst = (self.xr, self.yr, self.zr)[axis]
        return pltpu.make_async_remote_copy(
            src_ref=src, dst_ref=dst.at[rnd, 1 - high],
            send_sem=self.send_sem.at[rnd, face], recv_sem=self.recv_sem.at[rnd, face ^ 1],
            device_id=self.neighbour(face), device_id_type=MESH)

    def send(self, rnd, face):
        @pl.when(self.has[face])
        def _():
            self.copies(rnd, face).start()

    def wait_recv(self, rnd, face):
        axis, high = face // 2, face % 2
        src = self.source(rnd, face)
        dst = (self.xr, self.yr, self.zr)[axis]

        @pl.when(self.has[face])
        def _():
            pltpu.make_async_remote_copy(
                src_ref=src, dst_ref=dst.at[rnd, high],
                send_sem=self.send_sem.at[rnd, face], recv_sem=self.recv_sem.at[rnd, face],
                device_id=self.neighbour(face), device_id_type=MESH).wait_recv()

    def wait_send(self, rnd, face):
        @pl.when(self.has[face])
        def _():
            self.copies(rnd, face).wait_send()


GROUPS = (('gx',), ('gy', 'gz'))


def group_of(comm, group):
    sizes = [comm.counts[AXES.index(name)] for name in group]
    size, rank = 1, 0
    for name, n in zip(group, sizes):
        size, rank = size * n, rank * n + comm.pos[AXES.index(name)]

    def peer(off):
        left, where = lax.rem(rank + off, size), {}
        for name, n in reversed(tuple(zip(group, sizes))):
            where[name], left = lax.rem(left, n), lax.div(left, n)
        return where
    return size, rank, peer


def greet_faces(comm):
    sem = pltpu.get_barrier_semaphore()
    for face in range(FACES):
        @pl.when(comm.has[face])
        def _():
            pl.semaphore_signal(sem, inc=1, device_id=comm.neighbour(face), device_id_type=MESH)
    return sem, sum(flag.astype(jnp.int32) for flag in comm.has)


def greet_groups(comm):
    sem, total = pltpu.get_barrier_semaphore(), 0
    for group in GROUPS:
        size, _, peer = group_of(comm, group)
        for off in range(1, size):
            pl.semaphore_signal(sem, inc=1, device_id=peer(off), device_id_type=MESH)
        total += size - 1
    return sem, total


class Reducer:
    def __init__(self, comm, send_row, recv_rows, send_sem, recv_sem):
        self.comm, self.send_row, self.recv_rows, self.ss, self.rs = comm, send_row, recv_rows, send_sem, recv_sem

    def run(self, row):
        for stage, group in enumerate(GROUPS):
            size, rank, peer = group_of(self.comm, group)
            rows = self.recv_rows[stage]
            self.send_row[stage] = row
            copies = [pltpu.make_async_remote_copy(
                src_ref=self.send_row.at[stage], dst_ref=rows.at[rank], send_sem=self.ss.at[stage, off],
                recv_sem=self.rs.at[stage, off], device_id=peer(off), device_id_type=MESH) for off in range(1, size)]
            for copy in copies:
                copy.start()
            rows[rank] = row
            for copy in copies:
                copy.wait()
            row = total_of(rows[i] for i in range(size))
        return row


def store_plane_faces(comm, rnd, ref, p):
    comm.ys[rnd, 0, p] = ref[p + 1, R0:R0 + 1, :]
    comm.ys[rnd, 1, p] = ref[p + 1, R0 + NY - 1:R0 + NY, :]


def pack_x_faces(comm, rnd, ref):
    half = FOLD
    lane = lane_iota(half)
    a, b = ref[1, R0:R0 + half, :], ref[1, R0 + half:R0 + NY, :]
    comm.xs[rnd, 0] = jnp.where(lane < HALF, a, turn_half(b))
    a, b = ref[NP, R0:R0 + half, :], ref[NP, R0 + half:R0 + NY, :]
    comm.xs[rnd, 1] = jnp.where(lane < HALF, turn_half(a), b)


def face_mask(turn, rows=FOLD):
    return ((lane_iota(rows) + 1) & LOW) < turn


def pack_z(comm, rnd, ref, tree):
    def fold(p, carry):
        low, high = ref[p + 1, R0:R0 + FOLD, :], ref[p + 1, R0 + FOLD:R0 + NY, :]
        tree[p] = jnp.where(face_mask(2), low, spin(high, 2))
        return carry
    lax.fori_loop(0, NP, fold, 0, unroll=NP)
    join_z(comm, rnd, tree)


def join_z(comm, rnd, tree):
    parts = [tree[p] for p in range(NP)]
    for turns in TURNS:
        merged = []
        for i in range(0, NP, 4)[:len(parts) // 4]:
            out = spin(parts[i + 3], turns[-1])
            for n in (2, 1):
                out = jnp.where(face_mask(turns[n]), spin(parts[i + n], turns[n - 1]), out)
            merged.append(jnp.where(face_mask(turns[0]), parts[i], out))
        parts = merged
    for end in range(2):
        comm.zs[rnd, end] = halve_z(parts[0], 1 - end)


def halve_z(packed, keep):
    even = (lane_iota(NP) & 1) == 1 - keep
    return jnp.where(even, packed[:NP], spin(packed[NP:], 1 if keep else LANES - 1))


def unpack_z(comm, rnd, tree):
    odd = (lane_iota(NP) & 1) == 1
    low, high = comm.zr[rnd, 0], comm.zr[rnd, 1]
    parts = [jnp.concatenate([jnp.where(odd, spin(high, LOW - 2 - i), spin(low, LOW + i)) for i in range(2)], axis=0)]
    for turns in reversed(TURNS):
        parts = [q for part in parts for q in (part, *(spin(part, LANES - turn) for turn in turns))]
    for p in range(NP):
        tree[p] = parts[p]


def spread_z(comm, rnd, tree, ghost):
    unpack_z(comm, rnd, tree)

    def fold(p, carry):
        ghost[p, 0:FOLD, :] = spin(tree[p], 2)
        ghost[p, FOLD:NY, :] = tree[p]
        return carry
    lax.fori_loop(0, NP, fold, 0, unroll=NP)


def inner_planes(ref):
    low = lane_iota(NY) < HALF
    ref[0, R0:R0 + NY, :] = jnp.where(low, 0.0, turn_half(ref[NP, R0:R0 + NY, :]))
    ref[NP + 1, R0:R0 + NY, :] = jnp.where(low, turn_half(ref[1, R0:R0 + NY, :]), 0.0)


def x_ghosts(comm, rnd):
    low = lane_iota(FOLD) < HALF
    lo, hi = comm.xr[rnd, 0], comm.xr[rnd, 1]
    below = [jnp.where(low, lo, 0.0), jnp.where(low, turn_half(lo), 0.0)]
    above = [jnp.where(low, 0.0, turn_half(hi)), jnp.where(low, 0.0, hi)]
    return below, above


def outer_layers(comm, rnd, ref):
    inner_planes(ref)
    below, above = x_ghosts(comm, rnd)
    for i in range(2):
        rows = slice(R0 + FOLD * i, R0 + FOLD * i + FOLD)
        ref[0, rows, :] = ref[0, rows, :] + below[i]
        ref[NP + 1, rows, :] = ref[NP + 1, rows, :] + above[i]
    for p in range(NP):
        ref[p + 1, R0 - 1:R0, :] = comm.yr[rnd, 0, p]
        ref[p + 1, R0 + NY:R0 + NY + 1, :] = comm.yr[rnd, 1, p]


def blank_rows(ref):
    for p in range(NP):
        ref[p + 1, R0 - 1:R0, :] = jnp.zeros((1, LANES), F32)
        ref[p + 1, R0 + NY:R0 + NY + 1, :] = jnp.zeros((1, LANES), F32)


def neighbours(ref, p, t, ghost=None):
    row = R0 + SUB * t
    lane = lane_iota() & LOW
    centre = ref[p + 1, own(t), :]
    xm = ref[p, own(t), :]
    xp = ref[p + 2, own(t), :]
    ym = ref[p + 1, row - 1:row + SUB - 1, :]
    yp = ref[p + 1, row + 1:row + SUB + 1, :]
    zm, zp = spin(centre, 1), spin(centre, LANES - 1)
    if ghost is not None:
        edge = ghost[p, tile(t), :]
        zm, zp = jnp.where(lane == 0, edge, zm), jnp.where(lane == LOW, edge, zp)
    return centre, (xm, xp, ym, yp, zm, zp)


def sweep(body, state=(), unroll=2):
    def plane(p, carry):
        carry = list(carry)
        body(p, carry)
        return tuple(carry)
    return lax.fori_loop(0, NP, plane, tuple(state), unroll=unroll)


def zero_tiles(n):
    return tuple(jnp.zeros(TILE, F32) for _ in range(n))


def send_faces(comm, rnd, ref, tree, folded=False):
    if not folded:
        for p in range(NP):
            store_plane_faces(comm, rnd, ref, p)
    for face in (2, 3):
        comm.send(rnd, face)
    (join_z if folded else functools.partial(pack_z, ref=ref))(comm, rnd, tree=tree)
    for face in (4, 5):
        comm.send(rnd, face)
    pack_x_faces(comm, rnd, ref)
    for face in (0, 1):
        comm.send(rnd, face)


def load_field(raw, ref):
    def body(p, state):
        ref[p + 1, R0:R0 + NY, :] = jnp.concatenate([raw[p], raw[p + NP]], axis=1)
    sweep(body, unroll=NP)


def fill_ghost_conductivity(comm, square, gx_slab, gy_slab, gz_slab):
    px, py, pz = comm.pos
    half = FOLD
    turn = 64 * lax.rem(pz, 2)
    lane = lane_iota(half)
    a, b = pltpu.roll(gx_slab[0:half, :], turn, 1), pltpu.roll(gx_slab[half:NY, :], turn, 1)
    x_face = jnp.where(lane < HALF, a, turn_half(b))
    for end in range(2):
        @pl.when(jnp.logical_not(comm.has[end]))
        def _():
            comm.xr[0, end] = x_face
    rows = pltpu.roll(gy_slab[...], turn, 1)
    y_face = jnp.where(lane_iota(NP) < HALF, rows[0:NP], turn_half(rows[NP:NX]))
    for end in range(2):
        @pl.when(jnp.logical_not(comm.has[2 + end]))
        def _():
            for p in range(NP):
                comm.yr[0, end, p] = y_face[one(p)]
    for end in range(2):
        @pl.when(jnp.logical_not(comm.has[4 + end]))
        def _():
            cols = spin(gz_slab[...], HALF * lax.rem(py, 2))
            shift = 0 if end else LOW
            square[...] = jnp.zeros(square.shape, F32)
            for x in range(NX):
                for c in range(2):
                    square[one((4 * (x % NP) + 2 * c + HALF * (x // NP) + shift) % LANES)] = cols[one(x)]
            turned = square[...].T
            second = ((lane_iota(FOLD) - shift) & 3) == 2
            comm.zr[0, end] = halve_z(jnp.where(second, turned[FOLD:NY], turned[:FOLD]), end)


def zero_ends(comm, rounds):
    for face in range(FACES):
        @pl.when(jnp.logical_not(comm.has[face]))
        def _():
            buf = (comm.xr, comm.yr, comm.zr)[face // 2]

            def clear(rnd, carry):
                buf[rnd, face % 2] = jnp.zeros(buf.shape[2:], F32)
                return carry
            lax.fori_loop(1, rounds, clear, 0)


def lanes_of(pos):
    return pl.ds(pl.multiple_of(lax.div(pos, 2) * LANES, LANES), LANES)


def start_up(comm, ins, raws, slabs, load_sem):
    k_hbm, g_hbm, f_hbm, u_hbm = ins
    px, py, pz = comm.pos
    loads = [pltpu.make_async_copy(k_hbm, raws[0], load_sem.at[0]),
             pltpu.make_async_copy(u_hbm, raws[1], load_sem.at[1])]
    x_row = jnp.where(comm.has[1], 0, 1)
    y_row = jnp.where(comm.has[3], 2, 3)
    z_row = jnp.where(comm.has[5], 4, 5)
    z_lanes = lanes_of(pz)
    y_lanes = lanes_of(py)
    loads.append(pltpu.make_async_copy(
        g_hbm.at[x_row, pl.ds(pl.multiple_of(py * NY, NY), NY), z_lanes], slabs[0], load_sem.at[2]))
    loads.append(pltpu.make_async_copy(
        g_hbm.at[y_row, pl.ds(pl.multiple_of(px * NX, NX), NX), z_lanes], slabs[1], load_sem.at[3]))
    loads.append(pltpu.make_async_copy(
        g_hbm.at[z_row, pl.ds(pl.multiple_of(px * NX, NX), NX), y_lanes], slabs[2], load_sem.at[4]))
    loads.append(pltpu.make_async_copy(f_hbm, raws[2], load_sem.at[5]))
    for load in loads:
        load.start()
    return loads


def first_exchange(comm, loads, greet, raws, slabs, k_ref, u_ref, tree, square, k_ghost, u_ghost):
    sem, total = greet
    loads[0].wait()
    load_field(raws[0], k_ref)
    pl.semaphore_wait(sem, total)
    send_faces(comm, 0, k_ref, tree)
    loads[1].wait()
    load_field(raws[1], u_ref)
    send_faces(comm, 1, u_ref, tree)
    for load in loads[2:]:
        load.wait()
    fill_ghost_conductivity(comm, square, *slabs)
    for rnd, ref, ghost in ((0, k_ref, k_ghost), (1, u_ref, u_ghost)):
        for face in range(FACES):
            comm.wait_recv(rnd, face)
        outer_layers(comm, rnd, ref)
        spread_z(comm, rnd, tree, ghost)


def first_residual(raw_f, k_ref, u_ref, k_ghost, u_ghost, p, t, d_ref):
    centre, others = neighbours(k_ref, p, t, k_ghost)
    u_own, u_others = neighbours(u_ref, p, t, u_ghost)
    twice = centre + centre
    weights = [twice * other / (centre + other) for other in others]
    diag = total_of(weights)
    au = total_of([w * (u_own - other) for w, other in zip(weights, u_others)])
    f_tile = jnp.concatenate([raw_f[p, tile(t), :], raw_f[p + NP, tile(t), :]], axis=1)
    d_ref[p, tile(t), :] = diag
    return weights, f_tile - au, 1.0 / diag


def write_plane(raw_ref, p, values):
    raw_ref[p] = values[:, :HALF]
    raw_ref[p + NP] = turn_half(values)[:, :HALF]


def dot_rows(a, b):
    prod = a[:2 * SUB] * b[:2 * SUB]
    return row_sum(prod[:SUB] + prod[SUB:])


def solve_coefficients(row, mom_ref, pc_ref, hist_ref, full_ref):
    lane24, line24 = lane_iota(24), row_iota(24)
    wide = jnp.broadcast_to(row, (24, LANES))
    base = lane_sum(jnp.where((lane24 == line24 + 1) & (line24 < 17), wide, 0.0))
    base = jnp.broadcast_to(base, (24, LANES))
    first, second = base[0:1], base[1:2]
    even = (line24 & 1) == 0
    mom = jnp.where(line24 >= 2, 2.0 * base - jnp.where(even, first, second), base)
    mom = jnp.where(line24 < 17, mom, 0.0)
    lane16, line16 = lane_iota(16), row_iota(16)
    wide = jnp.broadcast_to(row, WIDE)
    for k in range(NB):
        big = jnp.maximum(line16, k)
        small = jnp.minimum(line16, k)
        want = GRAM + NB * big + small
        col = lane_sum(jnp.where((lane16 == want) & (line16 < NB), wide, 0.0))
        full_ref[k] = jnp.broadcast_to(col, WIDE)
    zeros8 = jnp.zeros(TILE, F32)
    mom_ref[:SUB] = zeros8
    mom_ref[32:40] = zeros8
    pc_ref[:SUB] = zeros8
    pc_ref[24:32] = zeros8
    unit = jnp.where(line16 == 0, 1.0, 0.0)
    cvec, pvec, avec = unit, unit, jnp.zeros(WIDE, F32)
    rvec, mvec = mom, mom
    mu0 = mom[0:1]
    rho = dot_rows(cvec, rvec)
    ok = jnp.where(rho > 0.0, 1.0, 0.0)
    two_one = jnp.where(line16 == 1, 2.0, 1.0)
    for t in range(CG_ITERS):
        mom_ref[8:32] = mvec
        mom_ref[7:8] = mvec[1:2]
        pc_ref[8:24] = pvec
        qvec = mvec - 0.5 * (mom_ref[9:33] + mom_ref[7:31])
        npvec = 0.5 * (two_one * pc_ref[7:23] + pc_ref[9:25])
        curv = dot_rows(pvec, qvec)
        size = row_sum(jnp.abs(pvec))
        ok = jnp.where(size * size * mu0 < BOUND * curv, ok, 0.0)
        alpha = rho / curv
        avec = avec + alpha * pvec
        cvec = cvec - alpha * (pvec - npvec)
        rvec = rvec - alpha * qvec
        hist_ref[t] = cvec
        rho_new = dot_rows(cvec, rvec)
        size = row_sum(jnp.abs(cvec))
        ok = jnp.where(size * size * mu0 < BOUND * rho_new, ok, 0.0)
        beta = rho_new / rho
        pvec = cvec + beta * pvec
        mvec = rvec + beta * mvec
        rho = rho_new
    return avec, cvec, ok


def squares_row(hist_ref, full_ref):
    lane = lane_iota(1)
    out = jnp.zeros((1, LANES), F32)
    for t in range(CG_ITERS):
        cvec = hist_ref[t]
        acc = full_ref[0] * hist_ref[t, one(0)]
        for j in range(1, NB):
            acc = acc + full_ref[j] * hist_ref[t, one(j)]
        out = jnp.where(lane == t, dot_rows(acc, cvec), out)
    return out


def basis_kernel(counts, k_hbm, g_hbm, f_hbm, u_hbm, u_out, r_out, h_ref, ok_ref,
                 raw_k, raw_u, raw_f, slab_x, slab_y, slab_z, k_ref, u_ref, z_ref, coef_ref, d_ref, sums_ref,
                 mom_ref, pc_ref, hist_ref, full_ref, comb_ref, edge_ref, part_ref, tree, square, k_ghost, u_ghost,
                 xs, ys, zs, xr, yr, zr, send_row, rows_a, rows_b,
                 load_sem, send_sem, recv_sem, red_ss, red_rs):
    comm = Comm(counts, (xs, ys, zs, xr, yr, zr, send_sem, recv_sem))
    raws, slabs = (raw_k, raw_u, raw_f), (slab_x, slab_y, slab_z)
    loads = start_up(comm, (k_hbm, g_hbm, f_hbm, u_hbm), raws, slabs, load_sem)
    greet = greet_faces(comm)
    zero_ends(comm, CG_ITERS + 2)
    sums_ref[...] = jnp.zeros(sums_ref.shape, F32)

    def blank(k, carry):
        blank_rows(z_ref.at[k + 1])
        return carry
    lax.fori_loop(0, CG_ITERS, blank, 0)

    def nothing(p, state):
        z_ref[0, p + 1, R0:R0 + NY, :] = jnp.zeros((NY, LANES), F32)
    sweep(nothing, unroll=4)
    first_exchange(comm, loads, greet, raws, slabs, k_ref, u_ref, tree, square, k_ghost, u_ghost)

    def first(p, state):
        lane = lane_iota() & LOW
        for t in range(ROWS):
            weights, resid, inv = first_residual(raw_f, k_ref, u_ref, k_ghost, u_ghost, p, t, d_ref)
            factor = inv + inv
            scaled = [w * factor for w in weights]
            low, high = scaled[4:]
            edge_ref[p, tile(t), :] = jnp.where(lane == 0, low, jnp.where(lane == LOW, high, 0.0))
            scaled[4:] = jnp.where(lane == 0, 0.0, low), jnp.where(lane == LOW, 0.0, high)
            for i in range(FACES):
                coef_ref[p, t, i] = scaled[i]
            z_ref[1, p + 1, own(t), :] = resid * inv

    sweep(first, unroll=8)
    send_faces(comm, 2, z_ref.at[1], tree)

    def products(k):
        def body(p, accs):
            for t in range(ROWS):
                d = d_ref[p, tile(t), :]
                z_k = z_ref[k + 1, p + 1, own(t), :]
                dz = d * z_k
                ddz = d * dz
                for i in range(NB):
                    accs[i] = accs[i] + ddz * z_ref[i + 1, p + 1, own(t), :]
                accs[NB] = accs[NB] + dz * z_k
                accs[NB + 1] = accs[NB + 1] + dz * z_ref[k, p + 1, own(t), :]
        accs = sweep(body, zero_tiles(NB + 2), unroll=4)
        rows = [GRAM + NB * k + i for i in range(NB)] + [2 * k + 1, 2 * k]
        for row, acc in zip(rows, accs):
            sums_ref[pl.ds(row, 1), :] = row_sum(acc)

    def weight(k):
        return jnp.where(k == 0, 0.5, 1.0)

    def x_terms(k, rnd):
        factor = weight(k)
        below, above = x_ghosts(comm, rnd)
        for t in range(ROWS):
            part = slice(SUB * (t % 4), SUB * (t % 4) + SUB)
            for plane, face, layer in ((0, 0, below), (NP - 1, 1, above)):
                term = coef_ref[plane, t, face] * layer[t // 4][part]
                part_ref[plane, tile(t), :] = part_ref[plane, tile(t), :] + factor * term

    def late_terms(k, rnd):
        ref, factor = z_ref.at[k + 2], weight(k)
        unpack_z(comm, rnd, tree)
        first, last = row_iota(SUB) == 0, row_iota(SUB) == SUB - 1

        def body(p, state):
            turned = [spin(tree[p], 2), tree[p]]
            news = []
            for t in range(ROWS):
                part = slice(SUB * (t % 4), SUB * (t % 4) + SUB)
                term = edge_ref[p, tile(t), :] * turned[t // 4][part]
                for end, at, sub, mask in ((0, 0, 0, first), (1, ROWS - 1, SUB - 1, last)):
                    if t == at:
                        line = coef_ref[p, t, 2 + end, one(sub), :] * comm.yr[rnd, end, p]
                        term = term + jnp.where(mask, line, 0.0)
                news.append(part_ref[p, tile(t), :] + factor * term)
                ref[p + 1, own(t), :] = news[t]
            comm.ys[rnd + 1, 0, p] = news[0][:1]
            comm.ys[rnd + 1, 1, p] = news[ROWS - 1][SUB - 1:]
            for t in range(4):
                tree[p, tile(t), :] = jnp.where(face_mask(2, SUB), news[t], spin(news[t + 4], 2))
        sweep(body, unroll=NP)

    def apply(k, carry):
        rnd, factor = k + 2, weight(k)
        ref = z_ref.at[k + 1]
        inner_planes(ref)

        def step(p, state):
            for t in range(ROWS):
                _, others = neighbours(ref, p, t)
                total = total_of(coef_ref[p, t, i] * others[i] for i in range(FACES))
                part_ref[p, tile(t), :] = factor * total - z_ref[k, p + 1, own(t), :]

        sweep(step)
        products(k)
        for face in range(FACES):
            comm.wait_recv(rnd, face)
            if face == 1:
                x_terms(k, rnd)
        late_terms(k, rnd)

        @pl.when(k < CG_ITERS - 1)
        def _():
            send_faces(comm, rnd + 1, z_ref.at[k + 2], tree, folded=True)
        return carry

    lax.fori_loop(0, CG_ITERS, apply, 0)
    products(CG_ITERS)

    total = jnp.broadcast_to(lane_sum(sums_ref[...]), (LANES, LANES))
    row = row_sum(jnp.where(lane_iota(LANES) == row_iota(LANES), total, 0.0))
    red = Reducer(comm, send_row, (rows_a, rows_b), red_ss, red_rs)
    row = red.run(row)
    avec, cvec, ok = solve_coefficients(row, mom_ref, pc_ref, hist_ref, full_ref)
    comb_ref[0] = avec
    comb_ref[1] = cvec

    a_co = [jnp.broadcast_to(comb_ref[0, one(i)], TILE) for i in range(CG_ITERS)]
    c_co = [jnp.broadcast_to(comb_ref[1, one(i)], TILE) for i in range(NB)]

    def combine(p, carry):
        for t in range(ROWS):
            row = own(t)
            rows = tile(t)
            basis = [z_ref[i + 1, p + 1, row, :] for i in range(NB)]
            ut, rt = a_co[0] * basis[0], c_co[0] * basis[0]
            for i in range(1, NB):
                if i < CG_ITERS:
                    ut = ut + a_co[i] * basis[i]
                rt = rt + c_co[i] * basis[i]
            ut = u_ref[p + 1, row, :] + ut
            rt = d_ref[p, rows, :] * rt
            u_out[p, rows, :] = ut[:, :HALF]
            u_out[p + NP, rows, :] = turn_half(ut)[:, :HALF]
            r_out[p, rows, :] = rt[:, :HALF]
            r_out[p + NP, rows, :] = turn_half(rt)[:, :HALF]
        return carry

    lax.fori_loop(0, NP, combine, 0, unroll=8)
    h_ref[...] = squares_row(hist_ref, full_ref)
    ok_ref[0, 0] = ok[0, 0].astype(jnp.int32)

    def drain(rnd, carry):
        for face in range(FACES):
            comm.wait_send(rnd, face)
        return carry
    lax.fori_loop(0, CG_ITERS + 2, drain, 0)


def plain_kernel(counts, k_hbm, g_hbm, f_hbm, u_hbm, u_out, r_out, h_ref,
                 raw_k, raw_u, raw_f, slab_x, slab_y, slab_z, k_ref, u_ref, p_ref, q_ref, r_ref, coef_ref, d_ref, tree, square, k_ghost, u_ghost,
                 xs, ys, zs, xr, yr, zr, send_row, rows_a, rows_b,
                 load_sem, send_sem, recv_sem, red_ss, red_rs):
    comm = Comm(counts, (xs, ys, zs, xr, yr, zr, send_sem, recv_sem))
    raws, slabs = (raw_k, raw_u, raw_f), (slab_x, slab_y, slab_z)
    loads = start_up(comm, (k_hbm, g_hbm, f_hbm, u_hbm), raws, slabs, load_sem)
    greet = greet_groups(comm)
    zero_ends(comm, 3)
    first_exchange(comm, loads, greet, raws, slabs, k_ref, u_ref, tree, square, k_ghost, u_ghost)
    red = [Reducer(comm, send_row.at[i], (rows_a.at[i], rows_b.at[i]), red_ss.at[i], red_rs.at[i]) for i in range(2)]

    def reduce(which, accs):
        lane = lane_iota(1)
        row = jnp.zeros((1, LANES), F32)
        for i, acc in enumerate(accs):
            total = row_sum(lane_sum(acc))
            row = jnp.where(lane == i, jnp.broadcast_to(total, (1, LANES)), row)
        row = red[which].run(row)
        return [lane_sum(jnp.where(lane == i, row, 0.0)) for i in range(len(accs))]

    def first(p, state):
        for t in range(ROWS):
            weights, resid, inv = first_residual(raw_f, k_ref, u_ref, k_ghost, u_ghost, p, t, d_ref)
            for i in range(FACES):
                coef_ref[p, t, i] = weights[i]
            r_ref[p, tile(t), :] = resid
            z_new = resid * inv
            p_ref[p + 1, own(t), :] = z_new
            state[0] = state[0] + resid * z_new

    rho, = reduce(0, sweep(first, zero_tiles(1)))

    def iteration(it, carry):
        rho, hist = carry

        send_faces(comm, 2, p_ref, tree)
        for face in range(FACES):
            comm.wait_recv(2, face)
            comm.wait_send(2, face)
        outer_layers(comm, 2, p_ref)
        spread_z(comm, 2, tree, k_ghost)

        def apply(p, state):
            for t in range(ROWS):
                centre, others = neighbours(p_ref, p, t, k_ghost)
                q = total_of(coef_ref[p, t, i] * (centre - others[i]) for i in range(FACES))
                q_ref[p, tile(t), :] = q
                state[0] = state[0] + centre * q

        curv, = reduce(1, sweep(apply, zero_tiles(1)))
        alpha = jnp.broadcast_to(rho / curv, TILE)

        def update(p, accs):
            acc_z, acc_r = accs
            for t in range(ROWS):
                row = own(t)
                rows = tile(t)
                u_ref[p + 1, row, :] = u_ref[p + 1, row, :] + alpha * p_ref[p + 1, row, :]
                resid = r_ref[p, rows, :] - alpha * q_ref[p, rows, :]
                r_ref[p, rows, :] = resid
                acc_z = acc_z + resid * (resid / d_ref[p, rows, :])
                acc_r = acc_r + resid * resid
            return acc_z, acc_r

        rho_new, rr = reduce(0, lax.fori_loop(0, NP, update, zero_tiles(2)))
        beta = jnp.broadcast_to(rho_new / rho, TILE)

        def turn(p, carry):
            for t in range(ROWS):
                row = own(t)
                rows = tile(t)
                p_ref[p + 1, row, :] = r_ref[p, rows, :] / d_ref[p, rows, :] + beta * p_ref[p + 1, row, :]
            return carry

        lax.fori_loop(0, NP, turn, 0)
        hist = jnp.where(lane_iota(1) == it, jnp.broadcast_to(rr, (1, LANES)), hist)
        return rho_new, hist

    _, hist = lax.fori_loop(0, CG_ITERS, iteration, (rho, jnp.zeros((1, LANES), F32)))
    h_ref[...] = hist

    def finish(p, carry):
        write_plane(u_out, p, u_ref[p + 1, R0:R0 + NY, :])
        write_plane(r_out, p, r_ref[p])
        return carry

    lax.fori_loop(0, NP, finish, 0)
    for rnd in range(2):
        for face in range(FACES):
            comm.wait_send(rnd, face)


def finish_kernel(u_in, r_in, u_hbm, r_hbm, sems):
    copies = [pltpu.make_async_copy(u_in, u_hbm, sems.at[0]), pltpu.make_async_copy(r_in, r_hbm, sems.at[1])]
    for copy in copies:
        copy.start()
    for copy in copies:
        copy.wait()


def scratch_for(kind, counts):
    field = (NP + 2, NY + 16, LANES)
    block = (NP, NY, LANES)
    vm = lambda *shape: pltpu.VMEM(shape, F32)
    raws = [vm(NX, NY, NZ)] * 3 + [vm(NY, LANES), vm(NX, LANES), vm(NX, LANES)]
    if kind == 'basis':
        rounds, reds = CG_ITERS + 2, ()
        work = [vm(*field), vm(*field), vm(NB + 1, *field), vm(NP, ROWS, FACES, *TILE), vm(*block), vm(LANES, LANES),
                vm(40, LANES), vm(32, LANES), vm(CG_ITERS, 16, LANES), vm(NB, 16, LANES), vm(2, 16, LANES), vm(*block), vm(*block)]
    else:
        rounds, reds = 3, (2,)
        work = [vm(*field), vm(*field), vm(*field), vm(*block), vm(*block), vm(NP, ROWS, FACES, *TILE), vm(*block)]
    work += [vm(NP, FOLD, LANES), vm(LANES, LANES), vm(*block), vm(*block)]
    x_side, y_side = vm(rounds, 2, FOLD, LANES), vm(rounds + 1, 2, NP, 1, LANES)
    faces = [x_side, y_side, vm(rounds, 2, NP, LANES)] * 2
    sizes = [counts[0], counts[1] * counts[2]]
    rows = [vm(*reds, 2, 1, LANES)] + [vm(*reds, n, 1, LANES) for n in sizes]
    dma = pltpu.SemaphoreType.DMA
    sems = [dma((6,)), dma((rounds, 6)), dma((rounds, 6)), dma((*reds, 2, max(sizes))), dma((*reds, 2, max(sizes)))]
    return raws + work + faces + rows + sems


def solution(mesh):
    counts = tuple(mesh.shape[name] for name in AXES)
    grid_spec = P(*AXES)
    block = jax.ShapeDtypeStruct((NX, NY, NZ), F32)

    def call(kernel, kind, ident, *more):
        hbm, vmem = pl.BlockSpec(memory_space=pltpu.HBM), pl.BlockSpec(memory_space=pltpu.VMEM)
        smem = [pl.BlockSpec(memory_space=pltpu.SMEM)] * len(more)
        return pl.pallas_call(
            functools.partial(kernel, counts),
            out_shape=(block, block, jax.ShapeDtypeStruct((1, LANES), F32), *more),
            in_specs=[hbm] * 4,
            out_specs=(vmem, vmem, vmem, *smem),
            scratch_shapes=scratch_for(kind, counts),
            compiler_params=pltpu.CompilerParams(collective_id=ident, has_side_effects=True, vmem_limit_bytes=VMEM_BYTES),
            name=kind,
        )

    def local_solve(k_cell, k_ghost, f_rhs, u_init):
        args = (k_cell, k_ghost, f_rhs, u_init)
        *fast, ok = call(basis_kernel, 'basis', 0, jax.ShapeDtypeStruct((1, 1), jnp.int32))(*args)
        u_out, r_out, row = lax.cond(ok[0, 0] > 0, lambda: tuple(fast),
                                     lambda: tuple(call(plain_kernel, 'plain', 1)(*args)))
        u_out, r_out = pl.pallas_call(
            finish_kernel,
            out_shape=(block, block),
            in_specs=[pl.BlockSpec(memory_space=pltpu.VMEM)] * 2,
            out_specs=(pl.BlockSpec(memory_space=pltpu.HBM),) * 2,
            scratch_shapes=[pltpu.SemaphoreType.DMA((2,))],
            compiler_params=pltpu.CompilerParams(vmem_limit_bytes=VMEM_BYTES),
            name='finish',
        )(u_out, r_out)
        return u_out, r_out, row[0, 0:CG_ITERS]

    return jax.shard_map(local_solve, mesh=mesh, in_specs=(grid_spec, P(), grid_spec, grid_spec),
                         out_specs=(grid_spec, grid_spec, P()), check_vma=False)
```

```python
import functools

import jax
import jax.numpy as jnp
from jax import lax
from jax.experimental import pallas as pl
from jax.experimental.pallas import tpu as pltpu
from jax.sharding import PartitionSpec as P

CG_ITERS = 8
NB = CG_ITERS + 1
NX, NY, NZ = 32, 64, 64
NP = NX // 2
R0 = 8
MESH = pl.DeviceIdType.MESH
AXES = ('gx', 'gy', 'gz')
BOUND = 4096.0
GRAM = 2 * NB
VMEM_BYTES = 60_000_000
F32 = jnp.float32
SUB, LANES, HALF, LOW = 8, 128, 64, 63
ROWS = NY // SUB
TILE = (SUB, LANES)
WIDE = (2 * SUB, LANES)
FACES = 6
PARTS = 4
FOLD = NY // 2
TURNS = ((4, 8, 12), (16, 32, 48))


def own(t):
    return slice(R0 + SUB * t, R0 + SUB * t + SUB)


def tile(t):
    return slice(SUB * t, SUB * t + SUB)


def one(i):
    return slice(i, i + 1)


def spin(values, by):
    return pltpu.roll(values, by, 1)


def turn_half(values):
    return spin(values, HALF)


def row_sum(values):
    return jnp.sum(values, axis=0, keepdims=True)


def lane_sum(values):
    return jnp.sum(values, axis=1, keepdims=True)


def total_of(parts):
    parts = list(parts)
    while len(parts) > 1:
        parts = [sum(parts[i + 1:i + 2], parts[i]) for i in range(0, len(parts), 2)]
    return parts[0]


def lane_iota(rows=8):
    return lax.broadcasted_iota(jnp.int32, (rows, LANES), 1)


def row_iota(rows):
    return lax.broadcasted_iota(jnp.int32, (rows, LANES), 0)


class Comm:
    def __init__(self, counts, bufs):
        self.counts = counts
        self.pos = [lax.axis_index(name) for name in AXES]
        self.has = []
        for axis in range(3):
            self.has.append(self.pos[axis] > 0)
            self.has.append(self.pos[axis] < counts[axis] - 1)
        (self.xs, self.ys, self.zs, self.xr, self.yr, self.zr, self.send_sem, self.recv_sem) = bufs

    def neighbour(self, face):
        return {AXES[face // 2]: self.pos[face // 2] + (1 if face % 2 else -1)}

    def source(self, rnd, face):
        axis, high = face // 2, face % 2
        return (self.xs, self.ys, self.zs)[axis].at[rnd, high]

    def copies(self, rnd, face):
        axis, high = face // 2, face % 2
        src = self.source(rnd, face)
        dst = (self.xr, self.yr, self.zr)[axis]
        return pltpu.make_async_remote_copy(
            src_ref=src, dst_ref=dst.at[rnd, 1 - high],
            send_sem=self.send_sem.at[rnd, face], recv_sem=self.recv_sem.at[rnd, face ^ 1],
            device_id=self.neighbour(face), device_id_type=MESH)

    def send(self, rnd, face):
        @pl.when(self.has[face])
        def _():
            self.copies(rnd, face).start()

    def wait_recv(self, rnd, face):
        axis, high = face // 2, face % 2
        src = self.source(rnd, face)
        dst = (self.xr, self.yr, self.zr)[axis]

        @pl.when(self.has[face])
        def _():
            pltpu.make_async_remote_copy(
                src_ref=src, dst_ref=dst.at[rnd, high],
                send_sem=self.send_sem.at[rnd, face], recv_sem=self.recv_sem.at[rnd, face],
                device_id=self.neighbour(face), device_id_type=MESH).wait_recv()

    def wait_send(self, rnd, face):
        @pl.when(self.has[face])
        def _():
            self.copies(rnd, face).wait_send()


GROUPS = (('gx',), ('gy', 'gz'))


def group_of(comm, group):
    sizes = [comm.counts[AXES.index(name)] for name in group]
    size, rank = 1, 0
    for name, n in zip(group, sizes):
        size, rank = size * n, rank * n + comm.pos[AXES.index(name)]

    def peer(off):
        left, where = lax.rem(rank + off, size), {}
        for name, n in reversed(tuple(zip(group, sizes))):
            where[name], left = lax.rem(left, n), lax.div(left, n)
        return where
    return size, rank, peer


def greet_faces(comm):
    sem = pltpu.get_barrier_semaphore()
    for face in range(FACES):
        @pl.when(comm.has[face])
        def _():
            pl.semaphore_signal(sem, inc=1, device_id=comm.neighbour(face), device_id_type=MESH)
    return sem, sum(flag.astype(jnp.int32) for flag in comm.has)


def greet_groups(comm):
    sem, total = pltpu.get_barrier_semaphore(), 0
    for group in GROUPS:
        size, _, peer = group_of(comm, group)
        for off in range(1, size):
            pl.semaphore_signal(sem, inc=1, device_id=peer(off), device_id_type=MESH)
        total += size - 1
    return sem, total


class Reducer:
    def __init__(self, comm, send_row, recv_rows, send_sem, recv_sem):
        self.comm, self.send_row, self.recv_rows, self.ss, self.rs = comm, send_row, recv_rows, send_sem, recv_sem

    def run(self, row):
        for stage, group in enumerate(GROUPS):
            size, rank, peer = group_of(self.comm, group)
            rows = self.recv_rows[stage]
            self.send_row[stage] = row
            copies = [pltpu.make_async_remote_copy(
                src_ref=self.send_row.at[stage], dst_ref=rows.at[rank], send_sem=self.ss.at[stage, off],
                recv_sem=self.rs.at[stage, off], device_id=peer(off), device_id_type=MESH) for off in range(1, size)]
            for copy in copies:
                copy.start()
            rows[rank] = row
            for copy in copies:
                copy.wait()
            row = total_of(rows[i] for i in range(size))
        return row


def store_plane_faces(comm, rnd, ref, p):
    comm.ys[rnd, 0, p] = ref[p + 1, R0:R0 + 1, :]
    comm.ys[rnd, 1, p] = ref[p + 1, R0 + NY - 1:R0 + NY, :]


def pack_x_faces(comm, rnd, ref):
    half = FOLD
    lane = lane_iota(half)
    a, b = ref[1, R0:R0 + half, :], ref[1, R0 + half:R0 + NY, :]
    comm.xs[rnd, 0] = jnp.where(lane < HALF, a, turn_half(b))
    a, b = ref[NP, R0:R0 + half, :], ref[NP, R0 + half:R0 + NY, :]
    comm.xs[rnd, 1] = jnp.where(lane < HALF, turn_half(a), b)


def face_mask(turn, rows=FOLD):
    return ((lane_iota(rows) + 1) & LOW) < turn


def pack_z(comm, rnd, ref, tree):
    def fold(p, carry):
        low, high = ref[p + 1, R0:R0 + FOLD, :], ref[p + 1, R0 + FOLD:R0 + NY, :]
        tree[p] = jnp.where(face_mask(2), low, spin(high, 2))
        return carry
    lax.fori_loop(0, NP, fold, 0, unroll=NP)
    join_z(comm, rnd, tree)


def join_z(comm, rnd, tree):
    parts = [tree[p] for p in range(NP)]
    for turns in TURNS:
        merged = []
        for i in range(0, NP, 4)[:len(parts) // 4]:
            out = spin(parts[i + 3], turns[-1])
            for n in (2, 1):
                out = jnp.where(face_mask(turns[n]), spin(parts[i + n], turns[n - 1]), out)
            merged.append(jnp.where(face_mask(turns[0]), parts[i], out))
        parts = merged
    for end in range(2):
        comm.zs[rnd, end] = halve_z(parts[0], 1 - end)


def halve_z(packed, keep):
    even = (lane_iota(NP) & 1) == 1 - keep
    return jnp.where(even, packed[:NP], spin(packed[NP:], 1 if keep else LANES - 1))


def unpack_z(comm, rnd, tree):
    odd = (lane_iota(NP) & 1) == 1
    low, high = comm.zr[rnd, 0], comm.zr[rnd, 1]
    parts = [jnp.concatenate([jnp.where(odd, spin(high, LOW - 2 - i), spin(low, LOW + i)) for i in range(2)], axis=0)]
    for turns in reversed(TURNS):
        parts = [q for part in parts for q in (part, *(spin(part, LANES - turn) for turn in turns))]
    for p in range(NP):
        tree[p] = parts[p]


def spread_z(comm, rnd, tree, ghost):
    unpack_z(comm, rnd, tree)

    def fold(p, carry):
        ghost[p, 0:FOLD, :] = spin(tree[p], 2)
        ghost[p, FOLD:NY, :] = tree[p]
        return carry
    lax.fori_loop(0, NP, fold, 0, unroll=NP)


def inner_planes(ref):
    low = lane_iota(NY) < HALF
    ref[0, R0:R0 + NY, :] = jnp.where(low, 0.0, turn_half(ref[NP, R0:R0 + NY, :]))
    ref[NP + 1, R0:R0 + NY, :] = jnp.where(low, turn_half(ref[1, R0:R0 + NY, :]), 0.0)


def x_ghosts(comm, rnd):
    low = lane_iota(FOLD) < HALF
    lo, hi = comm.xr[rnd, 0], comm.xr[rnd, 1]
    below = [jnp.where(low, lo, 0.0), jnp.where(low, turn_half(lo), 0.0)]
    above = [jnp.where(low, 0.0, turn_half(hi)), jnp.where(low, 0.0, hi)]
    return below, above


def outer_layers(comm, rnd, ref):
    inner_planes(ref)
    below, above = x_ghosts(comm, rnd)
    for i in range(2):
        rows = slice(R0 + FOLD * i, R0 + FOLD * i + FOLD)
        ref[0, rows, :] = ref[0, rows, :] + below[i]
        ref[NP + 1, rows, :] = ref[NP + 1, rows, :] + above[i]
    for p in range(NP):
        ref[p + 1, R0 - 1:R0, :] = comm.yr[rnd, 0, p]
        ref[p + 1, R0 + NY:R0 + NY + 1, :] = comm.yr[rnd, 1, p]


def blank_rows(ref):
    for p in range(NP):
        ref[p + 1, R0 - 1:R0, :] = jnp.zeros((1, LANES), F32)
        ref[p + 1, R0 + NY:R0 + NY + 1, :] = jnp.zeros((1, LANES), F32)


def neighbours(ref, p, t, ghost=None):
    row = R0 + SUB * t
    lane = lane_iota() & LOW
    centre = ref[p + 1, own(t), :]
    xm = ref[p, own(t), :]
    xp = ref[p + 2, own(t), :]
    ym = ref[p + 1, row - 1:row + SUB - 1, :]
    yp = ref[p + 1, row + 1:row + SUB + 1, :]
    zm, zp = spin(centre, 1), spin(centre, LANES - 1)
    if ghost is not None:
        edge = ghost[p, tile(t), :]
        zm, zp = jnp.where(lane == 0, edge, zm), jnp.where(lane == LOW, edge, zp)
    return centre, (xm, xp, ym, yp, zm, zp)


def sweep(body, state=(), unroll=2):
    def plane(p, carry):
        carry = list(carry)
        body(p, carry)
        return tuple(carry)
    return lax.fori_loop(0, NP, plane, tuple(state), unroll=unroll)


def zero_tiles(n):
    return tuple(jnp.zeros(TILE, F32) for _ in range(n))


def send_faces(comm, rnd, ref, tree, folded=False):
    if not folded:
        for p in range(NP):
            store_plane_faces(comm, rnd, ref, p)
    for face in (2, 3):
        comm.send(rnd, face)
    (join_z if folded else functools.partial(pack_z, ref=ref))(comm, rnd, tree=tree)
    for face in (4, 5):
        comm.send(rnd, face)
    pack_x_faces(comm, rnd, ref)
    for face in (0, 1):
        comm.send(rnd, face)


def load_field(raw, ref):
    def body(p, state):
        ref[p + 1, R0:R0 + NY, :] = jnp.concatenate([raw[p], raw[p + NP]], axis=1)
    sweep(body, unroll=NP)


def fill_ghost_conductivity(comm, square, gx_slab, gy_slab, gz_slab):
    px, py, pz = comm.pos
    half = FOLD
    turn = 64 * lax.rem(pz, 2)
    lane = lane_iota(half)
    a, b = pltpu.roll(gx_slab[0:half, :], turn, 1), pltpu.roll(gx_slab[half:NY, :], turn, 1)
    x_face = jnp.where(lane < HALF, a, turn_half(b))
    for end in range(2):
        @pl.when(jnp.logical_not(comm.has[end]))
        def _():
            comm.xr[0, end] = x_face
    rows = pltpu.roll(gy_slab[...], turn, 1)
    y_face = jnp.where(lane_iota(NP) < HALF, rows[0:NP], turn_half(rows[NP:NX]))
    for end in range(2):
        @pl.when(jnp.logical_not(comm.has[2 + end]))
        def _():
            for p in range(NP):
                comm.yr[0, end, p] = y_face[one(p)]
    for end in range(2):
        @pl.when(jnp.logical_not(comm.has[4 + end]))
        def _():
            cols = spin(gz_slab[...], HALF * lax.rem(py, 2))
            shift = 0 if end else LOW
            square[...] = jnp.zeros(square.shape, F32)
            for x in range(NX):
                for c in range(2):
                    square[one((4 * (x % NP) + 2 * c + HALF * (x // NP) + shift) % LANES)] = cols[one(x)]
            turned = square[...].T
            second = ((lane_iota(FOLD) - shift) & 3) == 2
            comm.zr[0, end] = halve_z(jnp.where(second, turned[FOLD:NY], turned[:FOLD]), end)


def zero_ends(comm, rounds):
    for face in range(FACES):
        @pl.when(jnp.logical_not(comm.has[face]))
        def _():
            buf = (comm.xr, comm.yr, comm.zr)[face // 2]

            def clear(rnd, carry):
                buf[rnd, face % 2] = jnp.zeros(buf.shape[2:], F32)
                return carry
            lax.fori_loop(1, rounds, clear, 0)


class Parts:
    def __init__(self, src, dst, sems, first):
        step = NX // PARTS
        self.copies = [pltpu.make_async_copy(src.at[pl.ds(step * i, step)], dst.at[pl.ds(step * i, step)],
                                             sems.at[first + i]) for i in range(PARTS)]

    def start(self):
        for copy in self.copies:
            copy.start()

    def wait(self):
        for copy in self.copies:
            copy.wait()


def lanes_of(pos):
    return pl.ds(pl.multiple_of(lax.div(pos, 2) * LANES, LANES), LANES)


def start_up(comm, ins, raws, slabs, load_sem):
    k_hbm, g_hbm, f_hbm, u_hbm = ins
    px, py, pz = comm.pos
    loads = [Parts(k_hbm, raws[0], load_sem, FACES),
             Parts(u_hbm, raws[1], load_sem, FACES + PARTS)]
    x_row = jnp.where(comm.has[1], 0, 1)
    y_row = jnp.where(comm.has[3], 2, 3)
    z_row = jnp.where(comm.has[5], 4, 5)
    z_lanes = lanes_of(pz)
    y_lanes = lanes_of(py)
    loads.append(pltpu.make_async_copy(
        g_hbm.at[x_row, pl.ds(pl.multiple_of(py * NY, NY), NY), z_lanes], slabs[0], load_sem.at[2]))
    loads.append(pltpu.make_async_copy(
        g_hbm.at[y_row, pl.ds(pl.multiple_of(px * NX, NX), NX), z_lanes], slabs[1], load_sem.at[3]))
    loads.append(pltpu.make_async_copy(
        g_hbm.at[z_row, pl.ds(pl.multiple_of(px * NX, NX), NX), y_lanes], slabs[2], load_sem.at[4]))
    loads.append(Parts(f_hbm, raws[2], load_sem, FACES + 2 * PARTS))
    for load in loads:
        load.start()
    return loads


def first_exchange(comm, loads, greet, raws, slabs, k_ref, u_ref, tree, square, k_ghost, u_ghost):
    sem, total = greet
    loads[0].wait()
    load_field(raws[0], k_ref)
    pl.semaphore_wait(sem, total)
    send_faces(comm, 0, k_ref, tree)
    loads[1].wait()
    load_field(raws[1], u_ref)
    send_faces(comm, 1, u_ref, tree)
    for load in loads[2:]:
        load.wait()
    fill_ghost_conductivity(comm, square, *slabs)
    for rnd, ref, ghost in ((0, k_ref, k_ghost), (1, u_ref, u_ghost)):
        for face in range(FACES):
            comm.wait_recv(rnd, face)
        outer_layers(comm, rnd, ref)
        spread_z(comm, rnd, tree, ghost)


def first_residual(raw_f, k_ref, u_ref, k_ghost, u_ghost, p, t, d_ref):
    centre, others = neighbours(k_ref, p, t, k_ghost)
    u_own, u_others = neighbours(u_ref, p, t, u_ghost)
    twice = centre + centre
    weights = [twice * other / (centre + other) for other in others]
    diag = total_of(weights)
    au = total_of([w * (u_own - other) for w, other in zip(weights, u_others)])
    f_tile = jnp.concatenate([raw_f[p, tile(t), :], raw_f[p + NP, tile(t), :]], axis=1)
    d_ref[p, tile(t), :] = diag
    return weights, f_tile - au, 1.0 / diag


def write_plane(raw_ref, p, values):
    raw_ref[p] = values[:, :HALF]
    raw_ref[p + NP] = turn_half(values)[:, :HALF]


def dot_rows(a, b):
    prod = a[:2 * SUB] * b[:2 * SUB]
    return row_sum(prod[:SUB] + prod[SUB:])


def solve_coefficients(row, mom_ref, pc_ref, hist_ref, full_ref):
    lane24, line24 = lane_iota(24), row_iota(24)
    wide = jnp.broadcast_to(row, (24, LANES))
    base = lane_sum(jnp.where((lane24 == line24 + 1) & (line24 < 17), wide, 0.0))
    base = jnp.broadcast_to(base, (24, LANES))
    first, second = base[0:1], base[1:2]
    even = (line24 & 1) == 0
    mom = jnp.where(line24 >= 2, 2.0 * base - jnp.where(even, first, second), base)
    mom = jnp.where(line24 < 17, mom, 0.0)
    lane16, line16 = lane_iota(16), row_iota(16)
    wide = jnp.broadcast_to(row, WIDE)
    for k in range(NB):
        big = jnp.maximum(line16, k)
        small = jnp.minimum(line16, k)
        want = GRAM + NB * big + small
        col = lane_sum(jnp.where((lane16 == want) & (line16 < NB), wide, 0.0))
        full_ref[k] = jnp.broadcast_to(col, WIDE)
    zeros8 = jnp.zeros(TILE, F32)
    mom_ref[:SUB] = zeros8
    mom_ref[32:40] = zeros8
    pc_ref[:SUB] = zeros8
    pc_ref[24:32] = zeros8
    unit = jnp.where(line16 == 0, 1.0, 0.0)
    cvec, pvec, avec = unit, unit, jnp.zeros(WIDE, F32)
    rvec, mvec = mom, mom
    mu0 = mom[0:1]
    rho = dot_rows(cvec, rvec)
    ok = jnp.where(rho > 0.0, 1.0, 0.0)
    two_one = jnp.where(line16 == 1, 2.0, 1.0)
    for t in range(CG_ITERS):
        mom_ref[8:32] = mvec
        mom_ref[7:8] = mvec[1:2]
        pc_ref[8:24] = pvec
        qvec = mvec - 0.5 * (mom_ref[9:33] + mom_ref[7:31])
        npvec = 0.5 * (two_one * pc_ref[7:23] + pc_ref[9:25])
        curv = dot_rows(pvec, qvec)
        size = row_sum(jnp.abs(pvec))
        ok = jnp.where(size * size * mu0 < BOUND * curv, ok, 0.0)
        alpha = rho / curv
        avec = avec + alpha * pvec
        cvec = cvec - alpha * (pvec - npvec)
        rvec = rvec - alpha * qvec
        hist_ref[t] = cvec
        rho_new = dot_rows(cvec, rvec)
        size = row_sum(jnp.abs(cvec))
        ok = jnp.where(size * size * mu0 < BOUND * rho_new, ok, 0.0)
        beta = rho_new / rho
        pvec = cvec + beta * pvec
        mvec = rvec + beta * mvec
        rho = rho_new
    return avec, cvec, ok


def squares_row(hist_ref, full_ref):
    lane = lane_iota(1)
    out = jnp.zeros((1, LANES), F32)
    for t in range(CG_ITERS):
        cvec = hist_ref[t]
        acc = full_ref[0] * hist_ref[t, one(0)]
        for j in range(1, NB):
            acc = acc + full_ref[j] * hist_ref[t, one(j)]
        out = jnp.where(lane == t, dot_rows(acc, cvec), out)
    return out


def basis_kernel(counts, k_hbm, g_hbm, f_hbm, u_hbm, u_out, r_out, h_ref, ok_ref,
                 raw_k, raw_u, raw_f, slab_x, slab_y, slab_z, k_ref, u_ref, z_ref, coef_ref, d_ref, sums_ref,
                 mom_ref, pc_ref, hist_ref, full_ref, comb_ref, edge_ref, part_ref, tree, square, k_ghost, u_ghost,
                 xs, ys, zs, xr, yr, zr, send_row, rows_a, rows_b,
                 load_sem, send_sem, recv_sem, red_ss, red_rs):
    comm = Comm(counts, (xs, ys, zs, xr, yr, zr, send_sem, recv_sem))
    raws, slabs = (raw_k, raw_u, raw_f), (slab_x, slab_y, slab_z)
    loads = start_up(comm, (k_hbm, g_hbm, f_hbm, u_hbm), raws, slabs, load_sem)
    greet = greet_faces(comm)
    zero_ends(comm, CG_ITERS + 2)
    sums_ref[...] = jnp.zeros(sums_ref.shape, F32)

    def blank(k, carry):
        blank_rows(z_ref.at[k + 1])
        return carry
    lax.fori_loop(0, CG_ITERS, blank, 0)

    def nothing(p, state):
        z_ref[0, p + 1, R0:R0 + NY, :] = jnp.zeros((NY, LANES), F32)
    sweep(nothing, unroll=4)
    first_exchange(comm, loads, greet, raws, slabs, k_ref, u_ref, tree, square, k_ghost, u_ghost)

    def first(p, state):
        lane = lane_iota() & LOW
        for t in range(ROWS):
            weights, resid, inv = first_residual(raw_f, k_ref, u_ref, k_ghost, u_ghost, p, t, d_ref)
            factor = inv + inv
            scaled = [w * factor for w in weights]
            low, high = scaled[4:]
            edge_ref[p, tile(t), :] = jnp.where(lane == 0, low, jnp.where(lane == LOW, high, 0.0))
            scaled[4:] = jnp.where(lane == 0, 0.0, low), jnp.where(lane == LOW, 0.0, high)
            for i in range(FACES):
                coef_ref[p, t, i] = scaled[i]
            z_ref[1, p + 1, own(t), :] = resid * inv

    sweep(first, unroll=8)
    send_faces(comm, 2, z_ref.at[1], tree)

    def products(k):
        def body(p, accs):
            for t in range(ROWS):
                d = d_ref[p, tile(t), :]
                z_k = z_ref[k + 1, p + 1, own(t), :]
                dz = d * z_k
                ddz = d * dz
                for i in range(NB):
                    accs[i] = accs[i] + ddz * z_ref[i + 1, p + 1, own(t), :]
                accs[NB] = accs[NB] + dz * z_k
                accs[NB + 1] = accs[NB + 1] + dz * z_ref[k, p + 1, own(t), :]
        accs = sweep(body, zero_tiles(NB + 2), unroll=4)
        rows = [GRAM + NB * k + i for i in range(NB)] + [2 * k + 1, 2 * k]
        for row, acc in zip(rows, accs):
            sums_ref[pl.ds(row, 1), :] = row_sum(acc)

    def weight(k):
        return jnp.where(k == 0, 0.5, 1.0)

    def x_terms(k, rnd):
        factor = weight(k)
        below, above = x_ghosts(comm, rnd)
        for t in range(ROWS):
            part = slice(SUB * (t % 4), SUB * (t % 4) + SUB)
            for plane, face, layer in ((0, 0, below), (NP - 1, 1, above)):
                term = coef_ref[plane, t, face] * layer[t // 4][part]
                part_ref[plane, tile(t), :] = part_ref[plane, tile(t), :] + factor * term

    def late_terms(k, rnd):
        ref, factor = z_ref.at[k + 2], weight(k)
        unpack_z(comm, rnd, tree)
        first, last = row_iota(SUB) == 0, row_iota(SUB) == SUB - 1

        def body(p, state):
            turned = [spin(tree[p], 2), tree[p]]
            news = []
            for t in range(ROWS):
                part = slice(SUB * (t % 4), SUB * (t % 4) + SUB)
                term = edge_ref[p, tile(t), :] * turned[t // 4][part]
                for end, at, sub, mask in ((0, 0, 0, first), (1, ROWS - 1, SUB - 1, last)):
                    if t == at:
                        line = coef_ref[p, t, 2 + end, one(sub), :] * comm.yr[rnd, end, p]
                        term = term + jnp.where(mask, line, 0.0)
                news.append(part_ref[p, tile(t), :] + factor * term)
                ref[p + 1, own(t), :] = news[t]
            comm.ys[rnd + 1, 0, p] = news[0][:1]
            comm.ys[rnd + 1, 1, p] = news[ROWS - 1][SUB - 1:]
            for t in range(4):
                tree[p, tile(t), :] = jnp.where(face_mask(2, SUB), news[t], spin(news[t + 4], 2))
        sweep(body, unroll=NP)

    def apply(k, carry):
        rnd, factor = k + 2, weight(k)
        ref = z_ref.at[k + 1]
        inner_planes(ref)

        def step(p, state):
            for t in range(ROWS):
                _, others = neighbours(ref, p, t)
                total = total_of(coef_ref[p, t, i] * others[i] for i in range(FACES))
                part_ref[p, tile(t), :] = factor * total - z_ref[k, p + 1, own(t), :]

        sweep(step)
        products(k)
        for face in range(FACES):
            comm.wait_recv(rnd, face)
            if face == 1:
                x_terms(k, rnd)
        late_terms(k, rnd)

        @pl.when(k < CG_ITERS - 1)
        def _():
            send_faces(comm, rnd + 1, z_ref.at[k + 2], tree, folded=True)
        return carry

    lax.fori_loop(0, CG_ITERS, apply, 0)
    products(CG_ITERS)

    total = jnp.broadcast_to(lane_sum(sums_ref[...]), (LANES, LANES))
    row = row_sum(jnp.where(lane_iota(LANES) == row_iota(LANES), total, 0.0))
    red = Reducer(comm, send_row, (rows_a, rows_b), red_ss, red_rs)
    row = red.run(row)
    avec, cvec, ok = solve_coefficients(row, mom_ref, pc_ref, hist_ref, full_ref)
    comb_ref[0] = avec
    comb_ref[1] = cvec

    a_co = [jnp.broadcast_to(comb_ref[0, one(i)], TILE) for i in range(CG_ITERS)]
    c_co = [jnp.broadcast_to(comb_ref[1, one(i)], TILE) for i in range(NB)]

    def combine(p, carry):
        for t in range(ROWS):
            row = own(t)
            rows = tile(t)
            basis = [z_ref[i + 1, p + 1, row, :] for i in range(NB)]
            ut, rt = a_co[0] * basis[0], c_co[0] * basis[0]
            for i in range(1, NB):
                if i < CG_ITERS:
                    ut = ut + a_co[i] * basis[i]
                rt = rt + c_co[i] * basis[i]
            ut = u_ref[p + 1, row, :] + ut
            rt = d_ref[p, rows, :] * rt
            u_out[p, rows, :] = ut[:, :HALF]
            u_out[p + NP, rows, :] = turn_half(ut)[:, :HALF]
            r_out[p, rows, :] = rt[:, :HALF]
            r_out[p + NP, rows, :] = turn_half(rt)[:, :HALF]
        return carry

    lax.fori_loop(0, NP, combine, 0, unroll=8)
    h_ref[...] = squares_row(hist_ref, full_ref)
    ok_ref[0, 0] = ok[0, 0].astype(jnp.int32)

    def drain(rnd, carry):
        for face in range(FACES):
            comm.wait_send(rnd, face)
        return carry
    lax.fori_loop(0, CG_ITERS + 2, drain, 0)


def plain_kernel(counts, k_hbm, g_hbm, f_hbm, u_hbm, u_out, r_out, h_ref,
                 raw_k, raw_u, raw_f, slab_x, slab_y, slab_z, k_ref, u_ref, p_ref, q_ref, r_ref, coef_ref, d_ref, tree, square, k_ghost, u_ghost,
                 xs, ys, zs, xr, yr, zr, send_row, rows_a, rows_b,
                 load_sem, send_sem, recv_sem, red_ss, red_rs):
    comm = Comm(counts, (xs, ys, zs, xr, yr, zr, send_sem, recv_sem))
    raws, slabs = (raw_k, raw_u, raw_f), (slab_x, slab_y, slab_z)
    loads = start_up(comm, (k_hbm, g_hbm, f_hbm, u_hbm), raws, slabs, load_sem)
    greet = greet_groups(comm)
    zero_ends(comm, 3)
    first_exchange(comm, loads, greet, raws, slabs, k_ref, u_ref, tree, square, k_ghost, u_ghost)
    red = [Reducer(comm, send_row.at[i], (rows_a.at[i], rows_b.at[i]), red_ss.at[i], red_rs.at[i]) for i in range(2)]

    def reduce(which, accs):
        lane = lane_iota(1)
        row = jnp.zeros((1, LANES), F32)
        for i, acc in enumerate(accs):
            total = row_sum(lane_sum(acc))
            row = jnp.where(lane == i, jnp.broadcast_to(total, (1, LANES)), row)
        row = red[which].run(row)
        return [lane_sum(jnp.where(lane == i, row, 0.0)) for i in range(len(accs))]

    def first(p, state):
        for t in range(ROWS):
            weights, resid, inv = first_residual(raw_f, k_ref, u_ref, k_ghost, u_ghost, p, t, d_ref)
            for i in range(FACES):
                coef_ref[p, t, i] = weights[i]
            r_ref[p, tile(t), :] = resid
            z_new = resid * inv
            p_ref[p + 1, own(t), :] = z_new
            state[0] = state[0] + resid * z_new

    rho, = reduce(0, sweep(first, zero_tiles(1)))

    def iteration(it, carry):
        rho, hist = carry

        send_faces(comm, 2, p_ref, tree)
        for face in range(FACES):
            comm.wait_recv(2, face)
            comm.wait_send(2, face)
        outer_layers(comm, 2, p_ref)
        spread_z(comm, 2, tree, k_ghost)

        def apply(p, state):
            for t in range(ROWS):
                centre, others = neighbours(p_ref, p, t, k_ghost)
                q = total_of(coef_ref[p, t, i] * (centre - others[i]) for i in range(FACES))
                q_ref[p, tile(t), :] = q
                state[0] = state[0] + centre * q

        curv, = reduce(1, sweep(apply, zero_tiles(1)))
        alpha = jnp.broadcast_to(rho / curv, TILE)

        def update(p, accs):
            acc_z, acc_r = accs
            for t in range(ROWS):
                row = own(t)
                rows = tile(t)
                u_ref[p + 1, row, :] = u_ref[p + 1, row, :] + alpha * p_ref[p + 1, row, :]
                resid = r_ref[p, rows, :] - alpha * q_ref[p, rows, :]
                r_ref[p, rows, :] = resid
                acc_z = acc_z + resid * (resid / d_ref[p, rows, :])
                acc_r = acc_r + resid * resid
            return acc_z, acc_r

        rho_new, rr = reduce(0, lax.fori_loop(0, NP, update, zero_tiles(2)))
        beta = jnp.broadcast_to(rho_new / rho, TILE)

        def turn(p, carry):
            for t in range(ROWS):
                row = own(t)
                rows = tile(t)
                p_ref[p + 1, row, :] = r_ref[p, rows, :] / d_ref[p, rows, :] + beta * p_ref[p + 1, row, :]
            return carry

        lax.fori_loop(0, NP, turn, 0)
        hist = jnp.where(lane_iota(1) == it, jnp.broadcast_to(rr, (1, LANES)), hist)
        return rho_new, hist

    _, hist = lax.fori_loop(0, CG_ITERS, iteration, (rho, jnp.zeros((1, LANES), F32)))
    h_ref[...] = hist

    def finish(p, carry):
        write_plane(u_out, p, u_ref[p + 1, R0:R0 + NY, :])
        write_plane(r_out, p, r_ref[p])
        return carry

    lax.fori_loop(0, NP, finish, 0)
    for rnd in range(2):
        for face in range(FACES):
            comm.wait_send(rnd, face)


def finish_kernel(u_in, r_in, u_hbm, r_hbm, sems):
    copies = [Parts(u_in, u_hbm, sems, 0), Parts(r_in, r_hbm, sems, PARTS)]
    for copy in copies:
        copy.start()
    for copy in copies:
        copy.wait()


def scratch_for(kind, counts):
    field = (NP + 2, NY + 16, LANES)
    block = (NP, NY, LANES)
    vm = lambda *shape: pltpu.VMEM(shape, F32)
    raws = [vm(NX, NY, NZ)] * 3 + [vm(NY, LANES), vm(NX, LANES), vm(NX, LANES)]
    if kind == 'basis':
        rounds, reds = CG_ITERS + 2, ()
        work = [vm(*field), vm(*field), vm(NB + 1, *field), vm(NP, ROWS, FACES, *TILE), vm(*block), vm(LANES, LANES),
                vm(40, LANES), vm(32, LANES), vm(CG_ITERS, 16, LANES), vm(NB, 16, LANES), vm(2, 16, LANES), vm(*block), vm(*block)]
    else:
        rounds, reds = 3, (2,)
        work = [vm(*field), vm(*field), vm(*field), vm(*block), vm(*block), vm(NP, ROWS, FACES, *TILE), vm(*block)]
    work += [vm(NP, FOLD, LANES), vm(LANES, LANES), vm(*block), vm(*block)]
    x_side, y_side = vm(rounds, 2, FOLD, LANES), vm(rounds + 1, 2, NP, 1, LANES)
    faces = [x_side, y_side, vm(rounds, 2, NP, LANES)] * 2
    sizes = [counts[0], counts[1] * counts[2]]
    rows = [vm(*reds, 2, 1, LANES)] + [vm(*reds, n, 1, LANES) for n in sizes]
    dma = pltpu.SemaphoreType.DMA
    sems = [dma((FACES + 3 * PARTS,)), dma((rounds, 6)), dma((rounds, 6)), dma((*reds, 2, max(sizes))), dma((*reds, 2, max(sizes)))]
    return raws + work + faces + rows + sems


def solution(mesh):
    counts = tuple(mesh.shape[name] for name in AXES)
    grid_spec = P(*AXES)
    block = jax.ShapeDtypeStruct((NX, NY, NZ), F32)

    def call(kernel, kind, ident, *more):
        hbm, vmem = pl.BlockSpec(memory_space=pltpu.HBM), pl.BlockSpec(memory_space=pltpu.VMEM)
        smem = [pl.BlockSpec(memory_space=pltpu.SMEM)] * len(more)
        return pl.pallas_call(
            functools.partial(kernel, counts),
            out_shape=(block, block, jax.ShapeDtypeStruct((1, LANES), F32), *more),
            in_specs=[hbm] * 4,
            out_specs=(vmem, vmem, vmem, *smem),
            scratch_shapes=scratch_for(kind, counts),
            compiler_params=pltpu.CompilerParams(collective_id=ident, has_side_effects=True, vmem_limit_bytes=VMEM_BYTES),
            name=kind,
        )

    def local_solve(k_cell, k_ghost, f_rhs, u_init):
        args = (k_cell, k_ghost, f_rhs, u_init)
        *fast, ok = call(basis_kernel, 'basis', 0, jax.ShapeDtypeStruct((1, 1), jnp.int32))(*args)
        u_out, r_out, row = lax.cond(ok[0, 0] > 0, lambda: tuple(fast),
                                     lambda: tuple(call(plain_kernel, 'plain', 1)(*args)))
        u_out, r_out = pl.pallas_call(
            finish_kernel,
            out_shape=(block, block),
            in_specs=[pl.BlockSpec(memory_space=pltpu.VMEM)] * 2,
            out_specs=(pl.BlockSpec(memory_space=pltpu.HBM),) * 2,
            scratch_shapes=[pltpu.SemaphoreType.DMA((2 * PARTS,))],
            compiler_params=pltpu.CompilerParams(vmem_limit_bytes=VMEM_BYTES),
            name='finish',
        )(u_out, r_out)
        return u_out, r_out, row[0, 0:CG_ITERS]

    return jax.shard_map(local_solve, mesh=mesh, in_specs=(grid_spec, P(), grid_spec, grid_spec),
                         out_specs=(grid_spec, grid_spec, P()), check_vma=False)
```
